256 devices in a mesh: maps: 16 (over z, y_hi), row: 4 (over y_lo, core), col: 4 (over x).
Axes of the slice: x: 4, y: 4 (y_hi: 2, y_lo: 2; y = y_hi * 2 + y_lo), z: 8, core: 2. Of those that a mesh axis runs over, the one named last changes fastest.
Arguments:
- shear: float32 [2, 16, 2048, 2048], P(None, 'maps', 'row', 'col'), parts along dimension 1, may hold values from -600 to 600
- smoothing: float32 [16], P('maps'), parts along dimension 0, may hold values from 0.6 to 1.2
- offsets: int32 [16, 128, 128], P('maps', ('row', 'col')), parts along dimension 0, may hold values from 0 to 255
- thresholds: int32 [16, 16], P('maps'), parts along dimension 0, may hold values from -4 to 19
Outputs:
- snr: float32 [16, 2048, 2048], P('maps', ('row', 'col')), parts along dimension 0
- heights: float32 [16, 128, 128], P('maps', ('row', 'col')), parts along dimension 0
- counts: float32 [16, 16], P('maps'), parts along dimension 0
The draws below stay inside these ranges and needn't reach their ends.
There are 16 independent parts, one for each index of `maps`. The reference program is written for one: setup_inputs(seed, part) draws one part's arguments, and reference() takes and returns one part's arrays. A program takes and returns all parts, laid end to end along the dimension named above; each array names one. Nothing has to cross between parts.
All inputs are finite; a program needn't handle non-finite values.
Results may differ from the reference program's by a relative error of at most 0.00014.
Values sent between devices are 32-bit elements; how exact they have to be, the bound alone decides.
No kernel may reach another device: no remote copies, remote signals or barrier semaphores. Data moves between devices by JAX's collectives and lax.ppermute only.
A program may use at most 64 MiB of HBM per device.

```python
import math
import jax
import jax.numpy as jnp
from jax import lax

NX = 2048
NY = 2048
MAPS = 1
CELL = 16
NBINS = 16


def draw_shear(key, part):
    noise_key = jax.random.fold_in(jax.random.fold_in(key, 7), 0)
    ramp = 1.0 + 2.0 * jnp.arange(NX, dtype=jnp.float32) / (NX - 1)
    base = jnp.clip(jax.random.normal(noise_key, (2, MAPS, NX, NY), jnp.float32), -6.0, 6.0)
    return base * ramp[:, None]


def set_ends(drawn, rng, least, high):
    dims = drawn.shape
    spot = [jax.random.randint(jax.random.fold_in(rng, axis), (), 0, dims[axis]) for axis in range(len(dims))]
    drawn = drawn.at[tuple(spot)].set(least)
    longest = dims.index(max(dims))
    spot[longest] = (spot[longest] + 1) % dims[longest]
    return drawn.at[tuple(spot)].set(high)


def setup_inputs(seed: int = 0, part: int = 0) -> dict:
    splits = jax.random.split(jax.random.key(seed), 5)
    own_keys = jax.random.split(jax.random.fold_in(splits[4], part), 5)
    shear = draw_shear(jax.random.fold_in(jax.random.fold_in(splits[4], part), 71), part)
    smoothing = jnp.clip(jnp.exp(jax.random.uniform(own_keys[1], (MAPS,), jnp.float32, math.log(0.6), math.log(1.2))), 0.6, 1.2)
    offsets = set_ends(jax.random.randint(own_keys[2], (MAPS, NX // CELL, NY // CELL), 0, CELL * CELL), jax.random.fold_in(own_keys[2], 1), 0, (CELL * CELL) - 1).astype(jnp.int32)
    thresholds = set_ends(jax.random.randint(own_keys[3], (MAPS, NBINS), -4, 20), jax.random.fold_in(own_keys[3], 1), -4, 19).astype(jnp.int32)
    return dict(shear=shear, smoothing=smoothing, offsets=offsets, thresholds=thresholds)


def neighbour_max(field):
    nearest = None
    for step_row in (-1, 0, 1):
        for step_col in (-1, 0, 1):
            if step_row == 0 and step_col == 0:
                continue
            moved = jnp.roll(field, (step_row, step_col), axis=(1, 2))
            nearest = moved if nearest is None else jnp.maximum(nearest, moved)
    return nearest

def reference(shear, smoothing, offsets, thresholds):
    gamma = lax.complex(shear[0], shear[1])
    spectrum = jnp.fft.fft2(gamma, axes=(1, 2))
    freq_x = (jnp.fft.fftfreq(NX) * NX)[:, None]
    freq_y = (jnp.fft.fftfreq(NY) * NY)[None, :]
    square = jnp.maximum(freq_x * freq_x + freq_y * freq_y, 1.0)
    width = smoothing[:, None, None]
    damp = jnp.exp(-2.0 * math.pi ** 2 * width * width * ((freq_x / NX) ** 2 + (freq_y / NY) ** 2))
    kernel = lax.complex((freq_x * freq_x - freq_y * freq_y) / square * damp, -2.0 * freq_x * freq_y / square * damp)
    kappa = jnp.real(jnp.fft.ifft2(kernel * spectrum, axes=(1, 2)))
    rms = jnp.sqrt(lax.optimization_barrier(jnp.mean(kappa * kappa, axis=(1, 2))) + 1e-06)
    snr = kappa / rms[:, None, None]
    height_map = kappa - neighbour_max(kappa)
    full = jnp.repeat(jnp.repeat(offsets, CELL, axis=1), CELL, axis=2)
    code = (jnp.arange(NX, dtype=jnp.int32) % CELL)[:, None] * CELL + (jnp.arange(NY, dtype=jnp.int32) % CELL)[None, :]
    chosen = full == code[None]
    maps = kappa.shape[0]

    def pick(values):
        picked = jnp.where(chosen, values, 0.0)
        return picked.reshape(maps, NX // CELL, CELL, NY // CELL, CELL).sum(axis=(2, 4))
    heights = pick(height_map) / rms[:, None, None]
    values = pick(kappa) / rms[:, None, None]
    weight = jax.nn.sigmoid(heights / 0.05)
    levels = 0.25 * thresholds.astype(jnp.float32)
    above = jax.nn.sigmoid((values[..., None] - levels[:, None, None, :]) / 0.1)
    counts = lax.optimization_barrier(jnp.sum(weight[..., None] * above, axis=(1, 2)))
    return (snr, heights, counts)
```

```python
from functools import partial
import math

import jax
import jax.numpy as jnp
from jax import lax
from jax.experimental import pallas as pl
from jax.experimental.pallas import tpu as pltpu
from jax.sharding import PartitionSpec as P

N = 2048
INNER = 512
DEV = 16
ROWS = 128
LANES = 128
HALF = 64
CELL = 16
BLOCK = ROWS + 8
CLASSES = ((0, 0, 4), (2, 4, 4), (1, 8, 8))
MIB = 1 << 20


def call(kernel, out, scratch, limit, flops, ins):
    return pl.pallas_call(
        kernel,
        out_shape=out,
        in_specs=ins,
        scratch_shapes=scratch,
        compiler_params=pltpu.CompilerParams(vmem_limit_bytes=limit * MIB),
        cost_estimate=pl.CostEstimate(flops=flops, bytes_accessed=4 * MIB, transcendentals=0),
    )


def split(x):
    high = x.astype(jnp.bfloat16)
    return high, (x - high.astype(jnp.float32)).astype(jnp.bfloat16)


def dot3(left, right):
    dot = partial(jnp.dot, preferred_element_type=jnp.float32)
    return dot(left[0], right[0]) + (dot(left[0], right[1]) + dot(left[1], right[0]))


def angle(steps):
    wrapped = jnp.bitwise_and(steps, N - 1)
    wrapped = jnp.where(wrapped >= N // 2, wrapped - N, wrapped)
    return wrapped.astype(jnp.float32) * (2.0 * math.pi / N)


def iota(shape, dim):
    return lax.broadcasted_iota(jnp.int32, shape, dim)


def put(high_ref, low_ref, rows, cols, value):
    high, low = split(value)
    high_ref[rows, cols] = high
    low_ref[rows, cols] = low


def sample_form(refs, scratch):
    cos_ref, sin_ref = scratch
    for (start, _, blocks), (high_ref, low_ref) in zip(CLASSES, refs):
        width = LANES * blocks
        col = iota((HALF, width), 1)
        freq = start + 4 * (HALF * (col // LANES) + col % HALF)
        quarter = jnp.where(col % LANES >= HALF, 1, 0)
        if start == 0:
            freq = jnp.where(col == HALF, N // 2, freq)
            quarter = jnp.where(col == HALF, 0, quarter)
        fine = angle(freq * iota((HALF, width), 0))
        cos_ref[:, :width] = jnp.cos(fine)
        sin_ref[:, :width] = jnp.sin(fine)
        coarse = angle(freq[:8] * (HALF * iota((8, width), 0)) + INNER * quarter[:8])
        cos_high, sin_high = jnp.cos(coarse), jnp.sin(coarse)
        for part in range(INNER // HALF):
            cos_part, sin_part = cos_high[part : part + 1], sin_high[part : part + 1]
            rows = pl.ds(HALF * part, HALF)
            cos_fine, sin_fine = cos_ref[:, :width], sin_ref[:, :width]
            put(high_ref, low_ref, rows, slice(None), cos_part * cos_fine - sin_part * sin_fine)
            if start == 1:
                rows = pl.ds(INNER + HALF * part, HALF)
                value = -(sin_part * cos_fine + cos_part * sin_fine)
                put(high_ref, low_ref, rows, slice(None), value)


def frequency_form(refs, scratch):
    cos_ref, sin_ref = scratch
    fine = angle(4 * iota((HALF, INNER), 0) * iota((HALF, INNER), 1))
    cos_ref[:, :INNER] = jnp.cos(fine)
    sin_ref[:, :INNER] = jnp.sin(fine)
    for (start, _, blocks), (high_ref, low_ref) in zip(CLASSES, refs):
        coarse = angle((start + 4 * HALF * iota((8, INNER), 0)) * iota((8, INNER), 1))
        cos_high, sin_high = jnp.cos(coarse), jnp.sin(coarse)
        for part in range(blocks):
            cos_part, sin_part = cos_high[part : part + 1], sin_high[part : part + 1]
            cos_fine, sin_fine = cos_ref[:, :INNER], sin_ref[:, :INNER]
            cosine = cos_part * cos_fine - sin_part * sin_fine
            sine = -(sin_part * cos_fine + cos_part * sin_fine)
            if start == 0 and part == 0:
                flip = (1 - 2 * (iota((HALF, INNER), 1) & 1)).astype(jnp.float32)
                sine = jnp.where(iota((HALF, INNER), 0) == 0, flip, sine)
            upper, lower = pl.ds(LANES * part, HALF), pl.ds(LANES * part + HALF, HALF)
            put(high_ref, low_ref, upper, pl.ds(0, INNER), cosine)
            put(high_ref, low_ref, lower, pl.ds(0, INNER), sine)
            if start == 1:
                put(high_ref, low_ref, upper, pl.ds(INNER, INNER), sine)
                put(high_ref, low_ref, lower, pl.ds(INNER, INNER), -cosine)


def signed(freq):
    return jnp.where(freq < N // 2, freq, freq - N)


def lane_frequency(device, shape):
    lane = iota(shape, 1)
    block = jnp.where(device < 8, device % 4, device - 8)
    start = jnp.where(device < 4, 0, jnp.where(device < 8, 2, 1))
    freq = signed(start + 4 * (HALF * block + lane % HALF))
    nyquist = (device == 0) & (lane == HALF)
    freq = jnp.where(nyquist, -(N // 2), freq)
    single = nyquist | ((device == 0) & (lane == 0))
    return freq.astype(jnp.float32), jnp.where(single, 1.0, 2.0)


def tables_kernel(smooth_ref, device_ref, *refs):
    device = device_ref[0]
    scratch = refs[-2:]
    w_refs = tuple(zip(refs[0:6:2], refs[1:6:2]))
    f_refs = tuple(zip(refs[6:12:2], refs[7:12:2]))
    even_ref, odd_ref, last_ref = refs[12:15]
    sample_form(w_refs, scratch)
    frequency_form(f_refs, scratch)
    width = smooth_ref[0]
    decay = width * width * (-2.0 * math.pi**2 / (N * N))
    shape = (HALF, LANES)
    freq_y, weight = lane_frequency(device, shape)

    def factors(freq_x, weight):
        total = freq_x * freq_x + freq_y * freq_y
        scaled = jnp.exp(decay * total) * weight / jnp.maximum(total, 1.0)
        return (freq_x * freq_x - freq_y * freq_y) * scaled, 2.0 * freq_x * freq_y * scaled

    for start, first, blocks in CLASSES:
        for part in range(blocks):
            freq = signed(start + 4 * (HALF * part + iota(shape, 0)))
            row_weight = jnp.where(freq == 0, 1.0, 2.0) * (1.0 / (N * N))
            even, odd = factors(freq.astype(jnp.float32), weight * row_weight)
            rows = pl.ds(HALF * (first + part), HALF)
            even_ref[rows, :] = even
            odd_ref[rows, :] = odd
    even, odd = factors(jnp.full(shape, -N / 2, jnp.float32), weight * (1.0 / (N * N)))
    last_ref[0:8, :] = even[0:8]
    last_ref[8:16, :] = odd[0:8]


def tables(smoothing, device):
    low = jnp.bfloat16
    pairs = []
    for _ in range(2):
        for size in (INNER, INNER, 2 * INNER):
            pairs += [jax.ShapeDtypeStruct((size, size), low)] * 2
    out = pairs + [
        jax.ShapeDtypeStruct((N // 2, LANES), jnp.float32),
        jax.ShapeDtypeStruct((N // 2, LANES), jnp.float32),
        jax.ShapeDtypeStruct((16, LANES), jnp.float32),
    ]
    scratch = [pltpu.VMEM((HALF, 2 * INNER), jnp.float32)] * 2
    smem = pl.BlockSpec(memory_space=pltpu.SMEM)
    result = call(tables_kernel, out, scratch, 20, 10**7, [smem, smem])(smoothing, device)
    return result[0:6], result[6:12], result[12:15]


def quarters(blocks):
    first, second, third, fourth = blocks
    return (
        (first + third) + (second + fourth),
        (first + third) - (second + fourth),
        first - third,
        second - fourth,
    )


def columns_kernel(x_ref, w0h, w0l, w2h, w2l, w1h, w1l, out_ref):
    for field in range(2):
        zero, two, even, odd = quarters([x_ref[c, field] for c in range(4)])
        rows = pl.ds(ROWS * field, ROWS)

        def emit(value, first):
            for part in range(value.shape[1] // LANES):
                out_ref[first + part, rows, :] = value[:, LANES * part : LANES * (part + 1)]

        emit(dot3(split(zero), (w0h[...], w0l[...])), 0)
        emit(dot3(split(two), (w2h[...], w2l[...])), 4)
        both = jnp.concatenate([even, odd], axis=1)
        emit(dot3(split(both), (w1h[...], w1l[...])), 8)


def columns(x, table):
    out = jax.ShapeDtypeStruct((DEV, 2 * ROWS, LANES), jnp.float32)
    specs = [pl.BlockSpec(memory_space=pltpu.VMEM)] * 7
    return call(columns_kernel, out, (), 24, 2 * 10**9, specs)(x, *table)


def rows_kernel(device_ref, g_ref, *refs):
    w0h, w0l, w2h, w2l, w1h, w1l, f0h, f0l, f2h, f2l, f1h, f1l = refs[:12]
    even_ref, odd_ref, last_ref, out_ref, data_ref, spec_ref = refs[12:]
    device = device_ref[0]
    lane = iota((ROWS, LANES), 1)
    sign = jnp.where(lane < HALF, 1.0, -1.0)
    fix = (lane == HALF) & (device == 0)
    for s in range(DEV):
        first = g_ref[s, 0:ROWS, :]
        second = sign * pltpu.roll(g_ref[s, ROWS : 2 * ROWS, :], HALF, 1)
        rows = pl.ds(ROWS * s, ROWS)
        data_ref[rows, 0:LANES] = first
        data_ref[rows, LANES : 2 * LANES] = jnp.where(fix, -first, second)
    zero, two, even, odd = quarters([data_ref[INNER * r : INNER * (r + 1), :] for r in range(4)])
    spec_ref[0:INNER, :] = dot3((f0h[...], f0l[...]), split(zero))
    spec_ref[INNER : 2 * INNER, :] = dot3((f2h[...], f2l[...]), split(two))
    both = jnp.concatenate([even, odd], axis=0)
    spec_ref[2 * INNER : 4 * INNER, :] = dot3((f1h[...], f1l[...]), split(both))

    _, weight = lane_frequency(device, (8, LANES))
    total = jnp.zeros((HALF, LANES), jnp.float32)
    special = jnp.zeros((8, LANES), jnp.float32)
    row = iota((HALF, LANES), 0)
    for part in range(DEV):
        upper, lower = pl.ds(LANES * part, HALF), pl.ds(LANES * part + HALF, HALF)
        x_one, x_two = spec_ref[upper, 0:LANES], spec_ref[upper, LANES : 2 * LANES]
        y_one, y_two = spec_ref[lower, 0:LANES], spec_ref[lower, LANES : 2 * LANES]
        rows = pl.ds(HALF * part, HALF)
        even, odd = even_ref[rows, :], odd_ref[rows, :]
        cosine = even * x_one - odd * y_two
        sine = even * y_one + odd * x_two
        if part == 0:
            edge, other = y_one[0:8], y_two[0:8]
            side = iota((8, LANES), 1)
            turned = jnp.where(side < HALF, 1.0, -1.0) * pltpu.roll(edge, HALF, 1)
            corner = (side == HALF) & (device == 0)
            turned = jnp.where(corner, pltpu.roll(other, HALF, 1), turned)
            edge = last_ref[0:8, :] * edge + last_ref[8:16, :] * turned
            edge = jnp.concatenate([edge] * 8, axis=0)
            cosine = jnp.where(row == 0, even * x_one, cosine)
            sine = jnp.where(row == 0, edge, sine)
            special = (cosine * cosine + sine * sine)[0:8]
        total = total + (cosine * cosine + sine * sine)
        data_ref[LANES * part : LANES * part + HALF, 0:LANES] = cosine
        data_ref[LANES * part + HALF : LANES * (part + 1), 0:LANES] = sine
    special = jnp.where(iota((8, LANES), 0) == 0, special, 0.0)
    energy = jnp.sum(total, axis=0, keepdims=True) + jnp.sum(special, axis=0, keepdims=True)
    energy = 0.5 * energy / weight[0:1]

    zero = dot3((w0h[...], w0l[...]), split(data_ref[0:INNER, 0:LANES]))
    two = dot3((w2h[...], w2l[...]), split(data_ref[INNER : 2 * INNER, 0:LANES]))
    odd = dot3((w1h[...], w1l[...]), split(data_ref[2 * INNER : 4 * INNER, 0:LANES]))
    plus, minus = zero + two, zero - two
    real, turned = odd[0:INNER], odd[INNER : 2 * INNER]
    for r, value in enumerate((plus + real, minus + turned, plus - real, minus - turned)):
        for part in range(4):
            out_ref[4 * r + part, 0:ROWS, :] = value[ROWS * part : ROWS * (part + 1)]
    for s in range(DEV):
        out_ref[s, ROWS : ROWS + 1, :] = out_ref[(s - 1) % DEV, ROWS - 1 : ROWS, :]
        out_ref[s, ROWS + 1 : ROWS + 2, :] = out_ref[(s + 1) % DEV, 0:1, :]
        out_ref[s, ROWS + 2 : ROWS + 3, :] = energy
        out_ref[s, ROWS + 3 : BLOCK, :] = jnp.zeros((BLOCK - ROWS - 3, LANES), jnp.float32)


def row_pass(device, g, sample, frequency, factors):
    out = jax.ShapeDtypeStruct((DEV, BLOCK, LANES), jnp.float32)
    scratch = [pltpu.VMEM((N, 2 * LANES), jnp.float32)] * 2
    specs = [pl.BlockSpec(memory_space=pltpu.SMEM)] + [pl.BlockSpec(memory_space=pltpu.VMEM)] * 16
    run = call(rows_kernel, out, scratch, 36, 4 * 10**9, specs)
    return run(device, g, *sample, *frequency, *factors)


def peaks_kernel(bins_ref, x_ref, f0h, f0l, f2h, f2l, f1h, f1l, offsets_ref, *refs):
    kappa_ref, heights_ref, counts_ref, inverse_ref, field_ref, wide_ref, pick_ref = refs

    def block(first, count):
        body = jnp.concatenate([x_ref[s] for s in range(first, first + count)], axis=1)
        pad = jnp.zeros((8, body.shape[1]), jnp.float32)
        return split(jnp.concatenate([body, pad], axis=0))

    zero = dot3(block(0, 4), (f0h[...], f0l[...]))
    two = dot3(block(4, 4), (f2h[...], f2l[...]))
    odd = dot3(block(8, 8), (f1h[...], f1l[...]))
    plus, minus = zero + two, zero - two
    real, turned = odd[:, 0:INNER], odd[:, INNER : 2 * INNER]
    energy = x_ref[0, ROWS : BLOCK, :]
    for s in range(1, DEV):
        energy = energy + x_ref[s, ROWS : BLOCK, :]
    mean = jnp.sum(energy[2:3, :], axis=1, keepdims=True)
    inverse = 1.0 / jnp.sqrt(mean + 1e-06)
    for c, value in enumerate((plus + real, minus + turned, plus - real, minus - turned)):
        cols = pl.ds(INNER * c, INNER)
        kappa_ref[:, cols] = value[0:ROWS]
        field_ref[8 : ROWS + 8, cols] = value[0:ROWS]
        field_ref[7:8, cols] = value[ROWS : ROWS + 1]
        field_ref[ROWS + 8 : ROWS + 9, cols] = value[ROWS + 1 : ROWS + 2]
    for start in (0,) + tuple(range(8, ROWS + 8, 16)) + (ROWS + 8,):
        size = 8 if start in (0, ROWS + 8) else 16
        value = field_ref[start : start + size, :]
        side = jnp.maximum(pltpu.roll(value, 1, 1), pltpu.roll(value, N - 1, 1))
        wide_ref[start : start + size, :] = jnp.maximum(side, value)
    blocks = iota((LANES, N), 1) // CELL == iota((LANES, N), 0)
    blocks = jnp.where(blocks, 1.0, 0.0).astype(jnp.bfloat16)
    offsets = offsets_ref[...].astype(jnp.float32).astype(jnp.bfloat16)
    offsets = jnp.concatenate([offsets, offsets], axis=0)
    spread = jnp.dot(offsets, blocks, preferred_element_type=jnp.float32)
    code = (iota((CELL, N), 0) * CELL + (iota((CELL, N), 1) & (CELL - 1))).astype(jnp.float32)
    for p in range(ROWS // CELL):
        base = 8 + CELL * p
        value = field_ref[base : base + CELL, :]
        side = jnp.maximum(pltpu.roll(value, 1, 1), pltpu.roll(value, N - 1, 1))
        above = wide_ref[base - 1 : base - 1 + CELL, :]
        below = wide_ref[base + 1 : base + 1 + CELL, :]
        nearest = jnp.maximum(side, jnp.maximum(above, below))
        chosen = spread[p : p + 1, :] == code
        height = jnp.sum(jnp.where(chosen, value - nearest, 0.0), axis=0, keepdims=True)
        level = jnp.sum(jnp.where(chosen, value, 0.0), axis=0, keepdims=True)
        pick_ref[p : p + 1, :] = height
        pick_ref[8 + p : 9 + p, :] = level
    high, low = split(pick_ref[...])
    gather = partial(
        lax.dot_general,
        dimension_numbers=(((1,), (1,)), ((), ())),
        preferred_element_type=jnp.float32,
    )
    picked = (gather(high, blocks) + gather(low, blocks)) * inverse
    heights, values = picked[0:8], picked[8:16]
    heights_ref[...] = heights
    inverse_ref[...] = jnp.broadcast_to(inverse, (8, LANES))
    weight = jax.nn.sigmoid(heights * 20.0)
    lane = iota((1, LANES), 1)
    counts = jnp.zeros((1, LANES), jnp.float32)
    for k in range(16):
        level = 0.25 * bins_ref[0, k].astype(jnp.float32)
        above = weight * jax.nn.sigmoid((values - level) * 10.0)
        summed = jnp.sum(jnp.sum(above, axis=0, keepdims=True), axis=1, keepdims=True)
        counts = counts + jnp.where(lane == k, summed, 0.0)
    for s in range(DEV):
        counts_ref[s] = jnp.broadcast_to(counts, (8, LANES))


def peak_pass(thresholds, x, table, offsets):
    f32 = jnp.float32
    out = [
        jax.ShapeDtypeStruct((ROWS, N), f32),
        jax.ShapeDtypeStruct((8, LANES), f32),
        jax.ShapeDtypeStruct((DEV, 8, LANES), f32),
        jax.ShapeDtypeStruct((8, LANES), f32),
    ]
    scratch = [
        pltpu.VMEM((ROWS + 16, N), f32),
        pltpu.VMEM((ROWS + 16, N), f32),
        pltpu.VMEM((16, N), f32),
    ]
    specs = [pl.BlockSpec(memory_space=pltpu.SMEM)] + [pl.BlockSpec(memory_space=pltpu.VMEM)] * 8
    run = call(peaks_kernel, out, scratch, 28, 2 * 10**9, specs)
    return run(thresholds, x, *table, offsets)


def body(shear, smoothing, offsets, thresholds):
    group = ("row", "col")
    device = lax.axis_index(group).astype(jnp.int32).reshape(1)
    sample, frequency, factors = tables(smoothing, device)
    x = shear.reshape(2, 4, ROWS, INNER).transpose(1, 0, 2, 3)
    x = lax.all_to_all(x, "col", split_axis=0, concat_axis=0, tiled=True)
    g = columns(x, sample)
    g = lax.all_to_all(g, group, split_axis=0, concat_axis=0, tiled=True)
    k = row_pass(device, g, sample, frequency, factors)
    k = lax.all_to_all(k, group, split_axis=0, concat_axis=0, tiled=True)
    kappa, heights, counts, inverse = peak_pass(thresholds, k, frequency, offsets[0])
    counts = lax.all_to_all(counts, group, split_axis=0, concat_axis=0, tiled=True)
    snr = kappa * inverse[0:1, 0:1]
    return snr[None], heights[None], jnp.sum(counts[:, 0:1, 0:16], axis=0)


def solution(mesh):
    return jax.shard_map(
        body,
        mesh=mesh,
        in_specs=(
            P(None, "maps", "row", "col"),
            P("maps"),
            P("maps", ("row", "col"), None),
            P("maps", None),
        ),
        out_specs=(
            P("maps", ("row", "col"), None),
            P("maps", ("row", "col"), None),
            P("maps", None),
        ),
        check_vma=False,
    )
```

```python
from functools import partial
import math

import jax
import jax.numpy as jnp
from jax import lax
from jax.experimental import pallas as pl
from jax.experimental.pallas import tpu as pltpu
from jax.sharding import PartitionSpec as P


N = 2048
INNER = 512
DEV = 16
ROWS = 128
LANES = 128
HALF = 64
CELL = 16
BLOCK = ROWS + 8
CLASSES = ((0, 0, 4), (2, 4, 4), (1, 8, 8))
MIB = 1 << 20
LIMIT = (20, 24, 24, 36, 28)


def call(kernel, out, scratch, limit, flops, ins):
    return pl.pallas_call(
        kernel,
        out_shape=out,
        in_specs=ins,
        scratch_shapes=scratch,
        compiler_params=pltpu.CompilerParams(vmem_limit_bytes=limit * MIB),
        cost_estimate=pl.CostEstimate(flops=flops, bytes_accessed=4 * MIB, transcendentals=0),
    )


def split(x):
    high = x.astype(jnp.bfloat16)
    return high, (x - high.astype(jnp.float32)).astype(jnp.bfloat16)


def dot(left, right):
    return jnp.dot(left, right, preferred_element_type=jnp.float32)


def from_left(high_ref, low_ref, x):
    high, low = split(x)
    width = x.shape[1]
    both = dot(high_ref[...], jnp.concatenate([high, low], axis=1))
    return both[:, :width] + (both[:, width:] + dot(low_ref[...], high))


def from_right(x, high_ref, low_ref):
    high, low = split(x)
    height = x.shape[0]
    both = dot(jnp.concatenate([high, low], axis=0), high_ref[...])
    return both[:height] + (both[height:] + dot(high, low_ref[...]))


def angle(steps):
    wrapped = jnp.bitwise_and(steps, N - 1)
    wrapped = jnp.where(wrapped >= N // 2, wrapped - N, wrapped)
    return wrapped.astype(jnp.float32) * (2.0 * math.pi / N)


def iota(shape, dim):
    return lax.broadcasted_iota(jnp.int32, shape, dim)


def put(high_ref, low_ref, rows, cols, value):
    high, low = split(value)
    high_ref[rows, cols] = high
    low_ref[rows, cols] = low


def sample_form(refs, scratch):
    cos_ref, sin_ref = scratch
    for (start, _, blocks), (high_ref, low_ref) in zip(CLASSES, refs):
        width = LANES * blocks
        col = iota((HALF, width), 1)
        freq = start + 4 * (HALF * (col // LANES) + col % HALF)
        quarter = jnp.where(col % LANES >= HALF, 1, 0)
        if start == 0:
            freq = jnp.where(col == HALF, N // 2, freq)
            quarter = jnp.where(col == HALF, 0, quarter)
        fine = angle(freq * iota((HALF, width), 0))
        cos_ref[:, :width] = jnp.cos(fine)
        sin_ref[:, :width] = jnp.sin(fine)
        coarse = angle(freq[:8] * (HALF * iota((8, width), 0)) + INNER * quarter[:8])
        cos_high, sin_high = jnp.cos(coarse), jnp.sin(coarse)
        for part in range(INNER // HALF):
            cos_part, sin_part = cos_high[part : part + 1], sin_high[part : part + 1]
            rows = pl.ds(HALF * part, HALF)
            cos_fine, sin_fine = cos_ref[:, :width], sin_ref[:, :width]
            put(high_ref, low_ref, rows, slice(None), cos_part * cos_fine - sin_part * sin_fine)
            if start == 1:
                rows = pl.ds(INNER + HALF * part, HALF)
                value = -(sin_part * cos_fine + cos_part * sin_fine)
                put(high_ref, low_ref, rows, slice(None), value)


def frequency_form(refs, scratch):
    cos_ref, sin_ref = scratch
    fine = angle(4 * iota((HALF, INNER), 0) * iota((HALF, INNER), 1))
    cos_ref[:, :INNER] = jnp.cos(fine)
    sin_ref[:, :INNER] = jnp.sin(fine)
    for (start, _, blocks), (high_ref, low_ref) in zip(CLASSES, refs):
        coarse = angle((start + 4 * HALF * iota((8, INNER), 0)) * iota((8, INNER), 1))
        cos_high, sin_high = jnp.cos(coarse), jnp.sin(coarse)
        for part in range(blocks):
            cos_part, sin_part = cos_high[part : part + 1], sin_high[part : part + 1]
            cos_fine, sin_fine = cos_ref[:, :INNER], sin_ref[:, :INNER]
            cosine = cos_part * cos_fine - sin_part * sin_fine
            sine = -(sin_part * cos_fine + cos_part * sin_fine)
            if start == 0 and part == 0:
                flip = (1 - 2 * (iota((HALF, INNER), 1) & 1)).astype(jnp.float32)
                sine = jnp.where(iota((HALF, INNER), 0) == 0, flip, sine)
            upper, lower = pl.ds(LANES * part, HALF), pl.ds(LANES * part + HALF, HALF)
            put(high_ref, low_ref, upper, pl.ds(0, INNER), cosine)
            put(high_ref, low_ref, lower, pl.ds(0, INNER), sine)
            if start == 1:
                put(high_ref, low_ref, upper, pl.ds(INNER, INNER), sine)
                put(high_ref, low_ref, lower, pl.ds(INNER, INNER), -cosine)


def signed(freq):
    return jnp.where(freq < N // 2, freq, freq - N)


def lane_frequency(device, shape):
    lane = iota(shape, 1)
    block = jnp.where(device < 8, device % 4, device - 8)
    start = jnp.where(device < 4, 0, jnp.where(device < 8, 2, 1))
    freq = signed(start + 4 * (HALF * block + lane % HALF))
    nyquist = (device == 0) & (lane == HALF)
    freq = jnp.where(nyquist, -(N // 2), freq)
    single = nyquist | ((device == 0) & (lane == 0))
    return freq.astype(jnp.float32), jnp.where(single, 1.0, 2.0)


def tables_kernel(smooth_ref, device_ref, *refs):
    device = device_ref[0]
    scratch = refs[-2:]
    w_refs = tuple(zip(refs[0:6:2], refs[1:6:2]))
    f_refs = tuple(zip(refs[6:12:2], refs[7:12:2]))
    even_ref, odd_ref, last_ref = refs[12:15]
    sample_form(w_refs, scratch)
    frequency_form(f_refs, scratch)
    width = smooth_ref[0]
    decay = width * width * (-2.0 * math.pi**2 / (N * N))
    shape = (HALF, LANES)
    freq_y, weight = lane_frequency(device, shape)

    def factors(freq_x, weight):
        total = freq_x * freq_x + freq_y * freq_y
        scaled = jnp.exp(decay * total) * weight / jnp.maximum(total, 1.0)
        return (freq_x * freq_x - freq_y * freq_y) * scaled, 2.0 * freq_x * freq_y * scaled

    for start, first, blocks in CLASSES:
        for part in range(blocks):
            freq = signed(start + 4 * (HALF * part + iota(shape, 0)))
            row_weight = jnp.where(freq == 0, 1.0, 2.0) * (1.0 / (N * N))
            even, odd = factors(freq.astype(jnp.float32), weight * row_weight)
            rows = pl.ds(HALF * (first + part), HALF)
            even_ref[rows, :] = even
            odd_ref[rows, :] = odd
    even, odd = factors(jnp.full(shape, -N / 2, jnp.float32), weight * (1.0 / (N * N)))
    last_ref[0:8, :] = even[0:8]
    last_ref[8:16, :] = odd[0:8]


def tables(smoothing, device):
    low = jnp.bfloat16
    pairs = []
    for _ in range(2):
        for size in (INNER, INNER, 2 * INNER):
            pairs += [jax.ShapeDtypeStruct((size, size), low)] * 2
    out = pairs + [
        jax.ShapeDtypeStruct((N // 2, LANES), jnp.float32),
        jax.ShapeDtypeStruct((N // 2, LANES), jnp.float32),
        jax.ShapeDtypeStruct((16, LANES), jnp.float32),
    ]
    scratch = [pltpu.VMEM((HALF, 2 * INNER), jnp.float32)] * 2
    smem = pl.BlockSpec(memory_space=pltpu.SMEM)
    result = call(tables_kernel, out, scratch, LIMIT[0], 10**9, [smem, smem])(smoothing, device)
    return result[0:6], result[6:12], result[12:15]


def quarters(blocks):
    first, second, third, fourth = blocks
    return (
        (first + third) + (second + fourth),
        (first + third) - (second + fourth),
        first - third,
        second - fourth,
    )


def pack_kernel(place_ref, x_ref, *outs):
    for index in range(8):
        start = pl.multiple_of(((place_ref[0] + index) & 3) * ROWS, ROWS)
        outs[index][...] = x_ref[index // 4, 0, pl.ds(start, ROWS), :]


def pack(place, shear):
    out = [jax.ShapeDtypeStruct((ROWS, INNER), jnp.float32)] * 8
    specs = [pl.BlockSpec(memory_space=pltpu.SMEM), pl.BlockSpec(memory_space=pltpu.VMEM)]
    return call(pack_kernel, out, (), LIMIT[1], 10**6, specs)(place, shear)


def columns_kernel(field, place_ref, *refs):
    blocks, table, out_ref = refs[:4], refs[4:10], refs[-1]
    zero, two, even, odd = quarters([x[...] for x in blocks])
    place = place_ref[0]
    along = jnp.where(place == 0, 1.0, jnp.where(place == 2, -1.0, 0.0))
    across = jnp.where(place == 1, 1.0, jnp.where(place == 3, -1.0, 0.0))
    flip = jnp.where((place & 1) == 0, 1.0, -1.0)
    rows = pl.ds(ROWS * field, ROWS)
    other = pl.ds(ROWS - ROWS * field, ROWS)
    for part in range(DEV):
        out_ref[part, other, :] = refs[10][part, other, :] if field else jnp.zeros((ROWS, LANES), jnp.float32)

    def emit(value, first):
        for part in range(value.shape[1] // LANES):
            out_ref[first + part, rows, :] = value[:, LANES * part : LANES * (part + 1)]

    emit(from_right(zero, *table[0:2]), 0)
    emit(from_right(flip * two, *table[2:4]), 4)
    both = jnp.concatenate([along * even - across * odd, across * even + along * odd], axis=1)
    emit(from_right(both, *table[4:6]), 8)


def columns(field, place, blocks, table, *before):
    out = jax.ShapeDtypeStruct((DEV, 2 * ROWS, LANES), jnp.float32)
    specs = [pl.BlockSpec(memory_space=pltpu.SMEM)] + [pl.BlockSpec(memory_space=pltpu.VMEM)] * 10
    specs += [pl.BlockSpec(memory_space=pltpu.VMEM)] * len(before)
    kernel = partial(columns_kernel, field)
    run = call(kernel, out, (), LIMIT[1], 2 * 10**9, specs)
    return run(place, *blocks, *table, *before)


def rows_kernel(device_ref, g_ref, *refs):
    w0h, w0l, w2h, w2l, w1h, w1l, f0h, f0l, f2h, f2l, f1h, f1l = refs[:12]
    even_ref, odd_ref, last_ref, out_ref, spec_ref, data_ref = refs[12:]
    device = device_ref[0]

    def rows_of(r):
        wide = []
        for s in range(4 * r, 4 * r + 4):
            block = g_ref[s]
            wide.append(jnp.concatenate([block[:ROWS], block[ROWS:]], axis=1))
        return jnp.concatenate(wide, axis=0)

    zero, two, even, odd = quarters([rows_of(r) for r in range(4)])
    spec_ref[0:INNER, :] = from_left(f0h, f0l, zero)
    spec_ref[INNER : 2 * INNER, :] = from_left(f2h, f2l, two)
    both = jnp.concatenate([even, odd], axis=0)
    spec_ref[2 * INNER : 4 * INNER, :] = from_left(f1h, f1l, both)
    _, weight = lane_frequency(device, (8, LANES))
    total = jnp.zeros((HALF, LANES), jnp.float32)
    special = jnp.zeros((8, LANES), jnp.float32)
    row, lane = iota((HALF, LANES), 0), iota((HALF, LANES), 1)
    sign = jnp.where(lane < HALF, 1.0, -1.0)
    fix = (lane == HALF) & (device == 0)
    for part in range(DEV):
        upper, lower = pl.ds(LANES * part, HALF), pl.ds(LANES * part + HALF, HALF)
        x_one, x_two = spec_ref[upper, 0:LANES], spec_ref[upper, LANES : 2 * LANES]
        y_one, y_two = spec_ref[lower, 0:LANES], spec_ref[lower, LANES : 2 * LANES]
        x_two = jnp.where(fix, -x_one, sign * pltpu.roll(x_two, HALF, 1))
        y_two = jnp.where(fix, -y_one, sign * pltpu.roll(y_two, HALF, 1))
        rows = pl.ds(HALF * part, HALF)
        even, odd = even_ref[rows, :], odd_ref[rows, :]
        cosine = even * x_one - odd * y_two
        sine = even * y_one + odd * x_two
        if part == 0:
            edge, other = y_one[0:8], y_two[0:8]
            turned = sign[0:8] * pltpu.roll(edge, HALF, 1)
            turned = jnp.where(fix[0:8], pltpu.roll(other, HALF, 1), turned)
            edge = last_ref[0:8, :] * edge + last_ref[8:16, :] * turned
            edge = jnp.concatenate([edge] * 8, axis=0)
            cosine = jnp.where(row == 0, even * x_one, cosine)
            sine = jnp.where(row == 0, edge, sine)
            special = (cosine * cosine + sine * sine)[0:8]
        total = total + (cosine * cosine + sine * sine)
        data_ref[upper, :] = cosine
        data_ref[lower, :] = sine
    special = jnp.where(iota((8, LANES), 0) == 0, special, 0.0)
    energy = jnp.sum(total, axis=0, keepdims=True) + jnp.sum(special, axis=0, keepdims=True)
    energy = 0.5 * energy / weight[0:1]

    zero = from_left(w0h, w0l, data_ref[0:INNER, :])
    two = from_left(w2h, w2l, data_ref[INNER : 2 * INNER, :])
    odd = from_left(w1h, w1l, data_ref[2 * INNER : 4 * INNER, :])
    plus, minus = zero + two, zero - two
    real, turned = odd[0:INNER], odd[INNER : 2 * INNER]
    for r, value in enumerate((plus + real, minus + turned, plus - real, minus - turned)):
        for part in range(4):
            out_ref[4 * r + part, 0:ROWS, :] = value[ROWS * part : ROWS * (part + 1)]
    for s in range(DEV):
        out_ref[s, ROWS : ROWS + 1, :] = out_ref[(s - 1) % DEV, ROWS - 1 : ROWS, :]
        out_ref[s, ROWS + 1 : ROWS + 2, :] = out_ref[(s + 1) % DEV, 0:1, :]
        out_ref[s, ROWS + 2 : ROWS + 3, :] = energy
        out_ref[s, ROWS + 3 : BLOCK, :] = jnp.zeros((BLOCK - ROWS - 3, LANES), jnp.float32)


def row_pass(device, g, sample, frequency, factors):
    out = jax.ShapeDtypeStruct((DEV, BLOCK, LANES), jnp.float32)
    scratch = [pltpu.VMEM((N, 2 * LANES), jnp.float32), pltpu.VMEM((N, LANES), jnp.float32)]
    specs = [pl.BlockSpec(memory_space=pltpu.SMEM)] + [pl.BlockSpec(memory_space=pltpu.VMEM)] * 16
    run = call(rows_kernel, out, scratch, LIMIT[3], 4 * 10**9, specs)
    return run(device, g, *sample, *frequency, *factors)


def peaks_kernel(bins_ref, x_ref, f0h, f0l, f2h, f2l, f1h, f1l, offsets_ref, *refs):
    snr_ref, heights_ref, counts_ref, field_ref, wide_ref, pick_ref = refs

    def block(first, count):
        body = jnp.concatenate([x_ref[s] for s in range(first, first + count)], axis=1)
        pad = jnp.zeros((8, body.shape[1]), jnp.float32)
        return jnp.concatenate([body, pad], axis=0)

    zero = from_right(block(0, 4), f0h, f0l)
    two = from_right(block(4, 4), f2h, f2l)
    odd = from_right(block(8, 8), f1h, f1l)
    plus, minus = zero + two, zero - two
    real, turned = odd[:, 0:INNER], odd[:, INNER : 2 * INNER]
    energy = x_ref[0, ROWS : BLOCK, :]
    for s in range(1, DEV):
        energy = energy + x_ref[s, ROWS : BLOCK, :]
    mean = jnp.sum(energy[2:3, :], axis=1, keepdims=True)
    inverse = 1.0 / jnp.sqrt(mean + 1e-06)
    for c, value in enumerate((plus + real, minus + turned, plus - real, minus - turned)):
        cols = pl.ds(INNER * c, INNER)
        snr_ref[:, cols] = value[0:ROWS] * inverse
        field_ref[8 : ROWS + 8, cols] = value[0:ROWS]
        field_ref[7:8, cols] = value[ROWS : ROWS + 1]
        field_ref[ROWS + 8 : ROWS + 9, cols] = value[ROWS + 1 : ROWS + 2]
    for start in (0,) + tuple(range(8, ROWS + 8, 16)) + (ROWS + 8,):
        size = 8 if start in (0, ROWS + 8) else 16
        value = field_ref[start : start + size, :]
        side = jnp.maximum(pltpu.roll(value, 1, 1), pltpu.roll(value, N - 1, 1))
        wide_ref[start : start + size, :] = jnp.maximum(side, value)
    blocks = iota((LANES, N), 1) // CELL == iota((LANES, N), 0)
    blocks = jnp.where(blocks, 1.0, 0.0).astype(jnp.bfloat16)
    offsets = offsets_ref[...].astype(jnp.float32).astype(jnp.bfloat16)
    offsets = jnp.concatenate([offsets, offsets], axis=0)
    spread = jnp.dot(offsets, blocks, preferred_element_type=jnp.float32)
    code = (iota((CELL, N), 0) * CELL + (iota((CELL, N), 1) & (CELL - 1))).astype(jnp.float32)
    for p in range(ROWS // CELL):
        base = 8 + CELL * p
        value = field_ref[base : base + CELL, :]
        side = jnp.maximum(pltpu.roll(value, 1, 1), pltpu.roll(value, N - 1, 1))
        above = wide_ref[base - 1 : base - 1 + CELL, :]
        below = wide_ref[base + 1 : base + 1 + CELL, :]
        nearest = jnp.maximum(side, jnp.maximum(above, below))
        chosen = spread[p : p + 1, :] == code
        height = jnp.sum(jnp.where(chosen, value - nearest, 0.0), axis=0, keepdims=True)
        level = jnp.sum(jnp.where(chosen, value, 0.0), axis=0, keepdims=True)
        pick_ref[p : p + 1, :] = height
        pick_ref[8 + p : 9 + p, :] = level
    high, low = split(pick_ref[...])
    gather = partial(
        lax.dot_general,
        dimension_numbers=(((1,), (1,)), ((), ())),
        preferred_element_type=jnp.float32,
    )
    picked = (gather(high, blocks) + gather(low, blocks)) * inverse
    heights, values = picked[0:8], picked[8:16]
    heights_ref[...] = heights
    weight = jax.nn.sigmoid(heights * 20.0)
    lane = iota((1, LANES), 1)
    counts = jnp.zeros((1, LANES), jnp.float32)
    for k in range(16):
        level = 0.25 * bins_ref[0, k].astype(jnp.float32)
        above = weight * jax.nn.sigmoid((values - level) * 10.0)
        summed = jnp.sum(jnp.sum(above, axis=0, keepdims=True), axis=1, keepdims=True)
        counts = counts + jnp.where(lane == k, summed, 0.0)
    for s in range(DEV):
        counts_ref[s] = jnp.broadcast_to(counts, (8, LANES))


def peak_pass(thresholds, x, table, offsets):
    f32 = jnp.float32
    out = [
        jax.ShapeDtypeStruct((ROWS, N), f32),
        jax.ShapeDtypeStruct((8, LANES), f32),
        jax.ShapeDtypeStruct((DEV, 8, LANES), f32),
    ]
    scratch = [
        pltpu.VMEM((ROWS + 16, N), f32),
        pltpu.VMEM((ROWS + 16, N), f32),
        pltpu.VMEM((16, N), f32),
    ]
    specs = [pl.BlockSpec(memory_space=pltpu.SMEM)] + [pl.BlockSpec(memory_space=pltpu.VMEM)] * 8
    run = call(peaks_kernel, out, scratch, LIMIT[4], 2 * 10**9, specs)
    return run(thresholds, x, *table, offsets)


def body(shear, smoothing, offsets, thresholds):
    group = ("row", "col")
    device = lax.axis_index(group).astype(jnp.int32).reshape(1)
    place = lax.axis_index("col").astype(jnp.int32).reshape(1)

    def exchange(x):
        return lax.all_to_all(x, group, split_axis=0, concat_axis=0, tiled=True)

    blocks = pack(place, shear)
    fields = []
    for field in range(2):
        got = [blocks[4 * field], None, None, None]
        for step in (2, 1, 3):
            pairs = [(c, (c + step) % 4) for c in range(4)]
            got[4 - step] = lax.ppermute(blocks[4 * field + step], "col", pairs)
        fields.append(got)
    sample, frequency, factors = tables(smoothing, device)
    g = columns(0, place, fields[0], sample)
    g = columns(1, place, fields[1], sample, g)
    k = row_pass(device, exchange(g), sample, frequency, factors)
    out = peak_pass(thresholds, exchange(k), frequency, offsets[0])
    snr, heights, counts = out
    counts = exchange(counts)
    return snr[None], heights[None], jnp.sum(counts[:, 0:1, 0:16], axis=0)


def solution(mesh):
    return jax.shard_map(
        body,
        mesh=mesh,
        in_specs=(
            P(None, "maps", "row", "col"),
            P("maps"),
            P("maps", ("row", "col"), None),
            P("maps", None),
        ),
        out_specs=(
            P("maps", ("row", "col"), None),
            P("maps", ("row", "col"), None),
            P("maps", None),
        ),
        check_vma=False,
    )
```

```python
from functools import partial
import math

import jax
import jax.numpy as jnp
from jax import lax
from jax.experimental import pallas as pl
from jax.experimental.pallas import tpu as pltpu
from jax.sharding import PartitionSpec as P


N = 2048
INNER = 512
DEV = 16
ROWS = 128
LANES = 128
HALF = 64
CELL = 16
BLOCK = ROWS + 8
CLASSES = ((0, 0, 4), (2, 4, 4), (1, 8, 8))
MIB = 1 << 20
LIMIT = (20, 24, 24, 36, 28)
ORDER = (6, 2, 5, 7, 1, 3, 4)


def call(kernel, out, scratch, limit, flops, ins):
    return pl.pallas_call(
        kernel,
        out_shape=out,
        in_specs=ins,
        scratch_shapes=scratch,
        compiler_params=pltpu.CompilerParams(vmem_limit_bytes=limit * MIB),
        cost_estimate=pl.CostEstimate(flops=flops, bytes_accessed=4 * MIB, transcendentals=0),
    )


def split(x):
    high = x.astype(jnp.bfloat16)
    return high, (x - high.astype(jnp.float32)).astype(jnp.bfloat16)


def dot(left, right):
    return jnp.dot(left, right, preferred_element_type=jnp.float32)


def from_left(high_ref, low_ref, x):
    high, low = split(x)
    width = x.shape[1]
    both = dot(high_ref[...], jnp.concatenate([high, low], axis=1))
    return both[:, :width] + (both[:, width:] + dot(low_ref[...], high))


def from_right(x, high_ref, low_ref):
    high, low = split(x)
    height = x.shape[0]
    both = dot(jnp.concatenate([high, low], axis=0), high_ref[...])
    return both[:height] + (both[height:] + dot(high, low_ref[...]))


def angle(steps):
    wrapped = jnp.bitwise_and(steps, N - 1)
    wrapped = jnp.where(wrapped >= N // 2, wrapped - N, wrapped)
    return wrapped.astype(jnp.float32) * (2.0 * math.pi / N)


def iota(shape, dim):
    return lax.broadcasted_iota(jnp.int32, shape, dim)


def put(high_ref, low_ref, rows, cols, value):
    high, low = split(value)
    high_ref[rows, cols] = high
    low_ref[rows, cols] = low


def sample_form(refs, scratch):
    cos_ref, sin_ref = scratch
    for (start, _, blocks), (high_ref, low_ref) in zip(CLASSES, refs):
        width = LANES * blocks
        col = iota((HALF, width), 1)
        freq = start + 4 * (HALF * (col // LANES) + col % HALF)
        quarter = jnp.where(col % LANES >= HALF, 1, 0)
        if start == 0:
            freq = jnp.where(col == HALF, N // 2, freq)
            quarter = jnp.where(col == HALF, 0, quarter)
        fine = angle(freq * iota((HALF, width), 0))
        cos_ref[:, :width] = jnp.cos(fine)
        sin_ref[:, :width] = jnp.sin(fine)
        coarse = angle(freq[:8] * (HALF * iota((8, width), 0)) + INNER * quarter[:8])
        cos_high, sin_high = jnp.cos(coarse), jnp.sin(coarse)
        for part in range(INNER // HALF):
            cos_part, sin_part = cos_high[part : part + 1], sin_high[part : part + 1]
            rows = pl.ds(HALF * part, HALF)
            cos_fine, sin_fine = cos_ref[:, :width], sin_ref[:, :width]
            put(high_ref, low_ref, rows, slice(None), cos_part * cos_fine - sin_part * sin_fine)
            if start == 1:
                rows = pl.ds(INNER + HALF * part, HALF)
                value = -(sin_part * cos_fine + cos_part * sin_fine)
                put(high_ref, low_ref, rows, slice(None), value)


def frequency_form(refs, scratch):
    cos_ref, sin_ref = scratch
    fine = angle(4 * iota((HALF, INNER), 0) * iota((HALF, INNER), 1))
    cos_ref[:, :INNER] = jnp.cos(fine)
    sin_ref[:, :INNER] = jnp.sin(fine)
    for (start, _, blocks), (high_ref, low_ref) in zip(CLASSES, refs):
        coarse = angle((start + 4 * HALF * iota((8, INNER), 0)) * iota((8, INNER), 1))
        cos_high, sin_high = jnp.cos(coarse), jnp.sin(coarse)
        for part in range(blocks):
            cos_part, sin_part = cos_high[part : part + 1], sin_high[part : part + 1]
            cos_fine, sin_fine = cos_ref[:, :INNER], sin_ref[:, :INNER]
            cosine = cos_part * cos_fine - sin_part * sin_fine
            sine = -(sin_part * cos_fine + cos_part * sin_fine)
            if start == 0 and part == 0:
                flip = (1 - 2 * (iota((HALF, INNER), 1) & 1)).astype(jnp.float32)
                sine = jnp.where(iota((HALF, INNER), 0) == 0, flip, sine)
            upper, lower = pl.ds(LANES * part, HALF), pl.ds(LANES * part + HALF, HALF)
            put(high_ref, low_ref, upper, pl.ds(0, INNER), cosine)
            put(high_ref, low_ref, lower, pl.ds(0, INNER), sine)
            if start == 1:
                put(high_ref, low_ref, upper, pl.ds(INNER, INNER), sine)
                put(high_ref, low_ref, lower, pl.ds(INNER, INNER), -cosine)


def signed(freq):
    return jnp.where(freq < N // 2, freq, freq - N)


def lane_frequency(device, shape):
    lane = iota(shape, 1)
    block = jnp.where(device < 8, device % 4, device - 8)
    start = jnp.where(device < 4, 0, jnp.where(device < 8, 2, 1))
    freq = signed(start + 4 * (HALF * block + lane % HALF))
    nyquist = (device == 0) & (lane == HALF)
    freq = jnp.where(nyquist, -(N // 2), freq)
    single = nyquist | ((device == 0) & (lane == 0))
    return freq.astype(jnp.float32), jnp.where(single, 1.0, 2.0)


def tables_kernel(smooth_ref, device_ref, *refs):
    device = device_ref[0]
    scratch = refs[-2:]
    w_refs = tuple(zip(refs[0:6:2], refs[1:6:2]))
    f_refs = tuple(zip(refs[6:12:2], refs[7:12:2]))
    even_ref, odd_ref, last_ref = refs[12:15]
    sample_form(w_refs, scratch)
    frequency_form(f_refs, scratch)
    width = smooth_ref[0]
    decay = width * width * (-2.0 * math.pi**2 / (N * N))
    shape = (HALF, LANES)
    freq_y, weight = lane_frequency(device, shape)

    def factors(freq_x, weight):
        total = freq_x * freq_x + freq_y * freq_y
        scaled = jnp.exp(decay * total) * weight / jnp.maximum(total, 1.0)
        return (freq_x * freq_x - freq_y * freq_y) * scaled, 2.0 * freq_x * freq_y * scaled

    for start, first, blocks in CLASSES:
        for part in range(blocks):
            freq = signed(start + 4 * (HALF * part + iota(shape, 0)))
            row_weight = jnp.where(freq == 0, 1.0, 2.0) * (1.0 / (N * N))
            even, odd = factors(freq.astype(jnp.float32), weight * row_weight)
            rows = pl.ds(HALF * (first + part), HALF)
            even_ref[rows, :] = even
            odd_ref[rows, :] = odd
    even, odd = factors(jnp.full(shape, -N / 2, jnp.float32), weight * (1.0 / (N * N)))
    last_ref[0:8, :] = even[0:8]
    last_ref[8:16, :] = odd[0:8]


def tables(smoothing, device):
    low = jnp.bfloat16
    pairs = []
    for _ in range(2):
        for size in (INNER, INNER, 2 * INNER):
            pairs += [jax.ShapeDtypeStruct((size, size), low)] * 2
    out = pairs + [
        jax.ShapeDtypeStruct((N // 2, LANES), jnp.float32),
        jax.ShapeDtypeStruct((N // 2, LANES), jnp.float32),
        jax.ShapeDtypeStruct((16, LANES), jnp.float32),
    ]
    scratch = [pltpu.VMEM((HALF, 2 * INNER), jnp.float32)] * 2
    smem = pl.BlockSpec(memory_space=pltpu.SMEM)
    result = call(tables_kernel, out, scratch, LIMIT[0], 10**9, [smem, smem])(smoothing, device)
    return result[0:6], result[6:12], result[12:15]


def quarters(blocks):
    first, second, third, fourth = blocks
    return (
        (first + third) + (second + fourth),
        (first + third) - (second + fourth),
        first - third,
        second - fourth,
    )


def pack_kernel(device_ref, x_ref, *outs):
    for index in range(8):
        start = pl.multiple_of(((device_ref[0] + index) & 3) * ROWS, ROWS)
        outs[index][...] = x_ref[index // 4, 0, pl.ds(start, ROWS), :]


def pack(device, shear):
    out = [jax.ShapeDtypeStruct((ROWS, INNER), jnp.float32)] * 8
    specs = [pl.BlockSpec(memory_space=pltpu.SMEM), pl.BlockSpec(memory_space=pltpu.VMEM)]
    return call(pack_kernel, out, (), LIMIT[1], 10**6, specs)(device, shear)


def columns_kernel(device_ref, *refs):
    blocks, table = refs[:4], refs[4:10]
    keep_ref, send_ref, all_ref = refs[10:]
    zero, two, even, odd = quarters([x[...] for x in blocks])
    device = device_ref[0]
    place = device & 3
    along = jnp.where(place == 0, 1.0, jnp.where(place == 2, -1.0, 0.0))
    across = jnp.where(place == 1, 1.0, jnp.where(place == 3, -1.0, 0.0))
    flip = jnp.where((place & 1) == 0, 1.0, -1.0)

    def emit(value, first):
        for part in range(value.shape[1] // LANES):
            all_ref[first + part] = value[:, LANES * part : LANES * (part + 1)]

    emit(from_right(zero, *table[0:2]), 0)
    emit(from_right(flip * two, *table[2:4]), 4)
    both = jnp.concatenate([along * even - across * odd, across * even + along * odd], axis=1)
    emit(from_right(both, *table[4:6]), 8)
    for index in range(8):
        there = other_chip(device, index)
        keep_ref[index] = all_ref[there]
        send_ref[index] = all_ref[there ^ 4]


def other_chip(device, index):
    return ((device & 12) ^ (2 * (index & 4))) + ((device + index) & 3)


def columns(device, blocks, table):
    out = [jax.ShapeDtypeStruct((8, ROWS, LANES), jnp.float32)] * 2
    specs = [pl.BlockSpec(memory_space=pltpu.SMEM)] + [pl.BlockSpec(memory_space=pltpu.VMEM)] * 10
    scratch = [pltpu.VMEM((DEV, ROWS, LANES), jnp.float32)]
    return call(columns_kernel, out, scratch, LIMIT[1], 2 * 10**9, specs)(device, *blocks, *table)


def merge_kernel(keep_ref, got_ref, *outs):
    for index in range(8):
        outs[index][0] = keep_ref[index]
        outs[index][1] = got_ref[index]


def merge(keep, got):
    out = [jax.ShapeDtypeStruct((2,) + keep.shape[1:], jnp.float32)] * 8
    specs = [pl.BlockSpec(memory_space=pltpu.VMEM)] * 2
    return call(merge_kernel, out, (), 8, 10**8, specs)(keep, got)


def to_frequency(device, g_refs, f_refs, part_ref, out_ref):
    f0h, f0l, f2h, f2l, f1h, f1l = f_refs
    flip_core = jnp.where((device & 4) == 0, 1.0, -1.0)
    flip_chip = jnp.where((device & 8) == 0, 1.0, -1.0)
    for step in range(4):
        near, far = g_refs[step], g_refs[4 + step]
        same, other = near[0] + far[0], near[1] + far[1]
        rows = pl.ds(pl.multiple_of(((device - step) & 3) * ROWS, ROWS), ROWS)
        part_ref[0, rows, :] = same + other
        part_ref[1, rows, :] = flip_core * (same - other)
        same, other = flip_chip * (near[0] - far[0]), flip_chip * (near[1] - far[1])
        part_ref[2, rows, :] = jnp.where(flip_core > 0, same, other)
        part_ref[3, rows, :] = jnp.where(flip_core > 0, other, same)
    out_ref[0:INNER, :] = from_left(f0h, f0l, part_ref[0])
    out_ref[INNER : 2 * INNER, :] = from_left(f2h, f2l, part_ref[1])
    both = jnp.concatenate([part_ref[2], part_ref[3]], axis=0)
    out_ref[2 * INNER : 4 * INNER, :] = from_left(f1h, f1l, both)


def first_kernel(device_ref, *refs):
    to_frequency(device_ref[0], refs[:8], refs[8:14], refs[15], refs[14])


def first_pass(device, g, frequency):
    out = jax.ShapeDtypeStruct((N, LANES), jnp.float32)
    specs = [pl.BlockSpec(memory_space=pltpu.SMEM)] + [pl.BlockSpec(memory_space=pltpu.VMEM)] * 14
    scratch = [pltpu.VMEM((4, INNER, LANES), jnp.float32)]
    return call(first_kernel, out, scratch, LIMIT[2], 10**9, specs)(device, *g, *frequency)


def rows_kernel(device_ref, one_ref, *refs):
    g_refs, refs = refs[:8], refs[8:]
    w0h, w0l, w2h, w2l, w1h, w1l = refs[:6]
    even_ref, odd_ref, last_ref, out_ref, part_ref, two_ref, data_ref = refs[12:]
    device = device_ref[0]
    to_frequency(device, g_refs, refs[6:12], part_ref, two_ref)
    _, weight = lane_frequency(device, (8, LANES))
    total = jnp.zeros((HALF, LANES), jnp.float32)
    special = jnp.zeros((8, LANES), jnp.float32)
    row, lane = iota((HALF, LANES), 0), iota((HALF, LANES), 1)
    sign = jnp.where(lane < HALF, 1.0, -1.0)
    fix = (lane == HALF) & (device == 0)
    for part in range(DEV):
        upper, lower = pl.ds(LANES * part, HALF), pl.ds(LANES * part + HALF, HALF)
        x_one, x_two = one_ref[upper, :], two_ref[upper, :]
        y_one, y_two = one_ref[lower, :], two_ref[lower, :]
        x_two = jnp.where(fix, -x_one, sign * pltpu.roll(x_two, HALF, 1))
        y_two = jnp.where(fix, -y_one, sign * pltpu.roll(y_two, HALF, 1))
        rows = pl.ds(HALF * part, HALF)
        even, odd = even_ref[rows, :], odd_ref[rows, :]
        cosine = even * x_one - odd * y_two
        sine = even * y_one + odd * x_two
        if part == 0:
            edge, other = y_one[0:8], y_two[0:8]
            turned = sign[0:8] * pltpu.roll(edge, HALF, 1)
            turned = jnp.where(fix[0:8], pltpu.roll(other, HALF, 1), turned)
            edge = last_ref[0:8, :] * edge + last_ref[8:16, :] * turned
            edge = jnp.concatenate([edge] * 8, axis=0)
            cosine = jnp.where(row == 0, even * x_one, cosine)
            sine = jnp.where(row == 0, edge, sine)
            special = (cosine * cosine + sine * sine)[0:8]
        total = total + (cosine * cosine + sine * sine)
        data_ref[upper, :] = cosine
        data_ref[lower, :] = sine
    special = jnp.where(iota((8, LANES), 0) == 0, special, 0.0)
    energy = jnp.sum(total, axis=0, keepdims=True) + jnp.sum(special, axis=0, keepdims=True)
    energy = 0.5 * energy / weight[0:1]

    zero = from_left(w0h, w0l, data_ref[0:INNER, :])
    two = from_left(w2h, w2l, data_ref[INNER : 2 * INNER, :])
    odd = from_left(w1h, w1l, data_ref[2 * INNER : 4 * INNER, :])
    plus, minus = zero + two, zero - two
    real, turned = odd[0:INNER], odd[INNER : 2 * INNER]
    for r, value in enumerate((plus + real, minus + turned, plus - real, minus - turned)):
        for part in range(4):
            out_ref[4 * r + part, 0:ROWS, :] = value[ROWS * part : ROWS * (part + 1)]
    for s in range(DEV):
        out_ref[s, ROWS : ROWS + 1, :] = out_ref[(s - 1) % DEV, ROWS - 1 : ROWS, :]
        out_ref[s, ROWS + 1 : ROWS + 2, :] = out_ref[(s + 1) % DEV, 0:1, :]
        out_ref[s, ROWS + 2 : ROWS + 3, :] = energy
        out_ref[s, ROWS + 3 : BLOCK, :] = jnp.zeros((BLOCK - ROWS - 3, LANES), jnp.float32)


def row_pass(device, one, g, sample, frequency, factors):
    out = jax.ShapeDtypeStruct((DEV, BLOCK, LANES), jnp.float32)
    scratch = [
        pltpu.VMEM((4, INNER, LANES), jnp.float32),
        pltpu.VMEM((N, LANES), jnp.float32),
        pltpu.VMEM((N, LANES), jnp.float32),
    ]
    specs = [pl.BlockSpec(memory_space=pltpu.SMEM)] + [pl.BlockSpec(memory_space=pltpu.VMEM)] * 24
    run = call(rows_kernel, out, scratch, LIMIT[3], 3 * 10**9, specs)
    return run(device, one, *g, *sample, *frequency, *factors)


def peaks_kernel(bins_ref, x_ref, f0h, f0l, f2h, f2l, f1h, f1l, offsets_ref, *refs):
    snr_ref, heights_ref, counts_ref, field_ref, wide_ref, pick_ref = refs

    def block(first, count):
        body = jnp.concatenate([x_ref[s] for s in range(first, first + count)], axis=1)
        pad = jnp.zeros((8, body.shape[1]), jnp.float32)
        return jnp.concatenate([body, pad], axis=0)

    zero = from_right(block(0, 4), f0h, f0l)
    two = from_right(block(4, 4), f2h, f2l)
    odd = from_right(block(8, 8), f1h, f1l)
    plus, minus = zero + two, zero - two
    real, turned = odd[:, 0:INNER], odd[:, INNER : 2 * INNER]
    energy = x_ref[0, ROWS : BLOCK, :]
    for s in range(1, DEV):
        energy = energy + x_ref[s, ROWS : BLOCK, :]
    mean = jnp.sum(energy[2:3, :], axis=1, keepdims=True)
    inverse = 1.0 / jnp.sqrt(mean + 1e-06)
    for c, value in enumerate((plus + real, minus + turned, plus - real, minus - turned)):
        cols = pl.ds(INNER * c, INNER)
        snr_ref[:, cols] = value[0:ROWS] * inverse
        field_ref[8 : ROWS + 8, cols] = value[0:ROWS]
        field_ref[7:8, cols] = value[ROWS : ROWS + 1]
        field_ref[ROWS + 8 : ROWS + 9, cols] = value[ROWS + 1 : ROWS + 2]
    for start in (0,) + tuple(range(8, ROWS + 8, 16)) + (ROWS + 8,):
        size = 8 if start in (0, ROWS + 8) else 16
        value = field_ref[start : start + size, :]
        side = jnp.maximum(pltpu.roll(value, 1, 1), pltpu.roll(value, N - 1, 1))
        wide_ref[start : start + size, :] = jnp.maximum(side, value)
    blocks = iota((LANES, N), 1) // CELL == iota((LANES, N), 0)
    blocks = jnp.where(blocks, 1.0, 0.0).astype(jnp.bfloat16)
    offsets = offsets_ref[...].astype(jnp.float32).astype(jnp.bfloat16)
    offsets = jnp.concatenate([offsets, offsets], axis=0)
    spread = jnp.dot(offsets, blocks, preferred_element_type=jnp.float32)
    code = (iota((CELL, N), 0) * CELL + (iota((CELL, N), 1) & (CELL - 1))).astype(jnp.float32)
    for p in range(ROWS // CELL):
        base = 8 + CELL * p
        value = field_ref[base : base + CELL, :]
        side = jnp.maximum(pltpu.roll(value, 1, 1), pltpu.roll(value, N - 1, 1))
        above = wide_ref[base - 1 : base - 1 + CELL, :]
        below = wide_ref[base + 1 : base + 1 + CELL, :]
        nearest = jnp.maximum(side, jnp.maximum(above, below))
        chosen = spread[p : p + 1, :] == code
        height = jnp.sum(jnp.where(chosen, value - nearest, 0.0), axis=0, keepdims=True)
        level = jnp.sum(jnp.where(chosen, value, 0.0), axis=0, keepdims=True)
        pick_ref[p : p + 1, :] = height
        pick_ref[8 + p : 9 + p, :] = level
    high, low = split(pick_ref[...])
    gather = partial(
        lax.dot_general,
        dimension_numbers=(((1,), (1,)), ((), ())),
        preferred_element_type=jnp.float32,
    )
    picked = (gather(high, blocks) + gather(low, blocks)) * inverse
    heights, values = picked[0:8], picked[8:16]
    heights_ref[...] = heights
    weight = jax.nn.sigmoid(heights * 20.0)
    lane = iota((1, LANES), 1)
    counts = jnp.zeros((1, LANES), jnp.float32)
    for k in range(16):
        level = 0.25 * bins_ref[0, k].astype(jnp.float32)
        above = weight * jax.nn.sigmoid((values - level) * 10.0)
        summed = jnp.sum(jnp.sum(above, axis=0, keepdims=True), axis=1, keepdims=True)
        counts = counts + jnp.where(lane == k, summed, 0.0)
    for s in range(DEV):
        counts_ref[s] = jnp.broadcast_to(counts, (8, LANES))


def peak_pass(thresholds, x, table, offsets):
    f32 = jnp.float32
    out = [
        jax.ShapeDtypeStruct((ROWS, N), f32),
        jax.ShapeDtypeStruct((8, LANES), f32),
        jax.ShapeDtypeStruct((DEV, 8, LANES), f32),
    ]
    scratch = [
        pltpu.VMEM((ROWS + 16, N), f32),
        pltpu.VMEM((ROWS + 16, N), f32),
        pltpu.VMEM((16, N), f32),
    ]
    specs = [pl.BlockSpec(memory_space=pltpu.SMEM)] + [pl.BlockSpec(memory_space=pltpu.VMEM)] * 8
    run = call(peaks_kernel, out, scratch, LIMIT[4], 2 * 10**9, specs)
    return run(thresholds, x, *table, offsets)


def chip_pairs(index):
    return [(d, (d & 12 ^ (2 * (index & 4))) + ((d + index) & 3)) for d in range(DEV)]


def body(shear, smoothing, offsets, thresholds):
    group = ("row", "col")
    device = lax.axis_index(group).astype(jnp.int32).reshape(1)

    def exchange(x):
        return lax.all_to_all(x, group, split_axis=0, concat_axis=0, tiled=True)

    def scatter(keep, send):
        got = lax.ppermute(send, group, [(d, d ^ 4) for d in range(DEV)])
        blocks = merge(keep, got)
        done = [blocks[0]]
        for index in ORDER:
            done.append((index, lax.ppermute(blocks[index], group, chip_pairs(index))))
        return [blocks[0]] + [value for _, value in sorted(done[1:], key=lambda item: item[0])]

    blocks = pack(device, shear)
    fields = []
    for field in range(2):
        got = [blocks[4 * field], None, None, None]
        for step in (2, 1, 3):
            pairs = [(c, (c + step) % 4) for c in range(4)]
            got[4 - step] = lax.ppermute(blocks[4 * field + step], "col", pairs)
        fields.append(got)
    sample, frequency, factors = tables(smoothing, device)
    g = columns(device, fields[0], sample)
    one = scatter(*g)
    g = columns(device, fields[1], sample)
    two = scatter(*g)
    one = first_pass(device, one, frequency)
    k = row_pass(device, one, two, sample, frequency, factors)
    out = peak_pass(thresholds, exchange(k), frequency, offsets[0])
    snr, heights, counts = out
    counts = exchange(counts)
    return snr[None], heights[None], jnp.sum(counts[:, 0:1, 0:16], axis=0)


def solution(mesh):
    return jax.shard_map(
        body,
        mesh=mesh,
        in_specs=(
            P(None, "maps", "row", "col"),
            P("maps"),
            P("maps", ("row", "col"), None),
            P("maps", None),
        ),
        out_specs=(
            P("maps", ("row", "col"), None),
            P("maps", ("row", "col"), None),
            P("maps", None),
        ),
        check_vma=False,
    )
```

```python
from functools import partial
import math

import jax
import jax.numpy as jnp
from jax import lax
from jax.experimental import pallas as pl
from jax.experimental.pallas import tpu as pltpu
from jax.sharding import PartitionSpec as P


N = 2048
INNER = 512
DENSE = 256
DEV = 16
ROWS = 128
LANES = 128
HALF = 64
CELL = 16
BLOCK = ROWS + 8
CLASSES = ((0, 0, 2), (4, 2, 2), (2, 4, 4), (1, 8, 4), (3, 12, 4))
ROOT = math.sqrt(0.5)
MIB = 1 << 20
LIMIT = (20, 24, 24, 36, 28)
ORDER = (6, 2, 5, 7, 1, 3, 4)


def call(kernel, out, scratch, limit, flops, ins):
    return pl.pallas_call(
        kernel,
        out_shape=out,
        in_specs=ins,
        scratch_shapes=scratch,
        compiler_params=pltpu.CompilerParams(vmem_limit_bytes=limit * MIB),
        cost_estimate=pl.CostEstimate(flops=flops, bytes_accessed=4 * MIB, transcendentals=0),
    )


def split(x):
    high = x.astype(jnp.bfloat16)
    return high, (x - high.astype(jnp.float32)).astype(jnp.bfloat16)


def dot(left, right):
    return jnp.dot(left, right, preferred_element_type=jnp.float32)


def from_left(high_ref, low_ref, x):
    high, low = split(x)
    width = x.shape[1]
    both = dot(high_ref[...], jnp.concatenate([high, low], axis=1))
    return both[:, :width] + (both[:, width:] + dot(low_ref[...], high))


def from_right(x, high_ref, low_ref):
    high, low = split(x)
    height = x.shape[0]
    both = dot(jnp.concatenate([high, low], axis=0), high_ref[...])
    return both[:height] + (both[height:] + dot(high, low_ref[...]))


def pairs(refs):
    return tuple(zip(refs[0::2], refs[1::2]))


def take(x, start, size, axis):
    return lax.slice_in_dim(x, start, start + size, axis=axis)


def front(zero, two, even, odd, axis):
    near = [take(x, 0, DENSE, axis) for x in (zero, two, even, odd)]
    far = [take(x, DENSE, DENSE, axis) for x in (zero, two, even, odd)]
    change, total = ROOT * (far[2] - far[3]), ROOT * (far[2] + far[3])
    join = partial(jnp.concatenate, axis=axis)
    return (
        near[0] + far[0],
        near[0] - far[0],
        join([near[1], -far[1]]),
        join([near[2] + change, -near[3] - total]),
        join([near[2] - change, near[3] - total]),
    )


def back(values, axis):
    first, second, turn, one, three = values
    real = [take(x, 0, DENSE, axis) for x in (turn, one, three)]
    imag = [take(x, DENSE, DENSE, axis) for x in (turn, one, three)]
    change, total = real[1] - real[2], -imag[1] - imag[2]
    halves = (
        (first + second, real[0], real[1] + real[2], imag[2] - imag[1]),
        (first - second, -imag[0], ROOT * (total + change), ROOT * (total - change)),
    )
    blocks = []
    for zero, two, even, odd in halves:
        plus, minus = zero + two, zero - two
        blocks.append((plus + even, minus + odd, plus - even, minus - odd))
    return [jnp.concatenate([near, far], axis=axis) for near, far in zip(*blocks)]


def angle(steps):
    wrapped = jnp.bitwise_and(steps, N - 1)
    wrapped = jnp.where(wrapped >= N // 2, wrapped - N, wrapped)
    return wrapped.astype(jnp.float32) * (2.0 * math.pi / N)


def iota(shape, dim):
    return lax.broadcasted_iota(jnp.int32, shape, dim)


def put(high_ref, low_ref, rows, cols, value):
    high, low = split(value)
    high_ref[rows, cols] = high
    low_ref[rows, cols] = low


def sample_form(refs, scratch):
    cos_ref, sin_ref = scratch
    for (start, _, blocks), (high_ref, low_ref) in zip(CLASSES, refs):
        width = LANES * blocks
        col = iota((HALF, width), 1)
        freq = start + 8 * (HALF * (col // LANES) + col % HALF)
        quarter = jnp.where(col % LANES >= HALF, 1, 0)
        if start == 0:
            freq = jnp.where(col == HALF, N // 2, freq)
            quarter = jnp.where(col == HALF, 0, quarter)
        fine = angle(freq * iota((HALF, width), 0))
        cos_ref[:, :width] = jnp.cos(fine)
        sin_ref[:, :width] = jnp.sin(fine)
        coarse = angle(freq[:8] * (HALF * iota((8, width), 0)) + INNER * quarter[:8])
        cos_high, sin_high = jnp.cos(coarse), jnp.sin(coarse)
        for part in range(DENSE // HALF):
            cos_part, sin_part = cos_high[part : part + 1], sin_high[part : part + 1]
            rows = pl.ds(HALF * part, HALF)
            cos_fine, sin_fine = cos_ref[:, :width], sin_ref[:, :width]
            put(high_ref, low_ref, rows, slice(None), cos_part * cos_fine - sin_part * sin_fine)
            if blocks == 4:
                rows = pl.ds(DENSE + HALF * part, HALF)
                value = sin_part * cos_fine + cos_part * sin_fine
                put(high_ref, low_ref, rows, slice(None), value)


def frequency_form(refs, scratch):
    cos_ref, sin_ref = scratch
    fine = angle(8 * iota((HALF, DENSE), 0) * iota((HALF, DENSE), 1))
    cos_ref[:, :DENSE] = jnp.cos(fine)
    sin_ref[:, :DENSE] = jnp.sin(fine)
    for (start, _, blocks), (high_ref, low_ref) in zip(CLASSES, refs):
        coarse = angle((start + 8 * HALF * iota((8, DENSE), 0)) * iota((8, DENSE), 1))
        cos_high, sin_high = jnp.cos(coarse), jnp.sin(coarse)
        for part in range(blocks):
            cos_part, sin_part = cos_high[part : part + 1], sin_high[part : part + 1]
            cos_fine, sin_fine = cos_ref[:, :DENSE], sin_ref[:, :DENSE]
            cosine = cos_part * cos_fine - sin_part * sin_fine
            sine = sin_part * cos_fine + cos_part * sin_fine
            turned = -sine
            if start == 0 and part == 0:
                flip = (1 - 2 * (iota((HALF, DENSE), 1) & 1)).astype(jnp.float32)
                turned = jnp.where(iota((HALF, DENSE), 0) == 0, flip, turned)
            upper, lower = pl.ds(LANES * part, HALF), pl.ds(LANES * part + HALF, HALF)
            put(high_ref, low_ref, upper, pl.ds(0, DENSE), cosine)
            put(high_ref, low_ref, lower, pl.ds(0, DENSE), turned)
            if blocks == 4:
                put(high_ref, low_ref, upper, pl.ds(DENSE, DENSE), sine)
                put(high_ref, low_ref, lower, pl.ds(DENSE, DENSE), cosine)


def signed(freq):
    return jnp.where(freq < N // 2, freq, freq - N)


def lane_frequency(device, shape):
    lane = iota(shape, 1)
    block = jnp.where(device < 4, device & 1, device & 3)
    start = jnp.where(device < 2, 0, jnp.where(device < 4, 4, 2))
    start = jnp.where(device < 8, start, jnp.where(device < 12, 1, 3))
    freq = signed(start + 8 * (HALF * block + lane % HALF))
    nyquist = (device == 0) & (lane == HALF)
    freq = jnp.where(nyquist, -(N // 2), freq)
    single = nyquist | ((device == 0) & (lane == 0))
    return freq.astype(jnp.float32), jnp.where(single, 1.0, 2.0)


def tables_kernel(smooth_ref, device_ref, *refs):
    device = device_ref[0]
    scratch = refs[-2:]
    w_refs, f_refs = pairs(refs[0:10]), pairs(refs[10:20])
    even_ref, odd_ref, last_ref = refs[20:23]
    sample_form(w_refs, scratch)
    frequency_form(f_refs, scratch)
    width = smooth_ref[0]
    decay = width * width * (-2.0 * math.pi**2 / (N * N))
    shape = (HALF, LANES)
    freq_y, weight = lane_frequency(device, shape)

    def factors(freq_x, weight):
        total = freq_x * freq_x + freq_y * freq_y
        scaled = jnp.exp(decay * total) * weight / jnp.maximum(total, 1.0)
        return (freq_x * freq_x - freq_y * freq_y) * scaled, 2.0 * freq_x * freq_y * scaled

    for start, first, blocks in CLASSES:
        for part in range(blocks):
            freq = signed(start + 8 * (HALF * part + iota(shape, 0)))
            row_weight = jnp.where(freq == 0, 1.0, 2.0) * (1.0 / (N * N))
            even, odd = factors(freq.astype(jnp.float32), weight * row_weight)
            rows = pl.ds(HALF * (first + part), HALF)
            even_ref[rows, :] = even
            odd_ref[rows, :] = odd
    even, odd = factors(jnp.full(shape, -N / 2, jnp.float32), weight * (1.0 / (N * N)))
    last_ref[0:8, :] = even[0:8]
    last_ref[8:16, :] = odd[0:8]


def tables(smoothing, device):
    low = jnp.bfloat16
    table = []
    for _, _, blocks in CLASSES:
        table += [jax.ShapeDtypeStruct((LANES * blocks, LANES * blocks), low)] * 2
    out = table + table + [
        jax.ShapeDtypeStruct((N // 2, LANES), jnp.float32),
        jax.ShapeDtypeStruct((N // 2, LANES), jnp.float32),
        jax.ShapeDtypeStruct((16, LANES), jnp.float32),
    ]
    scratch = [pltpu.VMEM((HALF, INNER), jnp.float32)] * 2
    smem = pl.BlockSpec(memory_space=pltpu.SMEM)
    result = call(tables_kernel, out, scratch, LIMIT[0], 10**9, [smem, smem])(smoothing, device)
    return result[0:10], result[10:20], result[20:23]


def quarters(blocks):
    first, second, third, fourth = blocks
    return (
        (first + third) + (second + fourth),
        (first + third) - (second + fourth),
        first - third,
        second - fourth,
    )


def pack_kernel(device_ref, x_ref, *outs):
    for index in range(8):
        start = pl.multiple_of(((device_ref[0] + index) & 3) * ROWS, ROWS)
        outs[index][...] = x_ref[index // 4, 0, pl.ds(start, ROWS), :]


def pack(device, shear):
    out = [jax.ShapeDtypeStruct((ROWS, INNER), jnp.float32)] * 8
    specs = [pl.BlockSpec(memory_space=pltpu.SMEM), pl.BlockSpec(memory_space=pltpu.VMEM)]
    return call(pack_kernel, out, (), LIMIT[1], 10**6, specs)(device, shear)


def columns_kernel(device_ref, *refs):
    blocks, table = refs[:4], pairs(refs[4:14])
    keep_ref, send_ref, all_ref = refs[14:]
    zero, two, even, odd = quarters([x[...] for x in blocks])
    device = device_ref[0]
    place = device & 3
    along = jnp.where(place == 0, 1.0, jnp.where(place == 2, -1.0, 0.0))
    across = jnp.where(place == 1, 1.0, jnp.where(place == 3, -1.0, 0.0))
    flip = jnp.where((place & 1) == 0, 1.0, -1.0)

    even, odd = along * even - across * odd, across * even + along * odd
    operands = front(zero, flip * two, even, odd, 1)
    for (_, first, count), operand, refs in zip(CLASSES, operands, table):
        value = from_right(operand, *refs)
        for part in range(count):
            all_ref[first + part] = value[:, LANES * part : LANES * (part + 1)]
    for index in range(8):
        there = other_chip(device, index)
        keep_ref[index] = all_ref[there]
        send_ref[index] = all_ref[there ^ 4]


def other_chip(device, index):
    return ((device & 12) ^ (2 * (index & 4))) + ((device + index) & 3)


def columns(device, blocks, table):
    out = [jax.ShapeDtypeStruct((8, ROWS, LANES), jnp.float32)] * 2
    specs = [pl.BlockSpec(memory_space=pltpu.SMEM)] + [pl.BlockSpec(memory_space=pltpu.VMEM)] * 14
    scratch = [pltpu.VMEM((DEV, ROWS, LANES), jnp.float32)]
    return call(columns_kernel, out, scratch, LIMIT[1], 2 * 10**9, specs)(device, *blocks, *table)


def merge_kernel(keep_ref, got_ref, *outs):
    for index in range(8):
        outs[index][0] = keep_ref[index]
        outs[index][1] = got_ref[index]


def merge(keep, got):
    out = [jax.ShapeDtypeStruct((2,) + keep.shape[1:], jnp.float32)] * 8
    specs = [pl.BlockSpec(memory_space=pltpu.VMEM)] * 2
    return call(merge_kernel, out, (), 8, 10**8, specs)(keep, got)


def to_frequency(device, g_refs, f_refs, part_ref, out_ref):
    flip_core = jnp.where((device & 4) == 0, 1.0, -1.0)
    flip_chip = jnp.where((device & 8) == 0, 1.0, -1.0)
    for step in range(4):
        near, far = g_refs[step], g_refs[4 + step]
        same, other = near[0] + far[0], near[1] + far[1]
        rows = pl.ds(pl.multiple_of(((device - step) & 3) * ROWS, ROWS), ROWS)
        part_ref[0, rows, :] = same + other
        part_ref[1, rows, :] = flip_core * (same - other)
        same, other = flip_chip * (near[0] - far[0]), flip_chip * (near[1] - far[1])
        part_ref[2, rows, :] = jnp.where(flip_core > 0, same, other)
        part_ref[3, rows, :] = jnp.where(flip_core > 0, other, same)
    operands = front(*[part_ref[i] for i in range(4)], 0)
    for (_, first, count), operand, refs in zip(CLASSES, operands, f_refs):
        out_ref[LANES * first : LANES * (first + count), :] = from_left(*refs, operand)


def first_kernel(device_ref, *refs):
    to_frequency(device_ref[0], refs[:8], pairs(refs[8:18]), refs[19], refs[18])


def first_pass(device, g, frequency):
    out = jax.ShapeDtypeStruct((N, LANES), jnp.float32)
    specs = [pl.BlockSpec(memory_space=pltpu.SMEM)] + [pl.BlockSpec(memory_space=pltpu.VMEM)] * 18
    scratch = [pltpu.VMEM((4, INNER, LANES), jnp.float32)]
    return call(first_kernel, out, scratch, LIMIT[2], 10**9, specs)(device, *g, *frequency)


def rows_kernel(device_ref, one_ref, *refs):
    g_refs, refs = refs[:8], refs[8:]
    table = pairs(refs[:10])
    even_ref, odd_ref, last_ref, out_ref, part_ref, two_ref, data_ref = refs[20:]
    device = device_ref[0]
    to_frequency(device, g_refs, pairs(refs[10:20]), part_ref, two_ref)
    _, weight = lane_frequency(device, (8, LANES))
    total = jnp.zeros((HALF, LANES), jnp.float32)
    special = jnp.zeros((8, LANES), jnp.float32)
    row, lane = iota((HALF, LANES), 0), iota((HALF, LANES), 1)
    sign = jnp.where(lane < HALF, 1.0, -1.0)
    fix = (lane == HALF) & (device == 0)
    for part in range(DEV):
        upper, lower = pl.ds(LANES * part, HALF), pl.ds(LANES * part + HALF, HALF)
        x_one, x_two = one_ref[upper, :], two_ref[upper, :]
        y_one, y_two = one_ref[lower, :], two_ref[lower, :]
        x_two = jnp.where(fix, -x_one, sign * pltpu.roll(x_two, HALF, 1))
        y_two = jnp.where(fix, -y_one, sign * pltpu.roll(y_two, HALF, 1))
        rows = pl.ds(HALF * part, HALF)
        even, odd = even_ref[rows, :], odd_ref[rows, :]
        cosine = even * x_one - odd * y_two
        sine = even * y_one + odd * x_two
        if part == 0:
            edge, other = y_one[0:8], y_two[0:8]
            turned = sign[0:8] * pltpu.roll(edge, HALF, 1)
            turned = jnp.where(fix[0:8], pltpu.roll(other, HALF, 1), turned)
            edge = last_ref[0:8, :] * edge + last_ref[8:16, :] * turned
            edge = jnp.concatenate([edge] * 8, axis=0)
            cosine = jnp.where(row == 0, even * x_one, cosine)
            sine = jnp.where(row == 0, edge, sine)
            special = (cosine * cosine + sine * sine)[0:8]
        total = total + (cosine * cosine + sine * sine)
        data_ref[upper, :] = cosine
        data_ref[lower, :] = sine
    special = jnp.where(iota((8, LANES), 0) == 0, special, 0.0)
    energy = jnp.sum(total, axis=0, keepdims=True) + jnp.sum(special, axis=0, keepdims=True)
    energy = 0.5 * energy / weight[0:1]

    values = []
    for (_, first, count), refs in zip(CLASSES, table):
        values.append(from_left(*refs, data_ref[LANES * first : LANES * (first + count), :]))
    for r, value in enumerate(back(values, 0)):
        for part in range(4):
            out_ref[4 * r + part, 0:ROWS, :] = value[ROWS * part : ROWS * (part + 1)]
    for s in range(DEV):
        out_ref[s, ROWS : ROWS + 1, :] = out_ref[(s - 1) % DEV, ROWS - 1 : ROWS, :]
        out_ref[s, ROWS + 1 : ROWS + 2, :] = out_ref[(s + 1) % DEV, 0:1, :]
        out_ref[s, ROWS + 2 : ROWS + 3, :] = energy
        out_ref[s, ROWS + 3 : BLOCK, :] = jnp.zeros((BLOCK - ROWS - 3, LANES), jnp.float32)


def row_pass(device, one, g, sample, frequency, factors):
    out = jax.ShapeDtypeStruct((DEV, BLOCK, LANES), jnp.float32)
    scratch = [
        pltpu.VMEM((4, INNER, LANES), jnp.float32),
        pltpu.VMEM((N, LANES), jnp.float32),
        pltpu.VMEM((N, LANES), jnp.float32),
    ]
    specs = [pl.BlockSpec(memory_space=pltpu.SMEM)] + [pl.BlockSpec(memory_space=pltpu.VMEM)] * 32
    run = call(rows_kernel, out, scratch, LIMIT[3], 3 * 10**9, specs)
    return run(device, one, *g, *sample, *frequency, *factors)


def peaks_kernel(bins_ref, x_ref, *refs):
    table, offsets_ref, refs = pairs(refs[:10]), refs[10], refs[11:]
    snr_ref, heights_ref, counts_ref, field_ref, wide_ref, pick_ref = refs

    def block(first, count):
        body = jnp.concatenate([x_ref[s] for s in range(first, first + count)], axis=1)
        pad = jnp.zeros((8, body.shape[1]), jnp.float32)
        return jnp.concatenate([body, pad], axis=0)

    values = []
    for (_, first, count), pair in zip(CLASSES, table):
        values.append(from_right(block(first, count), *pair))
    energy = x_ref[0, ROWS : BLOCK, :]
    for s in range(1, DEV):
        energy = energy + x_ref[s, ROWS : BLOCK, :]
    mean = jnp.sum(energy[2:3, :], axis=1, keepdims=True)
    inverse = 1.0 / jnp.sqrt(mean + 1e-06)
    for c, value in enumerate(back(values, 1)):
        cols = pl.ds(INNER * c, INNER)
        snr_ref[:, cols] = value[0:ROWS] * inverse
        field_ref[8 : ROWS + 8, cols] = value[0:ROWS]
        field_ref[7:8, cols] = value[ROWS : ROWS + 1]
        field_ref[ROWS + 8 : ROWS + 9, cols] = value[ROWS + 1 : ROWS + 2]
    for start in (0,) + tuple(range(8, ROWS + 8, 16)) + (ROWS + 8,):
        size = 8 if start in (0, ROWS + 8) else 16
        value = field_ref[start : start + size, :]
        side = jnp.maximum(pltpu.roll(value, 1, 1), pltpu.roll(value, N - 1, 1))
        wide_ref[start : start + size, :] = jnp.maximum(side, value)
    blocks = iota((LANES, N), 1) // CELL == iota((LANES, N), 0)
    blocks = jnp.where(blocks, 1.0, 0.0).astype(jnp.bfloat16)
    offsets = offsets_ref[...].astype(jnp.float32).astype(jnp.bfloat16)
    offsets = jnp.concatenate([offsets, offsets], axis=0)
    spread = jnp.dot(offsets, blocks, preferred_element_type=jnp.float32)
    code = (iota((CELL, N), 0) * CELL + (iota((CELL, N), 1) & (CELL - 1))).astype(jnp.float32)
    for p in range(ROWS // CELL):
        base = 8 + CELL * p
        value = field_ref[base : base + CELL, :]
        side = jnp.maximum(pltpu.roll(value, 1, 1), pltpu.roll(value, N - 1, 1))
        above = wide_ref[base - 1 : base - 1 + CELL, :]
        below = wide_ref[base + 1 : base + 1 + CELL, :]
        nearest = jnp.maximum(side, jnp.maximum(above, below))
        chosen = spread[p : p + 1, :] == code
        height = jnp.sum(jnp.where(chosen, value - nearest, 0.0), axis=0, keepdims=True)
        level = jnp.sum(jnp.where(chosen, value, 0.0), axis=0, keepdims=True)
        pick_ref[p : p + 1, :] = height
        pick_ref[8 + p : 9 + p, :] = level
    high, low = split(pick_ref[...])
    gather = partial(
        lax.dot_general,
        dimension_numbers=(((1,), (1,)), ((), ())),
        preferred_element_type=jnp.float32,
    )
    picked = (gather(high, blocks) + gather(low, blocks)) * inverse
    heights, values = picked[0:8], picked[8:16]
    heights_ref[...] = heights
    weight = jax.nn.sigmoid(heights * 20.0)
    lane = iota((1, LANES), 1)
    counts = jnp.zeros((1, LANES), jnp.float32)
    for k in range(16):
        level = 0.25 * bins_ref[0, k].astype(jnp.float32)
        above = weight * jax.nn.sigmoid((values - level) * 10.0)
        summed = jnp.sum(jnp.sum(above, axis=0, keepdims=True), axis=1, keepdims=True)
        counts = counts + jnp.where(lane == k, summed, 0.0)
    for s in range(DEV):
        counts_ref[s] = jnp.broadcast_to(counts, (8, LANES))


def peak_pass(thresholds, x, table, offsets):
    f32 = jnp.float32
    out = [
        jax.ShapeDtypeStruct((ROWS, N), f32),
        jax.ShapeDtypeStruct((8, LANES), f32),
        jax.ShapeDtypeStruct((DEV, 8, LANES), f32),
    ]
    scratch = [
        pltpu.VMEM((ROWS + 16, N), f32),
        pltpu.VMEM((ROWS + 16, N), f32),
        pltpu.VMEM((16, N), f32),
    ]
    specs = [pl.BlockSpec(memory_space=pltpu.SMEM)] + [pl.BlockSpec(memory_space=pltpu.VMEM)] * 12
    run = call(peaks_kernel, out, scratch, LIMIT[4], 2 * 10**9, specs)
    return run(thresholds, x, *table, offsets)


def chip_pairs(index):
    return [(d, (d & 12 ^ (2 * (index & 4))) + ((d + index) & 3)) for d in range(DEV)]


def body(shear, smoothing, offsets, thresholds):
    group = ("row", "col")
    device = lax.axis_index(group).astype(jnp.int32).reshape(1)

    def exchange(x):
        return lax.all_to_all(x, group, split_axis=0, concat_axis=0, tiled=True)

    def scatter(keep, send):
        got = lax.ppermute(send, group, [(d, d ^ 4) for d in range(DEV)])
        blocks = merge(keep, got)
        done = [blocks[0]]
        for index in ORDER:
            done.append((index, lax.ppermute(blocks[index], group, chip_pairs(index))))
        return [blocks[0]] + [value for _, value in sorted(done[1:], key=lambda item: item[0])]

    blocks = pack(device, shear)
    fields = []
    for field in range(2):
        got = [blocks[4 * field], None, None, None]
        for step in (2, 1, 3):
            pairs = [(c, (c + step) % 4) for c in range(4)]
            got[4 - step] = lax.ppermute(blocks[4 * field + step], "col", pairs)
        fields.append(got)
    sample, frequency, factors = tables(smoothing, device)
    g = columns(device, fields[0], sample)
    one = scatter(*g)
    g = columns(device, fields[1], sample)
    two = scatter(*g)
    one = first_pass(device, one, frequency)
    k = row_pass(device, one, two, sample, frequency, factors)
    out = peak_pass(thresholds, exchange(k), frequency, offsets[0])
    snr, heights, counts = out
    counts = exchange(counts)
    return snr[None], heights[None], jnp.sum(counts[:, 0:1, 0:16], axis=0)


def solution(mesh):
    return jax.shard_map(
        body,
        mesh=mesh,
        in_specs=(
            P(None, "maps", "row", "col"),
            P("maps"),
            P("maps", ("row", "col"), None),
            P("maps", None),
        ),
        out_specs=(
            P("maps", ("row", "col"), None),
            P("maps", ("row", "col"), None),
            P("maps", None),
        ),
        check_vma=False,
    )
```

```python
from functools import partial
import math

import jax
import jax.numpy as jnp
from jax import lax
from jax.experimental import pallas as pl
from jax.experimental.pallas import tpu as pltpu
from jax.sharding import PartitionSpec as P


N = 2048
INNER = 512
DENSE = 256
DEV = 16
ROWS = 128
LANES = 128
HALF = 64
CELL = 16
BLOCK = ROWS + 8
CLASSES = ((0, 0, 2), (4, 2, 2), (2, 4, 4), (1, 8, 4), (3, 12, 4))
ROOT = math.sqrt(0.5)
MIB = 1 << 20
LIMIT = (20, 24, 24, 36, 32)
ORDER = (6, 5, 7, 4, 2, 1, 3)


def call(kernel, out, scratch, limit, flops, ins):
    return pl.pallas_call(
        kernel,
        out_shape=out,
        in_specs=ins,
        scratch_shapes=scratch,
        compiler_params=pltpu.CompilerParams(vmem_limit_bytes=limit * MIB),
        cost_estimate=pl.CostEstimate(flops=flops, bytes_accessed=4 * MIB, transcendentals=0),
    )


def split(x):
    high = x.astype(jnp.bfloat16)
    return high, (x - high.astype(jnp.float32)).astype(jnp.bfloat16)


def dot(left, right):
    return jnp.dot(left, right, preferred_element_type=jnp.float32)


def from_left(high_ref, low_ref, x):
    high, low = split(x)
    width = x.shape[1]
    both = dot(high_ref[...], jnp.concatenate([high, low], axis=1))
    return both[:, :width] + (both[:, width:] + dot(low_ref[...], high))


def from_right(x, high_ref, low_ref):
    high, low = split(x)
    height = x.shape[0]
    both = dot(jnp.concatenate([high, low], axis=0), high_ref[...])
    return both[:height] + (both[height:] + dot(high, low_ref[...]))


def pairs(refs):
    return tuple(zip(refs[0::2], refs[1::2]))


def take(x, start, size, axis):
    return lax.slice_in_dim(x, start, start + size, axis=axis)


def front(zero, two, even, odd, axis):
    near = [take(x, 0, DENSE, axis) for x in (zero, two, even, odd)]
    far = [take(x, DENSE, DENSE, axis) for x in (zero, two, even, odd)]
    change, total = ROOT * (far[2] - far[3]), ROOT * (far[2] + far[3])
    join = partial(jnp.concatenate, axis=axis)
    return (
        near[0] + far[0],
        near[0] - far[0],
        join([near[1], -far[1]]),
        join([near[2] + change, -near[3] - total]),
        join([near[2] - change, near[3] - total]),
    )


def back(values, axis):
    first, second, turn, one, three = values
    real = [take(x, 0, DENSE, axis) for x in (turn, one, three)]
    imag = [take(x, DENSE, DENSE, axis) for x in (turn, one, three)]
    change, total = real[1] - real[2], -imag[1] - imag[2]
    halves = (
        (first + second, real[0], real[1] + real[2], imag[2] - imag[1]),
        (first - second, -imag[0], ROOT * (total + change), ROOT * (total - change)),
    )
    blocks = []
    for zero, two, even, odd in halves:
        plus, minus = zero + two, zero - two
        blocks.append((plus + even, minus + odd, plus - even, minus - odd))
    return [jnp.concatenate([near, far], axis=axis) for near, far in zip(*blocks)]


def angle(steps):
    wrapped = jnp.bitwise_and(steps, N - 1)
    wrapped = jnp.where(wrapped >= N // 2, wrapped - N, wrapped)
    return wrapped.astype(jnp.float32) * (2.0 * math.pi / N)


def iota(shape, dim):
    return lax.broadcasted_iota(jnp.int32, shape, dim)


def put(high_ref, low_ref, rows, cols, value):
    high, low = split(value)
    high_ref[rows, cols] = high
    low_ref[rows, cols] = low


def sample_form(refs, scratch):
    cos_ref, sin_ref = scratch
    for (start, _, blocks), (high_ref, low_ref) in zip(CLASSES, refs):
        width = LANES * blocks
        col = iota((HALF, width), 1)
        freq = start + 8 * (HALF * (col // LANES) + col % HALF)
        quarter = jnp.where(col % LANES >= HALF, 1, 0)
        if start == 0:
            freq = jnp.where(col == HALF, N // 2, freq)
            quarter = jnp.where(col == HALF, 0, quarter)
        fine = angle(freq * iota((HALF, width), 0))
        cos_ref[:, :width] = jnp.cos(fine)
        sin_ref[:, :width] = jnp.sin(fine)
        coarse = angle(freq[:8] * (HALF * iota((8, width), 0)) + INNER * quarter[:8])
        cos_high, sin_high = jnp.cos(coarse), jnp.sin(coarse)
        for part in range(DENSE // HALF):
            cos_part, sin_part = cos_high[part : part + 1], sin_high[part : part + 1]
            rows = pl.ds(HALF * part, HALF)
            cos_fine, sin_fine = cos_ref[:, :width], sin_ref[:, :width]
            put(high_ref, low_ref, rows, slice(None), cos_part * cos_fine - sin_part * sin_fine)
            if blocks == 4:
                rows = pl.ds(DENSE + HALF * part, HALF)
                value = sin_part * cos_fine + cos_part * sin_fine
                put(high_ref, low_ref, rows, slice(None), value)


def frequency_form(refs, scratch):
    cos_ref, sin_ref = scratch
    fine = angle(8 * iota((HALF, DENSE), 0) * iota((HALF, DENSE), 1))
    cos_ref[:, :DENSE] = jnp.cos(fine)
    sin_ref[:, :DENSE] = jnp.sin(fine)
    for (start, _, blocks), (high_ref, low_ref) in zip(CLASSES, refs):
        coarse = angle((start + 8 * HALF * iota((8, DENSE), 0)) * iota((8, DENSE), 1))
        cos_high, sin_high = jnp.cos(coarse), jnp.sin(coarse)
        for part in range(blocks):
            cos_part, sin_part = cos_high[part : part + 1], sin_high[part : part + 1]
            cos_fine, sin_fine = cos_ref[:, :DENSE], sin_ref[:, :DENSE]
            cosine = cos_part * cos_fine - sin_part * sin_fine
            sine = sin_part * cos_fine + cos_part * sin_fine
            turned = -sine
            if start == 0 and part == 0:
                flip = (1 - 2 * (iota((HALF, DENSE), 1) & 1)).astype(jnp.float32)
                turned = jnp.where(iota((HALF, DENSE), 0) == 0, flip, turned)
            upper, lower = pl.ds(LANES * part, HALF), pl.ds(LANES * part + HALF, HALF)
            put(high_ref, low_ref, upper, pl.ds(0, DENSE), cosine)
            put(high_ref, low_ref, lower, pl.ds(0, DENSE), turned)
            if blocks == 4:
                put(high_ref, low_ref, upper, pl.ds(DENSE, DENSE), sine)
                put(high_ref, low_ref, lower, pl.ds(DENSE, DENSE), cosine)


def signed(freq):
    return jnp.where(freq < N // 2, freq, freq - N)


def lane_frequency(device, shape):
    lane = iota(shape, 1)
    block = jnp.where(device < 4, device & 1, device & 3)
    start = jnp.where(device < 2, 0, jnp.where(device < 4, 4, 2))
    start = jnp.where(device < 8, start, jnp.where(device < 12, 1, 3))
    freq = signed(start + 8 * (HALF * block + lane % HALF))
    nyquist = (device == 0) & (lane == HALF)
    freq = jnp.where(nyquist, -(N // 2), freq)
    single = nyquist | ((device == 0) & (lane == 0))
    return freq.astype(jnp.float32), jnp.where(single, 1.0, 2.0)


def tables_kernel(smooth_ref, device_ref, *refs):
    device = device_ref[0]
    scratch = refs[-2:]
    w_refs, f_refs = pairs(refs[0:10]), pairs(refs[10:20])
    even_ref, odd_ref, last_ref = refs[20:23]
    sample_form(w_refs, scratch)
    frequency_form(f_refs, scratch)
    width = smooth_ref[0]
    decay = width * width * (-2.0 * math.pi**2 / (N * N))
    shape = (HALF, LANES)
    freq_y, weight = lane_frequency(device, shape)

    def factors(freq_x, weight):
        total = freq_x * freq_x + freq_y * freq_y
        scaled = jnp.exp(decay * total) * weight / jnp.maximum(total, 1.0)
        return (freq_x * freq_x - freq_y * freq_y) * scaled, 2.0 * freq_x * freq_y * scaled

    for start, first, blocks in CLASSES:
        for part in range(blocks):
            freq = signed(start + 8 * (HALF * part + iota(shape, 0)))
            row_weight = jnp.where(freq == 0, 1.0, 2.0) * (1.0 / (N * N))
            even, odd = factors(freq.astype(jnp.float32), weight * row_weight)
            rows = pl.ds(HALF * (first + part), HALF)
            even_ref[rows, :] = even
            odd_ref[rows, :] = odd
    even, odd = factors(jnp.full(shape, -N / 2, jnp.float32), weight * (1.0 / (N * N)))
    last_ref[0:8, :] = even[0:8]
    last_ref[8:16, :] = odd[0:8]


def tables(smoothing, device):
    low = jnp.bfloat16
    table = []
    for _, _, blocks in CLASSES:
        table += [jax.ShapeDtypeStruct((LANES * blocks, LANES * blocks), low)] * 2
    out = table + table + [
        jax.ShapeDtypeStruct((N // 2, LANES), jnp.float32),
        jax.ShapeDtypeStruct((N // 2, LANES), jnp.float32),
        jax.ShapeDtypeStruct((16, LANES), jnp.float32),
    ]
    scratch = [pltpu.VMEM((HALF, INNER), jnp.float32)] * 2
    smem = pl.BlockSpec(memory_space=pltpu.SMEM)
    result = call(tables_kernel, out, scratch, LIMIT[0], 10**9, [smem, smem])(smoothing, device)
    return result[0:10], result[10:20], result[20:23]


def quarters(blocks):
    first, second, third, fourth = blocks
    return (
        (first + third) + (second + fourth),
        (first + third) - (second + fourth),
        first - third,
        second - fourth,
    )


def pack_kernel(device_ref, x_ref, *outs):
    for index in range(8):
        start = pl.multiple_of(((device_ref[0] + index) & 3) * ROWS, ROWS)
        outs[index][...] = x_ref[index // 4, 0, pl.ds(start, ROWS), :]


def pack(device, shear):
    out = [jax.ShapeDtypeStruct((ROWS, INNER), jnp.float32)] * 8
    specs = [pl.BlockSpec(memory_space=pltpu.SMEM), pl.BlockSpec(memory_space=pltpu.VMEM)]
    return call(pack_kernel, out, (), LIMIT[1], 10**6, specs)(device, shear)


def columns_kernel(device_ref, *refs):
    blocks, table = refs[:4], pairs(refs[4:14])
    keep_ref, send_ref, all_ref = refs[14:]
    zero, two, even, odd = quarters([x[...] for x in blocks])
    device = device_ref[0]
    place = device & 3
    along = jnp.where(place == 0, 1.0, jnp.where(place == 2, -1.0, 0.0))
    across = jnp.where(place == 1, 1.0, jnp.where(place == 3, -1.0, 0.0))
    flip = jnp.where((place & 1) == 0, 1.0, -1.0)

    even, odd = along * even - across * odd, across * even + along * odd
    operands = front(zero, flip * two, even, odd, 1)
    for (_, first, count), operand, refs in zip(CLASSES, operands, table):
        value = from_right(operand, *refs)
        for part in range(count):
            all_ref[first + part] = value[:, LANES * part : LANES * (part + 1)]
    for index in range(8):
        there = other_chip(device, index)
        keep_ref[index] = all_ref[there]
        send_ref[index] = all_ref[there ^ 4]


def other_chip(device, index):
    return ((device & 12) ^ (2 * (index & 4))) + ((device + index) & 3)


def columns(device, blocks, table):
    out = [jax.ShapeDtypeStruct((8, ROWS, LANES), jnp.float32)] * 2
    specs = [pl.BlockSpec(memory_space=pltpu.SMEM)] + [pl.BlockSpec(memory_space=pltpu.VMEM)] * 14
    scratch = [pltpu.VMEM((DEV, ROWS, LANES), jnp.float32)]
    return call(columns_kernel, out, scratch, LIMIT[1], 2 * 10**9, specs)(device, *blocks, *table)


def merge_kernel(keep_ref, got_ref, *outs):
    for index in range(8):
        outs[index][0] = keep_ref[index]
        outs[index][1] = got_ref[index]


def merge(keep, got):
    out = [jax.ShapeDtypeStruct((2,) + keep.shape[1:], jnp.float32)] * 8
    specs = [pl.BlockSpec(memory_space=pltpu.VMEM)] * 2
    return call(merge_kernel, out, (), 8, 10**8, specs)(keep, got)


def to_frequency(device, g_refs, f_refs, part_ref, out_ref):
    flip_core = jnp.where((device & 4) == 0, 1.0, -1.0)
    flip_chip = jnp.where((device & 8) == 0, 1.0, -1.0)
    for step in range(4):
        near, far = g_refs[step], g_refs[4 + step]
        same, other = near[0] + far[0], near[1] + far[1]
        rows = pl.ds(pl.multiple_of(((device - step) & 3) * ROWS, ROWS), ROWS)
        part_ref[0, rows, :] = same + other
        part_ref[1, rows, :] = flip_core * (same - other)
        same, other = flip_chip * (near[0] - far[0]), flip_chip * (near[1] - far[1])
        part_ref[2, rows, :] = jnp.where(flip_core > 0, same, other)
        part_ref[3, rows, :] = jnp.where(flip_core > 0, other, same)
    operands = front(*[part_ref[i] for i in range(4)], 0)
    for (_, first, count), operand, refs in zip(CLASSES, operands, f_refs):
        out_ref[LANES * first : LANES * (first + count), :] = from_left(*refs, operand)


def first_kernel(device_ref, *refs):
    to_frequency(device_ref[0], refs[:8], pairs(refs[8:18]), refs[19], refs[18])


def first_pass(device, g, frequency):
    out = jax.ShapeDtypeStruct((N, LANES), jnp.float32)
    specs = [pl.BlockSpec(memory_space=pltpu.SMEM)] + [pl.BlockSpec(memory_space=pltpu.VMEM)] * 18
    scratch = [pltpu.VMEM((4, INNER, LANES), jnp.float32)]
    return call(first_kernel, out, scratch, LIMIT[2], 10**9, specs)(device, *g, *frequency)


def rows_kernel(device_ref, one_ref, *refs):
    g_refs, refs = refs[:8], refs[8:]
    table = pairs(refs[:10])
    even_ref, odd_ref, last_ref, keep_ref, send_ref, part_ref, two_ref, data_ref, out_ref = refs[20:]
    device = device_ref[0]
    to_frequency(device, g_refs, pairs(refs[10:20]), part_ref, two_ref)
    _, weight = lane_frequency(device, (8, LANES))
    total = jnp.zeros((HALF, LANES), jnp.float32)
    special = jnp.zeros((8, LANES), jnp.float32)
    row, lane = iota((HALF, LANES), 0), iota((HALF, LANES), 1)
    sign = jnp.where(lane < HALF, 1.0, -1.0)
    fix = (lane == HALF) & (device == 0)
    for part in range(DEV):
        upper, lower = pl.ds(LANES * part, HALF), pl.ds(LANES * part + HALF, HALF)
        x_one, x_two = one_ref[upper, :], two_ref[upper, :]
        y_one, y_two = one_ref[lower, :], two_ref[lower, :]
        x_two = jnp.where(fix, -x_one, sign * pltpu.roll(x_two, HALF, 1))
        y_two = jnp.where(fix, -y_one, sign * pltpu.roll(y_two, HALF, 1))
        rows = pl.ds(HALF * part, HALF)
        even, odd = even_ref[rows, :], odd_ref[rows, :]
        cosine = even * x_one - odd * y_two
        sine = even * y_one + odd * x_two
        if part == 0:
            edge, other = y_one[0:8], y_two[0:8]
            turned = sign[0:8] * pltpu.roll(edge, HALF, 1)
            turned = jnp.where(fix[0:8], pltpu.roll(other, HALF, 1), turned)
            edge = last_ref[0:8, :] * edge + last_ref[8:16, :] * turned
            edge = jnp.concatenate([edge] * 8, axis=0)
            cosine = jnp.where(row == 0, even * x_one, cosine)
            sine = jnp.where(row == 0, edge, sine)
            special = (cosine * cosine + sine * sine)[0:8]
        total = total + (cosine * cosine + sine * sine)
        data_ref[upper, :] = cosine
        data_ref[lower, :] = sine
    special = jnp.where(iota((8, LANES), 0) == 0, special, 0.0)
    energy = jnp.sum(total, axis=0, keepdims=True) + jnp.sum(special, axis=0, keepdims=True)
    energy = 0.5 * energy / weight[0:1]

    values = []
    for (_, first, count), refs in zip(CLASSES, table):
        values.append(from_left(*refs, data_ref[LANES * first : LANES * (first + count), :]))
    for r, value in enumerate(back(values, 0)):
        for part in range(4):
            out_ref[4 * r + part, 0:ROWS, :] = value[ROWS * part : ROWS * (part + 1)]
    for s in range(DEV):
        out_ref[s, ROWS : ROWS + 1, :] = out_ref[(s - 1) % DEV, ROWS - 1 : ROWS, :]
        out_ref[s, ROWS + 1 : ROWS + 2, :] = out_ref[(s + 1) % DEV, 0:1, :]
        out_ref[s, ROWS + 2 : ROWS + 3, :] = energy
        out_ref[s, ROWS + 3 : BLOCK, :] = jnp.zeros((BLOCK - ROWS - 3, LANES), jnp.float32)
    for index in range(8):
        there = other_chip(device, index)
        keep_ref[index] = out_ref[there]
        send_ref[index] = out_ref[there ^ 4]


def row_pass(device, one, g, sample, frequency, factors):
    out = [jax.ShapeDtypeStruct((8, BLOCK, LANES), jnp.float32)] * 2
    scratch = [
        pltpu.VMEM((4, INNER, LANES), jnp.float32),
        pltpu.VMEM((N, LANES), jnp.float32),
        pltpu.VMEM((N, LANES), jnp.float32),
        pltpu.VMEM((DEV, BLOCK, LANES), jnp.float32),
    ]
    specs = [pl.BlockSpec(memory_space=pltpu.SMEM)] + [pl.BlockSpec(memory_space=pltpu.VMEM)] * 32
    run = call(rows_kernel, out, scratch, LIMIT[3], 3 * 10**9, specs)
    return run(device, one, *g, *sample, *frequency, *factors)


def peaks_kernel(bins_ref, device_ref, *refs):
    got, table, offsets_ref, refs = refs[:8], pairs(refs[8:18]), refs[18], refs[19:]
    snr_ref, heights_ref, counts_ref, field_ref, wide_ref, side_ref, pick_ref, x_ref = refs
    for index in range(8):
        there = other_chip(device_ref[0], (index & 4) | (-index & 3))
        x_ref[there] = got[index][0]
        x_ref[there ^ 4] = got[index][1]

    def block(first, count):
        body = jnp.concatenate([x_ref[s] for s in range(first, first + count)], axis=1)
        pad = jnp.zeros((8, body.shape[1]), jnp.float32)
        return jnp.concatenate([body, pad], axis=0)

    values = []
    for (_, first, count), pair in zip(CLASSES, table):
        values.append(from_right(block(first, count), *pair))
    energy = x_ref[0, ROWS : BLOCK, :]
    for s in range(1, DEV):
        energy = energy + x_ref[s, ROWS : BLOCK, :]
    mean = jnp.sum(energy[2:3, :], axis=1, keepdims=True)
    inverse = 1.0 / jnp.sqrt(mean + 1e-06)
    for c, value in enumerate(back(values, 1)):
        cols = pl.ds(INNER * c, INNER)
        snr_ref[:, cols] = value[0:ROWS] * inverse
        field_ref[8 : ROWS + 8, cols] = value[0:ROWS]
        field_ref[7:8, cols] = value[ROWS : ROWS + 1]
        field_ref[ROWS + 8 : ROWS + 9, cols] = value[ROWS + 1 : ROWS + 2]
    for start in (0,) + tuple(range(8, ROWS + 8, 16)) + (ROWS + 8,):
        size = 8 if start in (0, ROWS + 8) else 16
        value = field_ref[start : start + size, :]
        side = jnp.maximum(pltpu.roll(value, 1, 1), pltpu.roll(value, N - 1, 1))
        wide_ref[start : start + size, :] = jnp.maximum(side, value)
        side_ref[start : start + size, :] = side
    blocks = iota((LANES, N), 1) // CELL == iota((LANES, N), 0)
    blocks = jnp.where(blocks, 1.0, 0.0).astype(jnp.bfloat16)
    offsets = offsets_ref[...].astype(jnp.float32).astype(jnp.bfloat16)
    offsets = jnp.concatenate([offsets, offsets], axis=0)
    spread = jnp.dot(offsets, blocks, preferred_element_type=jnp.float32)
    code = (iota((CELL, N), 0) * CELL + (iota((CELL, N), 1) & (CELL - 1))).astype(jnp.float32)
    for p in range(ROWS // CELL):
        base = 8 + CELL * p
        value, side = field_ref[base : base + CELL, :], side_ref[base : base + CELL, :]
        above = wide_ref[base - 1 : base - 1 + CELL, :]
        below = wide_ref[base + 1 : base + 1 + CELL, :]
        nearest = jnp.maximum(side, jnp.maximum(above, below))
        chosen = spread[p : p + 1, :] == code
        height = jnp.sum(jnp.where(chosen, value - nearest, 0.0), axis=0, keepdims=True)
        level = jnp.sum(jnp.where(chosen, value, 0.0), axis=0, keepdims=True)
        pick_ref[p : p + 1, :] = height
        pick_ref[8 + p : 9 + p, :] = level
    high, low = split(pick_ref[...])
    gather = partial(
        lax.dot_general,
        dimension_numbers=(((1,), (1,)), ((), ())),
        preferred_element_type=jnp.float32,
    )
    picked = (gather(high, blocks) + gather(low, blocks)) * inverse
    heights, values = picked[0:8], picked[8:16]
    heights_ref[...] = heights
    weight = jax.nn.sigmoid(heights * 20.0)
    lane = iota((1, LANES), 1)
    counts = jnp.zeros((1, LANES), jnp.float32)
    for k in range(16):
        level = 0.25 * bins_ref[0, k].astype(jnp.float32)
        above = weight * jax.nn.sigmoid((values - level) * 10.0)
        summed = jnp.sum(jnp.sum(above, axis=0, keepdims=True), axis=1, keepdims=True)
        counts = counts + jnp.where(lane == k, summed, 0.0)
    for s in range(DEV):
        counts_ref[s] = jnp.broadcast_to(counts, (8, LANES))


def peak_pass(thresholds, device, x, table, offsets):
    f32 = jnp.float32
    out = [
        jax.ShapeDtypeStruct((ROWS, N), f32),
        jax.ShapeDtypeStruct((8, LANES), f32),
        jax.ShapeDtypeStruct((DEV, 8, LANES), f32),
    ]
    scratch = [
        pltpu.VMEM((ROWS + 16, N), f32),
        pltpu.VMEM((ROWS + 16, N), f32),
        pltpu.VMEM((ROWS + 16, N), f32),
        pltpu.VMEM((16, N), f32),
        pltpu.VMEM((DEV, BLOCK, LANES), f32),
    ]
    specs = [pl.BlockSpec(memory_space=pltpu.SMEM)] * 2 + [pl.BlockSpec(memory_space=pltpu.VMEM)] * 19
    run = call(peaks_kernel, out, scratch, LIMIT[4], 2 * 10**9, specs)
    return run(thresholds, device, *x, *table, offsets)


def chip_pairs(index):
    return [(d, (d & 12 ^ (2 * (index & 4))) + ((d + index) & 3)) for d in range(DEV)]


def body(shear, smoothing, offsets, thresholds):
    group = ("row", "col")
    device = lax.axis_index(group).astype(jnp.int32).reshape(1)

    def exchange(x):
        return lax.all_to_all(x, group, split_axis=0, concat_axis=0, tiled=True)

    def scatter(keep, send):
        got = lax.ppermute(send, group, [(d, d ^ 4) for d in range(DEV)])
        blocks = merge(keep, got)
        done = [blocks[0]]
        for index in ORDER:
            done.append((index, lax.ppermute(blocks[index], group, chip_pairs(index))))
        return [blocks[0]] + [value for _, value in sorted(done[1:], key=lambda item: item[0])]

    blocks = pack(device, shear)
    fields = []
    for field in range(2):
        got = [blocks[4 * field], None, None, None]
        for step in (2, 1, 3):
            pairs = [(c, (c + step) % 4) for c in range(4)]
            got[4 - step] = lax.ppermute(blocks[4 * field + step], "col", pairs)
        fields.append(got)
    sample, frequency, factors = tables(smoothing, device)
    g = columns(device, fields[0], sample)
    one = scatter(*g)
    g = columns(device, fields[1], sample)
    two = scatter(*g)
    one = first_pass(device, one, frequency)
    k = row_pass(device, one, two, sample, frequency, factors)
    out = peak_pass(thresholds, device, scatter(*k), frequency, offsets[0])
    snr, heights, counts = out
    counts = exchange(counts)
    return snr[None], heights[None], jnp.sum(counts[:, 0:1, 0:16], axis=0)


def solution(mesh):
    return jax.shard_map(
        body,
        mesh=mesh,
        in_specs=(
            P(None, "maps", "row", "col"),
            P("maps"),
            P("maps", ("row", "col"), None),
            P("maps", None),
        ),
        out_specs=(
            P("maps", ("row", "col"), None),
            P("maps", ("row", "col"), None),
            P("maps", None),
        ),
        check_vma=False,
    )
```

```python
from functools import partial
import math

import jax
import jax.numpy as jnp
from jax import lax
from jax.experimental import pallas as pl
from jax.experimental.pallas import tpu as pltpu
from jax.sharding import PartitionSpec as P


N = 2048
INNER = 512
DENSE = 256
DEV = 16
ROWS = 128
LANES = 128
HALF = 64
CELL = 16
BLOCK = ROWS + 8
CLASSES = ((0, 0, 2), (4, 2, 2), (2, 4, 4), (1, 8, 4), (3, 12, 4))
ROOT = math.sqrt(0.5)
MIB = 1 << 20
LIMIT = (20, 24, 24, 36, 32)
ORDER = (6, 5, 7, 4, 2, 1, 3)


def call(kernel, out, scratch, limit, flops, ins, outs=None):
    return pl.pallas_call(
        kernel,
        out_shape=out,
        in_specs=ins,
        **({} if outs is None else {"out_specs": outs}),
        scratch_shapes=scratch,
        compiler_params=pltpu.CompilerParams(vmem_limit_bytes=limit * MIB),
        cost_estimate=pl.CostEstimate(flops=flops, bytes_accessed=4 * MIB, transcendentals=0),
    )


def split(x):
    high = x.astype(jnp.bfloat16)
    return high, (x - high.astype(jnp.float32)).astype(jnp.bfloat16)


def dot(left, right):
    return jnp.dot(left, right, preferred_element_type=jnp.float32)


def from_left(high_ref, low_ref, x):
    high, low = split(x)
    width = x.shape[1]
    both = dot(high_ref[...], jnp.concatenate([high, low], axis=1))
    return both[:, :width] + (both[:, width:] + dot(low_ref[...], high))


def from_right(x, high_ref, low_ref):
    high, low = split(x)
    height = x.shape[0]
    both = dot(jnp.concatenate([high, low], axis=0), high_ref[...])
    return both[:height] + (both[height:] + dot(high, low_ref[...]))


def pairs(refs):
    return tuple(zip(refs[0::2], refs[1::2]))


def take(x, start, size, axis):
    return lax.slice_in_dim(x, start, start + size, axis=axis)


def front(zero, two, even, odd, axis):
    near = [take(x, 0, DENSE, axis) for x in (zero, two, even, odd)]
    far = [take(x, DENSE, DENSE, axis) for x in (zero, two, even, odd)]
    change, total = ROOT * (far[2] - far[3]), ROOT * (far[2] + far[3])
    join = partial(jnp.concatenate, axis=axis)
    return (
        near[0] + far[0],
        near[0] - far[0],
        join([near[1], -far[1]]),
        join([near[2] + change, -near[3] - total]),
        join([near[2] - change, near[3] - total]),
    )


def back(values, axis):
    first, second, turn, one, three = values
    real = [take(x, 0, DENSE, axis) for x in (turn, one, three)]
    imag = [take(x, DENSE, DENSE, axis) for x in (turn, one, three)]
    change, total = real[1] - real[2], -imag[1] - imag[2]
    halves = (
        (first + second, real[0], real[1] + real[2], imag[2] - imag[1]),
        (first - second, -imag[0], ROOT * (total + change), ROOT * (total - change)),
    )
    blocks = []
    for zero, two, even, odd in halves:
        plus, minus = zero + two, zero - two
        blocks.append((plus + even, minus + odd, plus - even, minus - odd))
    return [jnp.concatenate([near, far], axis=axis) for near, far in zip(*blocks)]


def angle(steps):
    wrapped = jnp.bitwise_and(steps, N - 1)
    wrapped = jnp.where(wrapped >= N // 2, wrapped - N, wrapped)
    return wrapped.astype(jnp.float32) * (2.0 * math.pi / N)


def iota(shape, dim):
    return lax.broadcasted_iota(jnp.int32, shape, dim)


def put(high_ref, low_ref, rows, cols, value):
    high, low = split(value)
    high_ref[rows, cols] = high
    low_ref[rows, cols] = low


def sample_form(refs, scratch):
    cos_ref, sin_ref = scratch
    for (start, _, blocks), (high_ref, low_ref) in zip(CLASSES, refs):
        width = LANES * blocks
        col = iota((HALF, width), 1)
        freq = start + 8 * (HALF * (col // LANES) + col % HALF)
        quarter = jnp.where(col % LANES >= HALF, 1, 0)
        if start == 0:
            freq = jnp.where(col == HALF, N // 2, freq)
            quarter = jnp.where(col == HALF, 0, quarter)
        fine = angle(freq * iota((HALF, width), 0))
        cos_ref[:, :width] = jnp.cos(fine)
        sin_ref[:, :width] = jnp.sin(fine)
        coarse = angle(freq[:8] * (HALF * iota((8, width), 0)) + INNER * quarter[:8])
        cos_high, sin_high = jnp.cos(coarse), jnp.sin(coarse)
        for part in range(DENSE // HALF):
            cos_part, sin_part = cos_high[part : part + 1], sin_high[part : part + 1]
            rows = pl.ds(HALF * part, HALF)
            cos_fine, sin_fine = cos_ref[:, :width], sin_ref[:, :width]
            put(high_ref, low_ref, rows, slice(None), cos_part * cos_fine - sin_part * sin_fine)
            if blocks == 4:
                rows = pl.ds(DENSE + HALF * part, HALF)
                value = sin_part * cos_fine + cos_part * sin_fine
                put(high_ref, low_ref, rows, slice(None), value)


def frequency_form(refs, scratch):
    cos_ref, sin_ref = scratch
    fine = angle(8 * iota((HALF, DENSE), 0) * iota((HALF, DENSE), 1))
    cos_ref[:, :DENSE] = jnp.cos(fine)
    sin_ref[:, :DENSE] = jnp.sin(fine)
    for (start, _, blocks), (high_ref, low_ref) in zip(CLASSES, refs):
        coarse = angle((start + 8 * HALF * iota((8, DENSE), 0)) * iota((8, DENSE), 1))
        cos_high, sin_high = jnp.cos(coarse), jnp.sin(coarse)
        for part in range(blocks):
            cos_part, sin_part = cos_high[part : part + 1], sin_high[part : part + 1]
            cos_fine, sin_fine = cos_ref[:, :DENSE], sin_ref[:, :DENSE]
            cosine = cos_part * cos_fine - sin_part * sin_fine
            sine = sin_part * cos_fine + cos_part * sin_fine
            turned = -sine
            if start == 0 and part == 0:
                flip = (1 - 2 * (iota((HALF, DENSE), 1) & 1)).astype(jnp.float32)
                turned = jnp.where(iota((HALF, DENSE), 0) == 0, flip, turned)
            upper, lower = pl.ds(LANES * part, HALF), pl.ds(LANES * part + HALF, HALF)
            put(high_ref, low_ref, upper, pl.ds(0, DENSE), cosine)
            put(high_ref, low_ref, lower, pl.ds(0, DENSE), turned)
            if blocks == 4:
                put(high_ref, low_ref, upper, pl.ds(DENSE, DENSE), sine)
                put(high_ref, low_ref, lower, pl.ds(DENSE, DENSE), cosine)


def signed(freq):
    return jnp.where(freq < N // 2, freq, freq - N)


def lane_frequency(device, shape):
    lane = iota(shape, 1)
    block = jnp.where(device < 4, device & 1, device & 3)
    start = jnp.where(device < 2, 0, jnp.where(device < 4, 4, 2))
    start = jnp.where(device < 8, start, jnp.where(device < 12, 1, 3))
    freq = signed(start + 8 * (HALF * block + lane % HALF))
    nyquist = (device == 0) & (lane == HALF)
    freq = jnp.where(nyquist, -(N // 2), freq)
    single = nyquist | ((device == 0) & (lane == 0))
    return freq.astype(jnp.float32), jnp.where(single, 1.0, 2.0)


def tables_kernel(smooth_ref, device_ref, *refs):
    device = device_ref[0]
    scratch = refs[-2:]
    w_refs, f_refs = pairs(refs[0:10]), pairs(refs[10:20])
    even_ref, odd_ref, last_ref = refs[20:23]
    sample_form(w_refs, scratch)
    frequency_form(f_refs, scratch)
    width = smooth_ref[0]
    decay = width * width * (-2.0 * math.pi**2 / (N * N))
    shape = (HALF, LANES)
    freq_y, weight = lane_frequency(device, shape)

    def factors(freq_x, weight):
        total = freq_x * freq_x + freq_y * freq_y
        scaled = jnp.exp(decay * total) * weight / jnp.maximum(total, 1.0)
        return (freq_x * freq_x - freq_y * freq_y) * scaled, 2.0 * freq_x * freq_y * scaled

    for start, first, blocks in CLASSES:
        for part in range(blocks):
            freq = signed(start + 8 * (HALF * part + iota(shape, 0)))
            row_weight = jnp.where(freq == 0, 1.0, 2.0) * (1.0 / (N * N))
            even, odd = factors(freq.astype(jnp.float32), weight * row_weight)
            rows = pl.ds(HALF * (first + part), HALF)
            even_ref[rows, :] = even
            odd_ref[rows, :] = odd
    even, odd = factors(jnp.full(shape, -N / 2, jnp.float32), weight * (1.0 / (N * N)))
    last_ref[0:8, :] = even[0:8]
    last_ref[8:16, :] = odd[0:8]


def tables(smoothing, device):
    low = jnp.bfloat16
    table = []
    for _, _, blocks in CLASSES:
        table += [jax.ShapeDtypeStruct((LANES * blocks, LANES * blocks), low)] * 2
    out = table + table + [
        jax.ShapeDtypeStruct((N // 2, LANES), jnp.float32),
        jax.ShapeDtypeStruct((N // 2, LANES), jnp.float32),
        jax.ShapeDtypeStruct((16, LANES), jnp.float32),
    ]
    scratch = [pltpu.VMEM((HALF, INNER), jnp.float32)] * 2
    smem = pl.BlockSpec(memory_space=pltpu.SMEM)
    result = call(tables_kernel, out, scratch, LIMIT[0], 10**9, [smem, smem])(smoothing, device)
    return result[0:10], result[10:20], result[20:23]


def quarters(blocks):
    first, second, third, fourth = blocks
    return (
        (first + third) + (second + fourth),
        (first + third) - (second + fourth),
        first - third,
        second - fourth,
    )


def way(device):
    return 1 - ((device & 4) >> 1)


def pack_kernel(device_ref, x_ref, *outs):
    device = device_ref[0]
    for index in range(8):
        start = pl.multiple_of(((device + way(device) * (index & 3)) & 3) * ROWS, ROWS)
        outs[index][...] = x_ref[index // 4, 0, pl.ds(start, ROWS), :]


def pack(device, shear):
    out = [jax.ShapeDtypeStruct((ROWS, INNER), jnp.float32)] * 8
    specs = [pl.BlockSpec(memory_space=pltpu.SMEM), pl.BlockSpec(memory_space=pltpu.VMEM)]
    return call(pack_kernel, out, (), LIMIT[1], 10**6, specs)(device, shear)


def columns_kernel(device_ref, *refs):
    blocks, table = refs[:4], pairs(refs[4:14])
    keep_ref, send_ref, all_ref = refs[14:]
    zero, two, even, odd = quarters([x[...] for x in blocks])
    device = device_ref[0]
    place = device & 3
    odd = way(device).astype(jnp.float32) * odd
    along = jnp.where(place == 0, 1.0, jnp.where(place == 2, -1.0, 0.0))
    across = jnp.where(place == 1, 1.0, jnp.where(place == 3, -1.0, 0.0))
    flip = jnp.where((place & 1) == 0, 1.0, -1.0)

    even, odd = along * even - across * odd, across * even + along * odd
    operands = front(zero, flip * two, even, odd, 1)
    for (_, first, count), operand, refs in zip(CLASSES, operands, table):
        value = from_right(operand, *refs)
        for part in range(count):
            all_ref[first + part] = value[:, LANES * part : LANES * (part + 1)]
    for index in range(8):
        keep_ref[index] = all_ref[other_chip(device, index)]
        send_ref[index] = all_ref[other_chip(device ^ 4, index)]


def other_chip(device, index):
    return ((device & 12) ^ (2 * (index & 4))) + ((device + way(device) * (index & 3)) & 3)


def columns(device, blocks, table):
    out = [jax.ShapeDtypeStruct((8, ROWS, LANES), jnp.float32)] * 2
    specs = [pl.BlockSpec(memory_space=pltpu.SMEM)] + [pl.BlockSpec(memory_space=pltpu.VMEM)] * 14
    scratch = [pltpu.VMEM((DEV, ROWS, LANES), jnp.float32)]
    return call(columns_kernel, out, scratch, LIMIT[1], 2 * 10**9, specs)(device, *blocks, *table)


def merge_kernel(keep_ref, got_ref, *outs):
    for index in range(8):
        outs[index][0] = keep_ref[index]
        outs[index][1] = got_ref[index]


def merge(keep, got):
    out = [jax.ShapeDtypeStruct((2,) + keep.shape[1:], jnp.float32)] * 8
    specs = [pl.BlockSpec(memory_space=pltpu.VMEM)] * 2
    return call(merge_kernel, out, (), 8, 10**8, specs)(keep, got)


def to_frequency(device, g_refs, f_refs, part_ref, out_ref):
    flip_core = jnp.where((device & 4) == 0, 1.0, -1.0)
    flip_chip = jnp.where((device & 8) == 0, 1.0, -1.0)
    for step in range(4):
        near, far = g_refs[step], g_refs[4 + step]
        same, other = near[0] + far[0], near[1] + far[1]
        rows = pl.ds(pl.multiple_of(((device - way(device) * step) & 3) * ROWS, ROWS), ROWS)
        part_ref[0, rows, :] = same + other
        part_ref[1, rows, :] = flip_core * (same - other)
        same, other = flip_chip * (near[0] - far[0]), flip_chip * (near[1] - far[1])
        part_ref[2, rows, :] = jnp.where(flip_core > 0, same, other)
        part_ref[3, rows, :] = jnp.where(flip_core > 0, other, same)
    operands = front(*[part_ref[i] for i in range(4)], 0)
    for (_, first, count), operand, refs in zip(CLASSES, operands, f_refs):
        out_ref[LANES * first : LANES * (first + count), :] = from_left(*refs, operand)


def first_kernel(device_ref, *refs):
    to_frequency(device_ref[0], refs[:8], pairs(refs[8:18]), refs[19], refs[18])


def first_pass(device, g, frequency):
    out = jax.ShapeDtypeStruct((N, LANES), jnp.float32)
    specs = [pl.BlockSpec(memory_space=pltpu.SMEM)] + [pl.BlockSpec(memory_space=pltpu.VMEM)] * 18
    scratch = [pltpu.VMEM((4, INNER, LANES), jnp.float32)]
    return call(first_kernel, out, scratch, LIMIT[2], 10**9, specs)(device, *g, *frequency)


def rows_kernel(device_ref, one_ref, *refs):
    g_refs, refs = refs[:8], refs[8:]
    table = pairs(refs[:10])
    even_ref, odd_ref, last_ref, keep_ref, send_ref, part_ref, two_ref, data_ref, out_ref = refs[20:]
    device = device_ref[0]
    to_frequency(device, g_refs, pairs(refs[10:20]), part_ref, two_ref)
    _, weight = lane_frequency(device, (8, LANES))
    total = jnp.zeros((HALF, LANES), jnp.float32)
    special = jnp.zeros((8, LANES), jnp.float32)
    row, lane = iota((HALF, LANES), 0), iota((HALF, LANES), 1)
    sign = jnp.where(lane < HALF, 1.0, -1.0)
    fix = (lane == HALF) & (device == 0)
    for part in range(DEV):
        upper, lower = pl.ds(LANES * part, HALF), pl.ds(LANES * part + HALF, HALF)
        x_one, x_two = one_ref[upper, :], two_ref[upper, :]
        y_one, y_two = one_ref[lower, :], two_ref[lower, :]
        x_two = jnp.where(fix, -x_one, sign * pltpu.roll(x_two, HALF, 1))
        y_two = jnp.where(fix, -y_one, sign * pltpu.roll(y_two, HALF, 1))
        rows = pl.ds(HALF * part, HALF)
        even, odd = even_ref[rows, :], odd_ref[rows, :]
        cosine = even * x_one - odd * y_two
        sine = even * y_one + odd * x_two
        if part == 0:
            edge, other = y_one[0:8], y_two[0:8]
            turned = sign[0:8] * pltpu.roll(edge, HALF, 1)
            turned = jnp.where(fix[0:8], pltpu.roll(other, HALF, 1), turned)
            edge = last_ref[0:8, :] * edge + last_ref[8:16, :] * turned
            edge = jnp.concatenate([edge] * 8, axis=0)
            cosine = jnp.where(row == 0, even * x_one, cosine)
            sine = jnp.where(row == 0, edge, sine)
            special = (cosine * cosine + sine * sine)[0:8]
        total = total + (cosine * cosine + sine * sine)
        data_ref[upper, :] = cosine
        data_ref[lower, :] = sine
    special = jnp.where(iota((8, LANES), 0) == 0, special, 0.0)
    energy = jnp.sum(total, axis=0, keepdims=True) + jnp.sum(special, axis=0, keepdims=True)
    energy = 0.5 * energy / weight[0:1]

    values = []
    for (_, first, count), refs in zip(CLASSES, table):
        values.append(from_left(*refs, data_ref[LANES * first : LANES * (first + count), :]))
    for r, value in enumerate(back(values, 0)):
        for part in range(4):
            out_ref[4 * r + part, 0:ROWS, :] = value[ROWS * part : ROWS * (part + 1)]
    for s in range(DEV):
        out_ref[s, ROWS : ROWS + 1, :] = out_ref[(s - 1) % DEV, ROWS - 1 : ROWS, :]
        out_ref[s, ROWS + 1 : ROWS + 2, :] = out_ref[(s + 1) % DEV, 0:1, :]
        out_ref[s, ROWS + 2 : ROWS + 3, :] = energy
        out_ref[s, ROWS + 3 : BLOCK, :] = jnp.zeros((BLOCK - ROWS - 3, LANES), jnp.float32)
    for index in range(8):
        keep_ref[index] = out_ref[other_chip(device, index)]
        send_ref[index] = out_ref[other_chip(device ^ 4, index)]


def row_pass(device, one, g, sample, frequency, factors):
    out = [jax.ShapeDtypeStruct((8, BLOCK, LANES), jnp.float32)] * 2
    scratch = [
        pltpu.VMEM((4, INNER, LANES), jnp.float32),
        pltpu.VMEM((N, LANES), jnp.float32),
        pltpu.VMEM((N, LANES), jnp.float32),
        pltpu.VMEM((DEV, BLOCK, LANES), jnp.float32),
    ]
    specs = [pl.BlockSpec(memory_space=pltpu.SMEM)] + [pl.BlockSpec(memory_space=pltpu.VMEM)] * 32
    run = call(rows_kernel, out, scratch, LIMIT[3], 3 * 10**9, specs)
    return run(device, one, *g, *sample, *frequency, *factors)


def peaks_kernel(bins_ref, device_ref, *refs):
    got, table, offsets_ref, refs = refs[:8], pairs(refs[8:18]), refs[18], refs[19:]
    snr_ref, heights_ref, counts_ref, field_ref, wide_ref, side_ref, pick_ref, x_ref, own_ref, sem = refs
    for index in range(8):
        there = other_chip(device_ref[0], (index & 4) | (-index & 3))
        x_ref[there] = got[index][0]
        x_ref[there ^ 4] = got[index][1]

    def block(first, count):
        body = jnp.concatenate([x_ref[s] for s in range(first, first + count)], axis=1)
        pad = jnp.zeros((8, body.shape[1]), jnp.float32)
        return jnp.concatenate([body, pad], axis=0)

    values = []
    for (_, first, count), pair in zip(CLASSES, table):
        values.append(from_right(block(first, count), *pair))
    energy = x_ref[0, ROWS : BLOCK, :]
    for s in range(1, DEV):
        energy = energy + x_ref[s, ROWS : BLOCK, :]
    mean = jnp.sum(energy[2:3, :], axis=1, keepdims=True)
    inverse = 1.0 / jnp.sqrt(mean + 1e-06)
    for c, value in enumerate(back(values, 1)):
        cols = pl.ds(INNER * c, INNER)
        own_ref[:, cols] = value[0:ROWS] * inverse
        field_ref[8 : ROWS + 8, cols] = value[0:ROWS]
        field_ref[7:8, cols] = value[ROWS : ROWS + 1]
        field_ref[ROWS + 8 : ROWS + 9, cols] = value[ROWS + 1 : ROWS + 2]
    for start in (0,) + tuple(range(8, ROWS + 8, 16)) + (ROWS + 8,):
        size = 8 if start in (0, ROWS + 8) else 16
        value = field_ref[start : start + size, :]
        side = jnp.maximum(pltpu.roll(value, 1, 1), pltpu.roll(value, N - 1, 1))
        wide_ref[start : start + size, :] = jnp.maximum(side, value)
        side_ref[start : start + size, :] = side
    copy = pltpu.make_async_copy(own_ref, snr_ref, sem.at[0])
    copy.start()
    blocks = lax.shift_right_logical(iota((LANES, N), 1), 4) == iota((LANES, N), 0)
    blocks = jnp.where(blocks, 1.0, 0.0).astype(jnp.bfloat16)
    offsets = offsets_ref[...].astype(jnp.float32).astype(jnp.bfloat16)
    offsets = jnp.concatenate([offsets, offsets], axis=0)
    spread = jnp.dot(offsets, blocks, preferred_element_type=jnp.float32)
    code = (iota((CELL, N), 0) * CELL + (iota((CELL, N), 1) & (CELL - 1))).astype(jnp.float32)
    for p in range(ROWS // CELL):
        base = 8 + CELL * p
        value, side = field_ref[base : base + CELL, :], side_ref[base : base + CELL, :]
        above = wide_ref[base - 1 : base - 1 + CELL, :]
        below = wide_ref[base + 1 : base + 1 + CELL, :]
        nearest = jnp.maximum(side, jnp.maximum(above, below))
        chosen = spread[p : p + 1, :] == code
        height = jnp.where(chosen, value - nearest, 0.0)
        level = jnp.where(chosen, value, 0.0)
        pick_ref[8 * p : 8 * p + 8, :] = height[0:8] + height[8:16]
        pick_ref[HALF + 8 * p : HALF + 8 * p + 8, :] = level[0:8] + level[8:16]
    high, low = split(pick_ref[...])
    gather = partial(
        lax.dot_general,
        dimension_numbers=(((1,), (1,)), ((), ())),
        preferred_element_type=jnp.float32,
    )
    both = gather(jnp.concatenate([high, low], axis=0), blocks)
    both = both[0:LANES] + both[LANES : 2 * LANES]
    rows = [jnp.sum(both[8 * p : 8 * p + 8], axis=0, keepdims=True) for p in range(16)]
    picked = jnp.concatenate(rows, axis=0) * inverse
    heights, values = picked[0:8], picked[8:16]
    heights_ref[...] = heights
    weight = jax.nn.sigmoid(heights * 20.0)
    lane = iota((1, LANES), 1)
    counts = jnp.zeros((1, LANES), jnp.float32)
    for k in range(16):
        level = 0.25 * bins_ref[0, k].astype(jnp.float32)
        above = weight * jax.nn.sigmoid((values - level) * 10.0)
        summed = jnp.sum(jnp.sum(above, axis=0, keepdims=True), axis=1, keepdims=True)
        counts = counts + jnp.where(lane == k, summed, 0.0)
    for s in range(DEV):
        counts_ref[s] = jnp.broadcast_to(counts, (8, LANES))
    copy.wait()


def peak_pass(thresholds, device, x, table, offsets):
    f32 = jnp.float32
    out = [
        jax.ShapeDtypeStruct((ROWS, N), f32),
        jax.ShapeDtypeStruct((8, LANES), f32),
        jax.ShapeDtypeStruct((DEV, 8, LANES), f32),
    ]
    scratch = [
        pltpu.VMEM((ROWS + 16, N), f32),
        pltpu.VMEM((ROWS + 16, N), f32),
        pltpu.VMEM((ROWS + 16, N), f32),
        pltpu.VMEM((LANES, N), f32),
        pltpu.VMEM((DEV, BLOCK, LANES), f32),
        pltpu.VMEM((ROWS, N), f32),
        pltpu.SemaphoreType.DMA((1,)),
    ]
    specs = [pl.BlockSpec(memory_space=pltpu.SMEM)] * 2 + [pl.BlockSpec(memory_space=pltpu.VMEM)] * 19
    places = [pl.BlockSpec(memory_space=pl.ANY)] + [pl.BlockSpec(memory_space=pltpu.VMEM)] * 2
    run = call(peaks_kernel, out, scratch, LIMIT[4], 2 * 10**9, specs, places)
    return run(thresholds, device, *x, *table, offsets)


def chip_pairs(index):
    return [(d, other_chip(d, index)) for d in range(DEV)]


def body(shear, smoothing, offsets, thresholds):
    group = ("row", "col")
    device = lax.axis_index(group).astype(jnp.int32).reshape(1)

    def exchange(x):
        return lax.all_to_all(x, group, split_axis=0, concat_axis=0, tiled=True)

    def scatter(keep, send):
        got = lax.ppermute(send, group, [(d, d ^ 4) for d in range(DEV)])
        blocks = merge(keep, got)
        done = [blocks[0]]
        for index in ORDER:
            done.append((index, lax.ppermute(blocks[index], group, chip_pairs(index))))
        return [blocks[0]] + [value for _, value in sorted(done[1:], key=lambda item: item[0])]

    blocks = pack(device, shear)
    fields = []
    for field in range(2):
        got = [blocks[4 * field], None, None, None]
        for step in (2, 1, 3):
            got[4 - step] = lax.ppermute(blocks[4 * field + step], group, chip_pairs(step))
        fields.append(got)
    sample, frequency, factors = tables(smoothing, device)
    g = columns(device, fields[0], sample)
    one = scatter(*g)
    g = columns(device, fields[1], sample)
    two = scatter(*g)
    one = first_pass(device, one, frequency)
    k = row_pass(device, one, two, sample, frequency, factors)
    out = peak_pass(thresholds, device, scatter(*k), frequency, offsets[0])
    snr, heights, counts = out
    counts = exchange(counts)
    return snr[None], heights[None], jnp.sum(counts[:, 0:1, 0:16], axis=0)


def solution(mesh):
    return jax.shard_map(
        body,
        mesh=mesh,
        in_specs=(
            P(None, "maps", "row", "col"),
            P("maps"),
            P("maps", ("row", "col"), None),
            P("maps", None),
        ),
        out_specs=(
            P("maps", ("row", "col"), None),
            P("maps", ("row", "col"), None),
            P("maps", None),
        ),
        check_vma=False,
    )
```

```python
from functools import partial
import math

import jax
import jax.numpy as jnp
from jax import lax
from jax.experimental import pallas as pl
from jax.experimental.pallas import tpu as pltpu
from jax.sharding import PartitionSpec as P


N = 2048
INNER = 512
DENSE = 256
DEV = 16
ROWS = 128
LANES = 128
HALF = 64
CELL = 16
BLOCK = ROWS + 8
CLASSES = ((0, 0, 2), (4, 2, 2), (2, 4, 4), (1, 8, 4), (3, 12, 4))
ROOT = math.sqrt(0.5)
MIB = 1 << 20
LIMIT = (20, 24, 24, 36, 32)
ORDER = (6, 5, 7, 4, 2, 1, 3)


def call(kernel, out, scratch, limit, flops, ins, outs=None):
    return pl.pallas_call(
        kernel,
        out_shape=out,
        in_specs=ins,
        **({} if outs is None else {"out_specs": outs}),
        scratch_shapes=scratch,
        compiler_params=pltpu.CompilerParams(vmem_limit_bytes=limit * MIB),
        cost_estimate=pl.CostEstimate(flops=flops, bytes_accessed=4 * MIB, transcendentals=0),
    )


def split(x):
    high = x.astype(jnp.bfloat16)
    return high, (x - high.astype(jnp.float32)).astype(jnp.bfloat16)


def dot(left, right):
    return jnp.dot(left, right, preferred_element_type=jnp.float32)


def from_left(high_ref, low_ref, x):
    high, low = split(x)
    width = x.shape[1]
    both = dot(high_ref[...], jnp.concatenate([high, low], axis=1))
    return both[:, :width] + (both[:, width:] + dot(low_ref[...], high))


def from_right(x, high_ref, low_ref):
    high, low = split(x)
    height = x.shape[0]
    both = dot(jnp.concatenate([high, low], axis=0), high_ref[...])
    return both[:height] + (both[height:] + dot(high, low_ref[...]))


def pairs(refs):
    return tuple(zip(refs[0::2], refs[1::2]))


def take(x, start, size, axis):
    return lax.slice_in_dim(x, start, start + size, axis=axis)


def front(zero, two, even, odd, axis):
    near = [take(x, 0, DENSE, axis) for x in (zero, two, even, odd)]
    far = [take(x, DENSE, DENSE, axis) for x in (zero, two, even, odd)]
    change, total = ROOT * (far[2] - far[3]), ROOT * (far[2] + far[3])
    join = partial(jnp.concatenate, axis=axis)
    return (
        near[0] + far[0],
        near[0] - far[0],
        join([near[1], -far[1]]),
        join([near[2] + change, -near[3] - total]),
        join([near[2] - change, near[3] - total]),
    )


def back(values, axis):
    first, second, turn, one, three = values
    real = [take(x, 0, DENSE, axis) for x in (turn, one, three)]
    imag = [take(x, DENSE, DENSE, axis) for x in (turn, one, three)]
    change, total = real[1] - real[2], -imag[1] - imag[2]
    halves = (
        (first + second, real[0], real[1] + real[2], imag[2] - imag[1]),
        (first - second, -imag[0], ROOT * (total + change), ROOT * (total - change)),
    )
    blocks = []
    for zero, two, even, odd in halves:
        plus, minus = zero + two, zero - two
        blocks.append((plus + even, minus + odd, plus - even, minus - odd))
    return [jnp.concatenate([near, far], axis=axis) for near, far in zip(*blocks)]


def angle(steps):
    wrapped = jnp.bitwise_and(steps, N - 1)
    wrapped = jnp.where(wrapped >= N // 2, wrapped - N, wrapped)
    return wrapped.astype(jnp.float32) * (2.0 * math.pi / N)


def iota(shape, dim):
    return lax.broadcasted_iota(jnp.int32, shape, dim)


def put(high_ref, low_ref, rows, cols, value):
    high, low = split(value)
    high_ref[rows, cols] = high
    low_ref[rows, cols] = low


def sample_form(refs, scratch):
    cos_ref, sin_ref = scratch
    for (start, _, blocks), (high_ref, low_ref) in zip(CLASSES, refs):
        width = LANES * blocks
        col = iota((HALF, width), 1)
        freq = start + 8 * (HALF * (col // LANES) + col % HALF)
        quarter = jnp.where(col % LANES >= HALF, 1, 0)
        if start == 0:
            freq = jnp.where(col == HALF, N // 2, freq)
            quarter = jnp.where(col == HALF, 0, quarter)
        fine = angle(freq * iota((HALF, width), 0))
        cos_ref[:, :width] = jnp.cos(fine)
        sin_ref[:, :width] = jnp.sin(fine)
        coarse = angle(freq[:8] * (HALF * iota((8, width), 0)) + INNER * quarter[:8])
        cos_high, sin_high = jnp.cos(coarse), jnp.sin(coarse)
        for part in range(DENSE // HALF):
            cos_part, sin_part = cos_high[part : part + 1], sin_high[part : part + 1]
            rows = pl.ds(HALF * part, HALF)
            cos_fine, sin_fine = cos_ref[:, :width], sin_ref[:, :width]
            put(high_ref, low_ref, rows, slice(None), cos_part * cos_fine - sin_part * sin_fine)
            if blocks == 4:
                rows = pl.ds(DENSE + HALF * part, HALF)
                value = sin_part * cos_fine + cos_part * sin_fine
                put(high_ref, low_ref, rows, slice(None), value)


def frequency_form(refs, scratch):
    cos_ref, sin_ref = scratch
    fine = angle(8 * iota((HALF, DENSE), 0) * iota((HALF, DENSE), 1))
    cos_ref[:, :DENSE] = jnp.cos(fine)
    sin_ref[:, :DENSE] = jnp.sin(fine)
    for (start, _, blocks), (high_ref, low_ref) in zip(CLASSES, refs):
        coarse = angle((start + 8 * HALF * iota((8, DENSE), 0)) * iota((8, DENSE), 1))
        cos_high, sin_high = jnp.cos(coarse), jnp.sin(coarse)
        for part in range(blocks):
            cos_part, sin_part = cos_high[part : part + 1], sin_high[part : part + 1]
            cos_fine, sin_fine = cos_ref[:, :DENSE], sin_ref[:, :DENSE]
            cosine = cos_part * cos_fine - sin_part * sin_fine
            sine = sin_part * cos_fine + cos_part * sin_fine
            turned = -sine
            if start == 0 and part == 0:
                flip = (1 - 2 * (iota((HALF, DENSE), 1) & 1)).astype(jnp.float32)
                turned = jnp.where(iota((HALF, DENSE), 0) == 0, flip, turned)
            upper, lower = pl.ds(LANES * part, HALF), pl.ds(LANES * part + HALF, HALF)
            put(high_ref, low_ref, upper, pl.ds(0, DENSE), cosine)
            put(high_ref, low_ref, lower, pl.ds(0, DENSE), turned)
            if blocks == 4:
                put(high_ref, low_ref, upper, pl.ds(DENSE, DENSE), sine)
                put(high_ref, low_ref, lower, pl.ds(DENSE, DENSE), cosine)


def signed(freq):
    return jnp.where(freq < N // 2, freq, freq - N)


def lane_frequency(device, shape):
    lane = iota(shape, 1)
    block = jnp.where(device < 4, device & 1, device & 3)
    start = jnp.where(device < 2, 0, jnp.where(device < 4, 4, 2))
    start = jnp.where(device < 8, start, jnp.where(device < 12, 1, 3))
    freq = signed(start + 8 * (HALF * block + lane % HALF))
    nyquist = (device == 0) & (lane == HALF)
    freq = jnp.where(nyquist, -(N // 2), freq)
    single = nyquist | ((device == 0) & (lane == 0))
    return freq.astype(jnp.float32), jnp.where(single, 1.0, 2.0)


def tables_kernel(smooth_ref, device_ref, *refs):
    device = device_ref[0]
    scratch = refs[-2:]
    w_refs, f_refs = pairs(refs[0:10]), pairs(refs[10:20])
    even_ref, odd_ref, last_ref = refs[20:23]
    sample_form(w_refs, scratch)
    frequency_form(f_refs, scratch)
    width = smooth_ref[0]
    decay = width * width * (-2.0 * math.pi**2 / (N * N))
    shape = (HALF, LANES)
    freq_y, weight = lane_frequency(device, shape)

    def factors(freq_x, weight):
        total = freq_x * freq_x + freq_y * freq_y
        scaled = jnp.exp(decay * total) * weight / jnp.maximum(total, 1.0)
        return (freq_x * freq_x - freq_y * freq_y) * scaled, 2.0 * freq_x * freq_y * scaled

    for start, first, blocks in CLASSES:
        for part in range(blocks):
            freq = signed(start + 8 * (HALF * part + iota(shape, 0)))
            row_weight = jnp.where(freq == 0, 1.0, 2.0) * (1.0 / (N * N))
            even, odd = factors(freq.astype(jnp.float32), weight * row_weight)
            rows = pl.ds(HALF * (first + part), HALF)
            even_ref[rows, :] = even
            odd_ref[rows, :] = odd
    even, odd = factors(jnp.full(shape, -N / 2, jnp.float32), weight * (1.0 / (N * N)))
    last_ref[0:8, :] = even[0:8]
    last_ref[8:16, :] = odd[0:8]


def tables(smoothing, device):
    low = jnp.bfloat16
    table = []
    for _, _, blocks in CLASSES:
        table += [jax.ShapeDtypeStruct((LANES * blocks, LANES * blocks), low)] * 2
    out = table + table + [
        jax.ShapeDtypeStruct((N // 2, LANES), jnp.float32),
        jax.ShapeDtypeStruct((N // 2, LANES), jnp.float32),
        jax.ShapeDtypeStruct((16, LANES), jnp.float32),
    ]
    scratch = [pltpu.VMEM((HALF, INNER), jnp.float32)] * 2
    smem = pl.BlockSpec(memory_space=pltpu.SMEM)
    result = call(tables_kernel, out, scratch, LIMIT[0], 10**9, [smem, smem])(smoothing, device)
    return result[0:10], result[10:20], result[20:23]


def quarters(blocks):
    first, second, third, fourth = blocks
    return (
        (first + third) + (second + fourth),
        (first + third) - (second + fourth),
        first - third,
        second - fourth,
    )


def pack_kernel(device_ref, x_ref, *outs):
    for index in range(8):
        start = pl.multiple_of(((device_ref[0] + index) & 3) * ROWS, ROWS)
        outs[index][...] = x_ref[index // 4, 0, pl.ds(start, ROWS), :]


def pack(device, shear):
    out = [jax.ShapeDtypeStruct((ROWS, INNER), jnp.float32)] * 8
    specs = [pl.BlockSpec(memory_space=pltpu.SMEM), pl.BlockSpec(memory_space=pltpu.VMEM)]
    return call(pack_kernel, out, (), LIMIT[1], 10**6, specs)(device, shear)


def columns_kernel(device_ref, *refs):
    blocks, table = refs[:4], pairs(refs[4:14])
    keep_ref, send_ref, all_ref = refs[14:]
    zero, two, even, odd = quarters([x[...] for x in blocks])
    device = device_ref[0]
    place = device & 3
    along = jnp.where(place == 0, 1.0, jnp.where(place == 2, -1.0, 0.0))
    across = jnp.where(place == 1, 1.0, jnp.where(place == 3, -1.0, 0.0))
    flip = jnp.where((place & 1) == 0, 1.0, -1.0)

    even, odd = along * even - across * odd, across * even + along * odd
    operands = front(zero, flip * two, even, odd, 1)
    for (_, first, count), operand, refs in zip(CLASSES, operands, table):
        value = from_right(operand, *refs)
        for part in range(count):
            all_ref[first + part] = value[:, LANES * part : LANES * (part + 1)]
    for index in range(8):
        there = other_chip(device, index)
        keep_ref[index] = all_ref[there]
        send_ref[index] = all_ref[there ^ 4]


def other_chip(device, index):
    return ((device & 12) ^ (2 * (index & 4))) + ((device + index) & 3)


def columns(device, blocks, table):
    out = [jax.ShapeDtypeStruct((8, ROWS, LANES), jnp.float32)] * 2
    specs = [pl.BlockSpec(memory_space=pltpu.SMEM)] + [pl.BlockSpec(memory_space=pltpu.VMEM)] * 14
    scratch = [pltpu.VMEM((DEV, ROWS, LANES), jnp.float32)]
    return call(columns_kernel, out, scratch, LIMIT[1], 2 * 10**9, specs)(device, *blocks, *table)


def merge_kernel(keep_ref, got_ref, *outs):
    for index in range(8):
        outs[index][0] = keep_ref[index]
        outs[index][1] = got_ref[index]


def merge(keep, got):
    out = [jax.ShapeDtypeStruct((2,) + keep.shape[1:], jnp.float32)] * 8
    specs = [pl.BlockSpec(memory_space=pltpu.VMEM)] * 2
    return call(merge_kernel, out, (), 8, 10**8, specs)(keep, got)


def to_frequency(device, g_refs, f_refs, part_ref, out_ref):
    flip_core = jnp.where((device & 4) == 0, 1.0, -1.0)
    flip_chip = jnp.where((device & 8) == 0, 1.0, -1.0)
    for step in range(4):
        near, far = g_refs[step], g_refs[4 + step]
        same, other = near[0] + far[0], near[1] + far[1]
        rows = pl.ds(pl.multiple_of(((device - step) & 3) * ROWS, ROWS), ROWS)
        part_ref[0, rows, :] = same + other
        part_ref[1, rows, :] = flip_core * (same - other)
        same, other = flip_chip * (near[0] - far[0]), flip_chip * (near[1] - far[1])
        part_ref[2, rows, :] = jnp.where(flip_core > 0, same, other)
        part_ref[3, rows, :] = jnp.where(flip_core > 0, other, same)
    operands = front(*[part_ref[i] for i in range(4)], 0)
    for (_, first, count), operand, refs in zip(CLASSES, operands, f_refs):
        out_ref[LANES * first : LANES * (first + count), :] = from_left(*refs, operand)


def first_kernel(device_ref, *refs):
    to_frequency(device_ref[0], refs[:8], pairs(refs[8:18]), refs[19], refs[18])


def first_pass(device, g, frequency):
    out = jax.ShapeDtypeStruct((N, LANES), jnp.float32)
    specs = [pl.BlockSpec(memory_space=pltpu.SMEM)] + [pl.BlockSpec(memory_space=pltpu.VMEM)] * 18
    scratch = [pltpu.VMEM((4, INNER, LANES), jnp.float32)]
    return call(first_kernel, out, scratch, LIMIT[2], 10**9, specs)(device, *g, *frequency)


def rows_kernel(device_ref, one_ref, *refs):
    g_refs, refs = refs[:8], refs[8:]
    table = pairs(refs[:10])
    even_ref, odd_ref, last_ref, keep_ref, send_ref, part_ref, two_ref, data_ref, out_ref = refs[20:]
    device = device_ref[0]
    to_frequency(device, g_refs, pairs(refs[10:20]), part_ref, two_ref)
    _, weight = lane_frequency(device, (8, LANES))
    total = jnp.zeros((HALF, LANES), jnp.float32)
    special = jnp.zeros((8, LANES), jnp.float32)
    row, lane = iota((HALF, LANES), 0), iota((HALF, LANES), 1)
    sign = jnp.where(lane < HALF, 1.0, -1.0)
    fix = (lane == HALF) & (device == 0)
    for part in range(DEV):
        upper, lower = pl.ds(LANES * part, HALF), pl.ds(LANES * part + HALF, HALF)
        x_one, x_two = one_ref[upper, :], two_ref[upper, :]
        y_one, y_two = one_ref[lower, :], two_ref[lower, :]
        x_two = jnp.where(fix, -x_one, sign * pltpu.roll(x_two, HALF, 1))
        y_two = jnp.where(fix, -y_one, sign * pltpu.roll(y_two, HALF, 1))
        rows = pl.ds(HALF * part, HALF)
        even, odd = even_ref[rows, :], odd_ref[rows, :]
        cosine = even * x_one - odd * y_two
        sine = even * y_one + odd * x_two
        if part == 0:
            edge, other = y_one[0:8], y_two[0:8]
            turned = sign[0:8] * pltpu.roll(edge, HALF, 1)
            turned = jnp.where(fix[0:8], pltpu.roll(other, HALF, 1), turned)
            edge = last_ref[0:8, :] * edge + last_ref[8:16, :] * turned
            edge = jnp.concatenate([edge] * 8, axis=0)
            cosine = jnp.where(row == 0, even * x_one, cosine)
            sine = jnp.where(row == 0, edge, sine)
            special = (cosine * cosine + sine * sine)[0:8]
        total = total + (cosine * cosine + sine * sine)
        data_ref[upper, :] = cosine
        data_ref[lower, :] = sine
    special = jnp.where(iota((8, LANES), 0) == 0, special, 0.0)
    energy = jnp.sum(total, axis=0, keepdims=True) + jnp.sum(special, axis=0, keepdims=True)
    energy = 0.5 * energy / weight[0:1]

    values = []
    for (_, first, count), refs in zip(CLASSES, table):
        values.append(from_left(*refs, data_ref[LANES * first : LANES * (first + count), :]))
    for r, value in enumerate(back(values, 0)):
        for part in range(4):
            out_ref[4 * r + part, 0:ROWS, :] = value[ROWS * part : ROWS * (part + 1)]
    for s in range(DEV):
        out_ref[s, ROWS : ROWS + 1, :] = out_ref[(s - 1) % DEV, ROWS - 1 : ROWS, :]
        out_ref[s, ROWS + 1 : ROWS + 2, :] = out_ref[(s + 1) % DEV, 0:1, :]
        out_ref[s, ROWS + 2 : ROWS + 3, :] = energy
        out_ref[s, ROWS + 3 : BLOCK, :] = jnp.zeros((BLOCK - ROWS - 3, LANES), jnp.float32)
    for index in range(8):
        there = other_chip(device, index)
        keep_ref[index] = out_ref[there]
        send_ref[index] = out_ref[there ^ 4]


def row_pass(device, one, g, sample, frequency, factors):
    out = [jax.ShapeDtypeStruct((8, BLOCK, LANES), jnp.float32)] * 2
    scratch = [
        pltpu.VMEM((4, INNER, LANES), jnp.float32),
        pltpu.VMEM((N, LANES), jnp.float32),
        pltpu.VMEM((N, LANES), jnp.float32),
        pltpu.VMEM((DEV, BLOCK, LANES), jnp.float32),
    ]
    specs = [pl.BlockSpec(memory_space=pltpu.SMEM)] + [pl.BlockSpec(memory_space=pltpu.VMEM)] * 32
    run = call(rows_kernel, out, scratch, LIMIT[3], 3 * 10**9, specs)
    return run(device, one, *g, *sample, *frequency, *factors)


def peaks_kernel(bins_ref, device_ref, *refs):
    got, table, offsets_ref, refs = refs[:8], pairs(refs[8:18]), refs[18], refs[19:]
    snr_ref, heights_ref, counts_ref, field_ref, wide_ref, side_ref, pick_ref, x_ref, own_ref, sem = refs
    for index in range(8):
        there = other_chip(device_ref[0], (index & 4) | (-index & 3))
        x_ref[there] = got[index][0]
        x_ref[there ^ 4] = got[index][1]

    def block(first, count):
        body = jnp.concatenate([x_ref[s] for s in range(first, first + count)], axis=1)
        pad = jnp.zeros((8, body.shape[1]), jnp.float32)
        return jnp.concatenate([body, pad], axis=0)

    values = []
    for (_, first, count), pair in zip(CLASSES, table):
        values.append(from_right(block(first, count), *pair))
    energy = x_ref[0, ROWS : BLOCK, :]
    for s in range(1, DEV):
        energy = energy + x_ref[s, ROWS : BLOCK, :]
    mean = jnp.sum(energy[2:3, :], axis=1, keepdims=True)
    inverse = 1.0 / jnp.sqrt(mean + 1e-06)
    for c, value in enumerate(back(values, 1)):
        cols = pl.ds(INNER * c, INNER)
        own_ref[:, cols] = value[0:ROWS] * inverse
        field_ref[8 : ROWS + 8, cols] = value[0:ROWS]
        field_ref[7:8, cols] = value[ROWS : ROWS + 1]
        field_ref[ROWS + 8 : ROWS + 9, cols] = value[ROWS + 1 : ROWS + 2]
    for start in (0,) + tuple(range(8, ROWS + 8, 16)) + (ROWS + 8,):
        size = 8 if start in (0, ROWS + 8) else 16
        value = field_ref[start : start + size, :]
        side = jnp.maximum(pltpu.roll(value, 1, 1), pltpu.roll(value, N - 1, 1))
        wide_ref[start : start + size, :] = jnp.maximum(side, value)
        side_ref[start : start + size, :] = side
    copies = []
    for part in range(8):
        rows = pl.ds(CELL * part, CELL)
        copies.append(pltpu.make_async_copy(own_ref.at[rows], snr_ref.at[rows], sem.at[part]))
        copies[-1].start()
    blocks = lax.shift_right_logical(iota((LANES, N), 1), 4) == iota((LANES, N), 0)
    blocks = jnp.where(blocks, 1.0, 0.0).astype(jnp.bfloat16)
    offsets = offsets_ref[...].astype(jnp.float32).astype(jnp.bfloat16)
    offsets = jnp.concatenate([offsets, offsets], axis=0)
    spread = jnp.dot(offsets, blocks, preferred_element_type=jnp.float32)
    code = (iota((CELL, N), 0) * CELL + (iota((CELL, N), 1) & (CELL - 1))).astype(jnp.float32)
    for p in range(ROWS // CELL):
        base = 8 + CELL * p
        value, side = field_ref[base : base + CELL, :], side_ref[base : base + CELL, :]
        above = wide_ref[base - 1 : base - 1 + CELL, :]
        below = wide_ref[base + 1 : base + 1 + CELL, :]
        nearest = jnp.maximum(side, jnp.maximum(above, below))
        chosen = spread[p : p + 1, :] == code
        height = jnp.where(chosen, value - nearest, 0.0)
        level = jnp.where(chosen, value, 0.0)
        pick_ref[8 * p : 8 * p + 8, :] = height[0:8] + height[8:16]
        pick_ref[HALF + 8 * p : HALF + 8 * p + 8, :] = level[0:8] + level[8:16]
    high, low = split(pick_ref[...])
    gather = partial(
        lax.dot_general,
        dimension_numbers=(((1,), (1,)), ((), ())),
        preferred_element_type=jnp.float32,
    )
    both = gather(jnp.concatenate([high, low], axis=0), blocks)
    both = both[0:LANES] + both[LANES : 2 * LANES]
    rows = [jnp.sum(both[8 * p : 8 * p + 8], axis=0, keepdims=True) for p in range(16)]
    picked = jnp.concatenate(rows, axis=0) * inverse
    heights, values = picked[0:8], picked[8:16]
    heights_ref[...] = heights
    weight = jax.nn.sigmoid(heights * 20.0)
    lane = iota((1, LANES), 1)
    counts = jnp.zeros((1, LANES), jnp.float32)
    for k in range(16):
        level = 0.25 * bins_ref[0, k].astype(jnp.float32)
        above = weight * jax.nn.sigmoid((values - level) * 10.0)
        summed = jnp.sum(jnp.sum(above, axis=0, keepdims=True), axis=1, keepdims=True)
        counts = counts + jnp.where(lane == k, summed, 0.0)
    for s in range(DEV):
        counts_ref[s] = jnp.broadcast_to(counts, (8, LANES))
    for copy in copies:
        copy.wait()


def peak_pass(thresholds, device, x, table, offsets):
    f32 = jnp.float32
    out = [
        jax.ShapeDtypeStruct((ROWS, N), f32),
        jax.ShapeDtypeStruct((8, LANES), f32),
        jax.ShapeDtypeStruct((DEV, 8, LANES), f32),
    ]
    scratch = [
        pltpu.VMEM((ROWS + 16, N), f32),
        pltpu.VMEM((ROWS + 16, N), f32),
        pltpu.VMEM((ROWS + 16, N), f32),
        pltpu.VMEM((LANES, N), f32),
        pltpu.VMEM((DEV, BLOCK, LANES), f32),
        pltpu.VMEM((ROWS, N), f32),
        pltpu.SemaphoreType.DMA((8,)),
    ]
    specs = [pl.BlockSpec(memory_space=pltpu.SMEM)] * 2 + [pl.BlockSpec(memory_space=pltpu.VMEM)] * 19
    places = [pl.BlockSpec(memory_space=pl.ANY)] + [pl.BlockSpec(memory_space=pltpu.VMEM)] * 2
    run = call(peaks_kernel, out, scratch, LIMIT[4], 2 * 10**9, specs, places)
    return run(thresholds, device, *x, *table, offsets)


def finish_kernel(counts_ref, heights_ref, total_ref, out_ref):
    total = counts_ref[0]
    for s in range(1, DEV):
        total = total + counts_ref[s]
    total_ref[...] = total[0:1, 0:16]
    out_ref[...] = heights_ref[...]


def finish(counts, heights):
    out = [
        jax.ShapeDtypeStruct((1, 16), jnp.float32),
        jax.ShapeDtypeStruct((8, LANES), jnp.float32),
    ]
    specs = [pl.BlockSpec(memory_space=pltpu.VMEM)] * 2
    return call(finish_kernel, out, (), 4, 10**6, specs)(counts, heights)


def chip_pairs(index):
    return [(d, (d & 12 ^ (2 * (index & 4))) + ((d + index) & 3)) for d in range(DEV)]


def body(shear, smoothing, offsets, thresholds):
    group = ("row", "col")
    device = lax.axis_index(group).astype(jnp.int32).reshape(1)

    def exchange(x):
        return lax.all_to_all(x, group, split_axis=0, concat_axis=0, tiled=True)

    def scatter(keep, send):
        got = lax.ppermute(send, group, [(d, d ^ 4) for d in range(DEV)])
        blocks = merge(keep, got)
        done = [blocks[0]]
        for index in ORDER:
            done.append((index, lax.ppermute(blocks[index], group, chip_pairs(index))))
        return [blocks[0]] + [value for _, value in sorted(done[1:], key=lambda item: item[0])]

    blocks = pack(device, shear)
    fields = []
    for field in range(2):
        got = [blocks[4 * field], None, None, None]
        for step in (2, 1, 3):
            pairs = [(c, (c + step) % 4) for c in range(4)]
            got[4 - step] = lax.ppermute(blocks[4 * field + step], "col", pairs)
        fields.append(got)
    sample, frequency, factors = tables(smoothing, device)
    g = columns(device, fields[0], sample)
    one = scatter(*g)
    g = columns(device, fields[1], sample)
    two = scatter(*g)
    one = first_pass(device, one, frequency)
    k = row_pass(device, one, two, sample, frequency, factors)
    out = peak_pass(thresholds, device, scatter(*k), frequency, offsets[0])
    snr, heights, counts = out
    counts, heights = finish(exchange(counts), heights)
    return snr[None], heights[None], counts


def solution(mesh):
    return jax.shard_map(
        body,
        mesh=mesh,
        in_specs=(
            P(None, "maps", "row", "col"),
            P("maps"),
            P("maps", ("row", "col"), None),
            P("maps", None),
        ),
        out_specs=(
            P("maps", ("row", "col"), None),
            P("maps", ("row", "col"), None),
            P("maps", None),
        ),
        check_vma=False,
    )
```

```python
from functools import partial
import math

import jax
import jax.numpy as jnp
from jax import lax
from jax.experimental import pallas as pl
from jax.experimental.pallas import tpu as pltpu
from jax.sharding import PartitionSpec as P


N = 2048
INNER = 512
DENSE = 256
DEV = 16
ROWS = 128
LANES = 128
HALF = 64
CELL = 16
BLOCK = ROWS + 8
CLASSES = ((0, 0, 2), (4, 2, 2), (2, 4, 4), (1, 8, 4), (3, 12, 4))
ROOT = math.sqrt(0.5)
MIB = 1 << 20
LIMIT = (20, 24, 24, 36, 32)
ORDER = (4, 5, 7, 2, 1, 3)


def call(kernel, out, scratch, limit, flops, ins, outs=None):
    return pl.pallas_call(
        kernel,
        out_shape=out,
        in_specs=ins,
        **({} if outs is None else {"out_specs": outs}),
        scratch_shapes=scratch,
        compiler_params=pltpu.CompilerParams(vmem_limit_bytes=limit * MIB),
        cost_estimate=pl.CostEstimate(flops=flops, bytes_accessed=4 * MIB, transcendentals=0),
    )


def split(x):
    high = x.astype(jnp.bfloat16)
    return high, (x - high.astype(jnp.float32)).astype(jnp.bfloat16)


def dot(left, right):
    return jnp.dot(left, right, preferred_element_type=jnp.float32)


def from_left(high_ref, low_ref, x):
    high, low = split(x)
    width = x.shape[1]
    both = dot(high_ref[...], jnp.concatenate([high, low], axis=1))
    return both[:, :width] + (both[:, width:] + dot(low_ref[...], high))


def from_right(x, high_ref, low_ref):
    high, low = split(x)
    height = x.shape[0]
    both = dot(jnp.concatenate([high, low], axis=0), high_ref[...])
    return both[:height] + (both[height:] + dot(high, low_ref[...]))


def pairs(refs):
    return tuple(zip(refs[0::2], refs[1::2]))


def take(x, start, size, axis):
    return lax.slice_in_dim(x, start, start + size, axis=axis)


def front(zero, two, even, odd, axis):
    near = [take(x, 0, DENSE, axis) for x in (zero, two, even, odd)]
    far = [take(x, DENSE, DENSE, axis) for x in (zero, two, even, odd)]
    change, total = ROOT * (far[2] - far[3]), ROOT * (far[2] + far[3])
    join = partial(jnp.concatenate, axis=axis)
    return (
        near[0] + far[0],
        near[0] - far[0],
        join([near[1], -far[1]]),
        join([near[2] + change, -near[3] - total]),
        join([near[2] - change, near[3] - total]),
    )


def back(values, axis):
    first, second, turn, one, three = values
    real = [take(x, 0, DENSE, axis) for x in (turn, one, three)]
    imag = [take(x, DENSE, DENSE, axis) for x in (turn, one, three)]
    change, total = real[1] - real[2], -imag[1] - imag[2]
    halves = (
        (first + second, real[0], real[1] + real[2], imag[2] - imag[1]),
        (first - second, -imag[0], ROOT * (total + change), ROOT * (total - change)),
    )
    blocks = []
    for zero, two, even, odd in halves:
        plus, minus = zero + two, zero - two
        blocks.append((plus + even, minus + odd, plus - even, minus - odd))
    return [jnp.concatenate([near, far], axis=axis) for near, far in zip(*blocks)]


def angle(steps):
    wrapped = jnp.bitwise_and(steps, N - 1)
    wrapped = jnp.where(wrapped >= N // 2, wrapped - N, wrapped)
    return wrapped.astype(jnp.float32) * (2.0 * math.pi / N)


def iota(shape, dim):
    return lax.broadcasted_iota(jnp.int32, shape, dim)


def put(high_ref, low_ref, rows, cols, value):
    high, low = split(value)
    high_ref[rows, cols] = high
    low_ref[rows, cols] = low


def sample_form(refs, scratch):
    cos_ref, sin_ref = scratch
    for (start, _, blocks), (high_ref, low_ref) in zip(CLASSES, refs):
        width = LANES * blocks
        col = iota((HALF, width), 1)
        freq = start + 8 * (HALF * (col // LANES) + col % HALF)
        quarter = jnp.where(col % LANES >= HALF, 1, 0)
        if start == 0:
            freq = jnp.where(col == HALF, N // 2, freq)
            quarter = jnp.where(col == HALF, 0, quarter)
        fine = angle(freq * iota((HALF, width), 0))
        cos_ref[:, :width] = jnp.cos(fine)
        sin_ref[:, :width] = jnp.sin(fine)
        coarse = angle(freq[:8] * (HALF * iota((8, width), 0)) + INNER * quarter[:8])
        cos_high, sin_high = jnp.cos(coarse), jnp.sin(coarse)
        for part in range(DENSE // HALF):
            cos_part, sin_part = cos_high[part : part + 1], sin_high[part : part + 1]
            rows = pl.ds(HALF * part, HALF)
            cos_fine, sin_fine = cos_ref[:, :width], sin_ref[:, :width]
            put(high_ref, low_ref, rows, slice(None), cos_part * cos_fine - sin_part * sin_fine)
            if blocks == 4:
                rows = pl.ds(DENSE + HALF * part, HALF)
                value = sin_part * cos_fine + cos_part * sin_fine
                put(high_ref, low_ref, rows, slice(None), value)


def frequency_form(refs, scratch):
    cos_ref, sin_ref = scratch
    fine = angle(8 * iota((HALF, DENSE), 0) * iota((HALF, DENSE), 1))
    cos_ref[:, :DENSE] = jnp.cos(fine)
    sin_ref[:, :DENSE] = jnp.sin(fine)
    for (start, _, blocks), (high_ref, low_ref) in zip(CLASSES, refs):
        coarse = angle((start + 8 * HALF * iota((8, DENSE), 0)) * iota((8, DENSE), 1))
        cos_high, sin_high = jnp.cos(coarse), jnp.sin(coarse)
        for part in range(blocks):
            cos_part, sin_part = cos_high[part : part + 1], sin_high[part : part + 1]
            cos_fine, sin_fine = cos_ref[:, :DENSE], sin_ref[:, :DENSE]
            cosine = cos_part * cos_fine - sin_part * sin_fine
            sine = sin_part * cos_fine + cos_part * sin_fine
            turned = -sine
            if start == 0 and part == 0:
                flip = (1 - 2 * (iota((HALF, DENSE), 1) & 1)).astype(jnp.float32)
                turned = jnp.where(iota((HALF, DENSE), 0) == 0, flip, turned)
            upper, lower = pl.ds(LANES * part, HALF), pl.ds(LANES * part + HALF, HALF)
            put(high_ref, low_ref, upper, pl.ds(0, DENSE), cosine)
            put(high_ref, low_ref, lower, pl.ds(0, DENSE), turned)
            if blocks == 4:
                put(high_ref, low_ref, upper, pl.ds(DENSE, DENSE), sine)
                put(high_ref, low_ref, lower, pl.ds(DENSE, DENSE), cosine)


def signed(freq):
    return jnp.where(freq < N // 2, freq, freq - N)


def lane_frequency(device, shape):
    lane = iota(shape, 1)
    block = jnp.where(device < 4, device & 1, device & 3)
    start = jnp.where(device < 2, 0, jnp.where(device < 4, 4, 2))
    start = jnp.where(device < 8, start, jnp.where(device < 12, 1, 3))
    freq = signed(start + 8 * (HALF * block + lane % HALF))
    nyquist = (device == 0) & (lane == HALF)
    freq = jnp.where(nyquist, -(N // 2), freq)
    single = nyquist | ((device == 0) & (lane == 0))
    return freq.astype(jnp.float32), jnp.where(single, 1.0, 2.0)


def tables_kernel(smooth_ref, device_ref, *refs):
    device = device_ref[0]
    scratch = refs[-2:]
    w_refs, f_refs = pairs(refs[0:10]), pairs(refs[10:20])
    even_ref, odd_ref, last_ref = refs[20:23]
    sample_form(w_refs, scratch)
    frequency_form(f_refs, scratch)
    width = smooth_ref[0]
    decay = width * width * (-2.0 * math.pi**2 / (N * N))
    shape = (HALF, LANES)
    freq_y, weight = lane_frequency(device, shape)

    def factors(freq_x, weight):
        total = freq_x * freq_x + freq_y * freq_y
        scaled = jnp.exp(decay * total) * weight / jnp.maximum(total, 1.0)
        return (freq_x * freq_x - freq_y * freq_y) * scaled, 2.0 * freq_x * freq_y * scaled

    for start, first, blocks in CLASSES:
        for part in range(blocks):
            freq = signed(start + 8 * (HALF * part + iota(shape, 0)))
            row_weight = jnp.where(freq == 0, 1.0, 2.0) * (1.0 / (N * N))
            even, odd = factors(freq.astype(jnp.float32), weight * row_weight)
            rows = pl.ds(HALF * (first + part), HALF)
            even_ref[rows, :] = even
            odd_ref[rows, :] = odd
    even, odd = factors(jnp.full(shape, -N / 2, jnp.float32), weight * (1.0 / (N * N)))
    last_ref[0:8, :] = even[0:8]
    last_ref[8:16, :] = odd[0:8]


def tables(smoothing, device):
    low = jnp.bfloat16
    table = []
    for _, _, blocks in CLASSES:
        table += [jax.ShapeDtypeStruct((LANES * blocks, LANES * blocks), low)] * 2
    out = table + table + [
        jax.ShapeDtypeStruct((N // 2, LANES), jnp.float32),
        jax.ShapeDtypeStruct((N // 2, LANES), jnp.float32),
        jax.ShapeDtypeStruct((16, LANES), jnp.float32),
    ]
    scratch = [pltpu.VMEM((HALF, INNER), jnp.float32)] * 2
    smem = pl.BlockSpec(memory_space=pltpu.SMEM)
    result = call(tables_kernel, out, scratch, LIMIT[0], 10**9, [smem, smem])(smoothing, device)
    return result[0:10], result[10:20], result[20:23]


def quarters(blocks):
    first, second, third, fourth = blocks
    return (
        (first + third) + (second + fourth),
        (first + third) - (second + fourth),
        first - third,
        second - fourth,
    )


def pack_kernel(device_ref, x_ref, *outs):
    for index in range(8):
        start = pl.multiple_of(((device_ref[0] + index) & 3) * ROWS, ROWS)
        outs[index][...] = x_ref[index // 4, 0, pl.ds(start, ROWS), :]


def pack(device, shear):
    out = [jax.ShapeDtypeStruct((ROWS, INNER), jnp.float32)] * 8
    specs = [pl.BlockSpec(memory_space=pltpu.SMEM), pl.BlockSpec(memory_space=pltpu.VMEM)]
    return call(pack_kernel, out, (), LIMIT[1], 10**6, specs)(device, shear)


def columns_kernel(device_ref, *refs):
    blocks, table = refs[:4], pairs(refs[4:14])
    keep_ref, send_ref, all_ref = refs[14:]
    zero, two, even, odd = quarters([x[...] for x in blocks])
    device = device_ref[0]
    place = device & 3
    along = jnp.where(place == 0, 1.0, jnp.where(place == 2, -1.0, 0.0))
    across = jnp.where(place == 1, 1.0, jnp.where(place == 3, -1.0, 0.0))
    flip = jnp.where((place & 1) == 0, 1.0, -1.0)

    even, odd = along * even - across * odd, across * even + along * odd
    operands = front(zero, flip * two, even, odd, 1)
    for (_, first, count), operand, refs in zip(CLASSES, operands, table):
        value = from_right(operand, *refs)
        for part in range(count):
            all_ref[first + part] = value[:, LANES * part : LANES * (part + 1)]
    for index in range(8):
        there = other_chip(device, index)
        keep_ref[index] = all_ref[there]
        send_ref[index] = all_ref[there ^ 4]


def other_chip(device, index):
    return ((device & 12) ^ (2 * (index & 4))) + ((device + index) & 3)


def columns(device, blocks, table):
    out = [jax.ShapeDtypeStruct((8, ROWS, LANES), jnp.float32)] * 2
    specs = [pl.BlockSpec(memory_space=pltpu.SMEM)] + [pl.BlockSpec(memory_space=pltpu.VMEM)] * 14
    scratch = [pltpu.VMEM((DEV, ROWS, LANES), jnp.float32)]
    return call(columns_kernel, out, scratch, LIMIT[1], 2 * 10**9, specs)(device, *blocks, *table)


def merge_kernel(keep_ref, got_ref, *outs):
    for index in range(8):
        out_ref = outs[(0, 1, 2, 3, 4, 5, 4, 6)[index]]
        first = 2 if index == 6 else 0
        out_ref[first] = keep_ref[index]
        out_ref[first + 1] = got_ref[index]


def relay_kernel(x_ref, out_ref):
    out_ref[...] = x_ref[2:4]


def relay(x):
    out = jax.ShapeDtypeStruct((2,) + x.shape[1:], jnp.float32)
    return call(relay_kernel, out, (), 8, 10**6, [pl.BlockSpec(memory_space=pltpu.VMEM)])(x)


def merge(keep, got):
    counts = (2, 2, 2, 2, 4, 2, 2)
    out = [jax.ShapeDtypeStruct((n,) + keep.shape[1:], jnp.float32) for n in counts]
    specs = [pl.BlockSpec(memory_space=pltpu.VMEM)] * 2
    return call(merge_kernel, out, (), 8, 10**8, specs)(keep, got)


def to_frequency(device, g_refs, f_refs, part_ref, out_ref):
    flip_core = jnp.where((device & 4) == 0, 1.0, -1.0)
    flip_chip = jnp.where((device & 8) == 0, 1.0, -1.0)
    for step in range(4):
        near, far = g_refs[step], g_refs[4 + step]
        same, other = near[0] + far[0], near[1] + far[1]
        rows = pl.ds(pl.multiple_of(((device - step) & 3) * ROWS, ROWS), ROWS)
        part_ref[0, rows, :] = same + other
        part_ref[1, rows, :] = flip_core * (same - other)
        same, other = flip_chip * (near[0] - far[0]), flip_chip * (near[1] - far[1])
        part_ref[2, rows, :] = jnp.where(flip_core > 0, same, other)
        part_ref[3, rows, :] = jnp.where(flip_core > 0, other, same)
    operands = front(*[part_ref[i] for i in range(4)], 0)
    for (_, first, count), operand, refs in zip(CLASSES, operands, f_refs):
        out_ref[LANES * first : LANES * (first + count), :] = from_left(*refs, operand)


def first_kernel(device_ref, *refs):
    to_frequency(device_ref[0], refs[:8], pairs(refs[8:18]), refs[19], refs[18])


def first_pass(device, g, frequency):
    out = jax.ShapeDtypeStruct((N, LANES), jnp.float32)
    specs = [pl.BlockSpec(memory_space=pltpu.SMEM)] + [pl.BlockSpec(memory_space=pltpu.VMEM)] * 18
    scratch = [pltpu.VMEM((4, INNER, LANES), jnp.float32)]
    return call(first_kernel, out, scratch, LIMIT[2], 10**9, specs)(device, *g, *frequency)


def rows_kernel(device_ref, one_ref, *refs):
    g_refs, refs = refs[:8], refs[8:]
    table = pairs(refs[:10])
    even_ref, odd_ref, last_ref, keep_ref, send_ref, part_ref, two_ref, data_ref, out_ref = refs[20:]
    device = device_ref[0]
    to_frequency(device, g_refs, pairs(refs[10:20]), part_ref, two_ref)
    _, weight = lane_frequency(device, (8, LANES))
    total = jnp.zeros((HALF, LANES), jnp.float32)
    special = jnp.zeros((8, LANES), jnp.float32)
    row, lane = iota((HALF, LANES), 0), iota((HALF, LANES), 1)
    sign = jnp.where(lane < HALF, 1.0, -1.0)
    fix = (lane == HALF) & (device == 0)
    for part in range(DEV):
        upper, lower = pl.ds(LANES * part, HALF), pl.ds(LANES * part + HALF, HALF)
        x_one, x_two = one_ref[upper, :], two_ref[upper, :]
        y_one, y_two = one_ref[lower, :], two_ref[lower, :]
        x_two = jnp.where(fix, -x_one, sign * pltpu.roll(x_two, HALF, 1))
        y_two = jnp.where(fix, -y_one, sign * pltpu.roll(y_two, HALF, 1))
        rows = pl.ds(HALF * part, HALF)
        even, odd = even_ref[rows, :], odd_ref[rows, :]
        cosine = even * x_one - odd * y_two
        sine = even * y_one + odd * x_two
        if part == 0:
            edge, other = y_one[0:8], y_two[0:8]
            turned = sign[0:8] * pltpu.roll(edge, HALF, 1)
            turned = jnp.where(fix[0:8], pltpu.roll(other, HALF, 1), turned)
            edge = last_ref[0:8, :] * edge + last_ref[8:16, :] * turned
            edge = jnp.concatenate([edge] * 8, axis=0)
            cosine = jnp.where(row == 0, even * x_one, cosine)
            sine = jnp.where(row == 0, edge, sine)
            special = (cosine * cosine + sine * sine)[0:8]
        total = total + (cosine * cosine + sine * sine)
        data_ref[upper, :] = cosine
        data_ref[lower, :] = sine
    special = jnp.where(iota((8, LANES), 0) == 0, special, 0.0)
    energy = jnp.sum(total, axis=0, keepdims=True) + jnp.sum(special, axis=0, keepdims=True)
    energy = 0.5 * energy / weight[0:1]

    values = []
    for (_, first, count), refs in zip(CLASSES, table):
        values.append(from_left(*refs, data_ref[LANES * first : LANES * (first + count), :]))
    for r, value in enumerate(back(values, 0)):
        for part in range(4):
            out_ref[4 * r + part, 0:ROWS, :] = value[ROWS * part : ROWS * (part + 1)]
    for s in range(DEV):
        out_ref[s, ROWS : ROWS + 1, :] = out_ref[(s - 1) % DEV, ROWS - 1 : ROWS, :]
        out_ref[s, ROWS + 1 : ROWS + 2, :] = out_ref[(s + 1) % DEV, 0:1, :]
        out_ref[s, ROWS + 2 : ROWS + 3, :] = energy
        out_ref[s, ROWS + 3 : BLOCK, :] = jnp.zeros((BLOCK - ROWS - 3, LANES), jnp.float32)
    for index in range(8):
        there = other_chip(device, index)
        keep_ref[index] = out_ref[there]
        send_ref[index] = out_ref[there ^ 4]


def row_pass(device, one, g, sample, frequency, factors):
    out = [jax.ShapeDtypeStruct((8, BLOCK, LANES), jnp.float32)] * 2
    scratch = [
        pltpu.VMEM((4, INNER, LANES), jnp.float32),
        pltpu.VMEM((N, LANES), jnp.float32),
        pltpu.VMEM((N, LANES), jnp.float32),
        pltpu.VMEM((DEV, BLOCK, LANES), jnp.float32),
    ]
    specs = [pl.BlockSpec(memory_space=pltpu.SMEM)] + [pl.BlockSpec(memory_space=pltpu.VMEM)] * 32
    run = call(rows_kernel, out, scratch, LIMIT[3], 3 * 10**9, specs)
    return run(device, one, *g, *sample, *frequency, *factors)


def peaks_kernel(bins_ref, device_ref, *refs):
    got, table, offsets_ref, refs = refs[:8], pairs(refs[8:18]), refs[18], refs[19:]
    snr_ref, heights_ref, counts_ref, field_ref, wide_ref, side_ref, pick_ref, x_ref, own_ref, sem = refs
    for index in range(8):
        there = other_chip(device_ref[0], (index & 4) | (-index & 3))
        x_ref[there] = got[index][0]
        x_ref[there ^ 4] = got[index][1]

    def block(first, count):
        body = jnp.concatenate([x_ref[s] for s in range(first, first + count)], axis=1)
        pad = jnp.zeros((8, body.shape[1]), jnp.float32)
        return jnp.concatenate([body, pad], axis=0)

    values = []
    for (_, first, count), pair in zip(CLASSES, table):
        values.append(from_right(block(first, count), *pair))
    energy = x_ref[0, ROWS : BLOCK, :]
    for s in range(1, DEV):
        energy = energy + x_ref[s, ROWS : BLOCK, :]
    mean = jnp.sum(energy[2:3, :], axis=1, keepdims=True)
    inverse = 1.0 / jnp.sqrt(mean + 1e-06)
    for c, value in enumerate(back(values, 1)):
        cols = pl.ds(INNER * c, INNER)
        own_ref[:, cols] = value[0:ROWS] * inverse
        field_ref[8 : ROWS + 8, cols] = value[0:ROWS]
        field_ref[7:8, cols] = value[ROWS : ROWS + 1]
        field_ref[ROWS + 8 : ROWS + 9, cols] = value[ROWS + 1 : ROWS + 2]
    for start in (0,) + tuple(range(8, ROWS + 8, 16)) + (ROWS + 8,):
        size = 8 if start in (0, ROWS + 8) else 16
        value = field_ref[start : start + size, :]
        side = jnp.maximum(pltpu.roll(value, 1, 1), pltpu.roll(value, N - 1, 1))
        wide_ref[start : start + size, :] = jnp.maximum(side, value)
        side_ref[start : start + size, :] = side
    copies = []
    for part in range(8):
        rows = pl.ds(CELL * part, CELL)
        copies.append(pltpu.make_async_copy(own_ref.at[rows], snr_ref.at[rows], sem.at[part]))
        copies[-1].start()
    blocks = lax.shift_right_logical(iota((LANES, N), 1), 4) == iota((LANES, N), 0)
    blocks = jnp.where(blocks, 1.0, 0.0).astype(jnp.bfloat16)
    offsets = offsets_ref[...].astype(jnp.float32).astype(jnp.bfloat16)
    offsets = jnp.concatenate([offsets, offsets], axis=0)
    spread = jnp.dot(offsets, blocks, preferred_element_type=jnp.float32)
    code = (iota((CELL, N), 0) * CELL + (iota((CELL, N), 1) & (CELL - 1))).astype(jnp.float32)
    for p in range(ROWS // CELL):
        base = 8 + CELL * p
        value, side = field_ref[base : base + CELL, :], side_ref[base : base + CELL, :]
        above = wide_ref[base - 1 : base - 1 + CELL, :]
        below = wide_ref[base + 1 : base + 1 + CELL, :]
        nearest = jnp.maximum(side, jnp.maximum(above, below))
        chosen = spread[p : p + 1, :] == code
        height = jnp.where(chosen, value - nearest, 0.0)
        level = jnp.where(chosen, value, 0.0)
        pick_ref[8 * p : 8 * p + 8, :] = height[0:8] + height[8:16]
        pick_ref[HALF + 8 * p : HALF + 8 * p + 8, :] = level[0:8] + level[8:16]
    high, low = split(pick_ref[...])
    gather = partial(
        lax.dot_general,
        dimension_numbers=(((1,), (1,)), ((), ())),
        preferred_element_type=jnp.float32,
    )
    both = gather(jnp.concatenate([high, low], axis=0), blocks)
    both = both[0:LANES] + both[LANES : 2 * LANES]
    rows = [jnp.sum(both[8 * p : 8 * p + 8], axis=0, keepdims=True) for p in range(16)]
    picked = jnp.concatenate(rows, axis=0) * inverse
    heights, values = picked[0:8], picked[8:16]
    heights_ref[...] = heights
    weight = jax.nn.sigmoid(heights * 20.0)
    lane = iota((1, LANES), 1)
    counts = jnp.zeros((1, LANES), jnp.float32)
    for k in range(16):
        level = 0.25 * bins_ref[0, k].astype(jnp.float32)
        above = weight * jax.nn.sigmoid((values - level) * 10.0)
        summed = jnp.sum(jnp.sum(above, axis=0, keepdims=True), axis=1, keepdims=True)
        counts = counts + jnp.where(lane == k, summed, 0.0)
    for s in range(DEV):
        counts_ref[s] = jnp.broadcast_to(counts, (8, LANES))
    for copy in copies:
        copy.wait()


def peak_pass(thresholds, device, x, table, offsets):
    f32 = jnp.float32
    out = [
        jax.ShapeDtypeStruct((ROWS, N), f32),
        jax.ShapeDtypeStruct((8, LANES), f32),
        jax.ShapeDtypeStruct((DEV, 8, LANES), f32),
    ]
    scratch = [
        pltpu.VMEM((ROWS + 16, N), f32),
        pltpu.VMEM((ROWS + 16, N), f32),
        pltpu.VMEM((ROWS + 16, N), f32),
        pltpu.VMEM((LANES, N), f32),
        pltpu.VMEM((DEV, BLOCK, LANES), f32),
        pltpu.VMEM((ROWS, N), f32),
        pltpu.SemaphoreType.DMA((8,)),
    ]
    specs = [pl.BlockSpec(memory_space=pltpu.SMEM)] * 2 + [pl.BlockSpec(memory_space=pltpu.VMEM)] * 19
    places = [pl.BlockSpec(memory_space=pl.ANY)] + [pl.BlockSpec(memory_space=pltpu.VMEM)] * 2
    run = call(peaks_kernel, out, scratch, LIMIT[4], 2 * 10**9, specs, places)
    return run(thresholds, device, *x, *table, offsets)


def finish_kernel(counts_ref, heights_ref, total_ref, out_ref):
    total = counts_ref[0]
    for s in range(1, DEV):
        total = total + counts_ref[s]
    total_ref[...] = total[0:1, 0:16]
    out_ref[...] = heights_ref[...]


def finish(counts, heights):
    out = [
        jax.ShapeDtypeStruct((1, 16), jnp.float32),
        jax.ShapeDtypeStruct((8, LANES), jnp.float32),
    ]
    specs = [pl.BlockSpec(memory_space=pltpu.VMEM)] * 2
    return call(finish_kernel, out, (), 4, 10**6, specs)(counts, heights)


def chip_pairs(index):
    return [(d, (d & 12 ^ (2 * (index & 4))) + ((d + index) & 3)) for d in range(DEV)]


def body(shear, smoothing, offsets, thresholds):
    group = ("row", "col")
    device = lax.axis_index(group).astype(jnp.int32).reshape(1)

    def exchange(x):
        return lax.all_to_all(x, group, split_axis=0, concat_axis=0, tiled=True)

    def scatter(keep, send):
        got = lax.ppermute(send, group, [(d, d ^ 4) for d in range(DEV)])
        blocks = merge(keep, got)
        done = {0: blocks[0]}
        for index in ORDER:
            block = blocks[min(index, 6)]
            done[index] = lax.ppermute(block, group, chip_pairs(index))
        done[6] = lax.ppermute(relay(done[4]), group, chip_pairs(2))
        return [done[index] for index in range(8)]

    blocks = pack(device, shear)
    fields = []
    for field in range(2):
        got = [blocks[4 * field], None, None, None]
        for step in (2, 1, 3):
            pairs = [(c, (c + step) % 4) for c in range(4)]
            got[4 - step] = lax.ppermute(blocks[4 * field + step], "col", pairs)
        fields.append(got)
    sample, frequency, factors = tables(smoothing, device)
    g = columns(device, fields[0], sample)
    one = scatter(*g)
    g = columns(device, fields[1], sample)
    two = scatter(*g)
    one = first_pass(device, one, frequency)
    k = row_pass(device, one, two, sample, frequency, factors)
    out = peak_pass(thresholds, device, scatter(*k), frequency, offsets[0])
    snr, heights, counts = out
    counts, heights = finish(exchange(counts), heights)
    return snr[None], heights[None], counts


def solution(mesh):
    return jax.shard_map(
        body,
        mesh=mesh,
        in_specs=(
            P(None, "maps", "row", "col"),
            P("maps"),
            P("maps", ("row", "col"), None),
            P("maps", None),
        ),
        out_specs=(
            P("maps", ("row", "col"), None),
            P("maps", ("row", "col"), None),
            P("maps", None),
        ),
        check_vma=False,
    )
```

```python
from functools import partial
import math

import jax
import jax.numpy as jnp
from jax import lax
from jax.experimental import pallas as pl
from jax.experimental.pallas import tpu as pltpu
from jax.sharding import PartitionSpec as P


N = 2048
INNER = 512
DENSE = 256
DEV = 16
ROWS = 128
LANES = 128
HALF = 64
CELL = 16
BLOCK = ROWS + 8
CLASSES = ((0, 0, 2), (4, 2, 2), (2, 4, 4), (1, 8, 4), (3, 12, 4))
ROOT = math.sqrt(0.5)
MIB = 1 << 20
LIMIT = (20, 24, 24, 36, 32)
ORDER = (3, 6, 5, 4, 1, 7)
PLACES = (0, 1, 2, 2, 3, 4, 5, 6)


def call(kernel, out, scratch, limit, flops, ins, outs=None):
    return pl.pallas_call(
        kernel,
        out_shape=out,
        in_specs=ins,
        **({} if outs is None else {"out_specs": outs}),
        scratch_shapes=scratch,
        compiler_params=pltpu.CompilerParams(vmem_limit_bytes=limit * MIB),
        cost_estimate=pl.CostEstimate(flops=flops, bytes_accessed=4 * MIB, transcendentals=0),
    )


def split(x):
    high = x.astype(jnp.bfloat16)
    return high, (x - high.astype(jnp.float32)).astype(jnp.bfloat16)


def dot(left, right):
    return jnp.dot(left, right, preferred_element_type=jnp.float32)


def from_left(high_ref, low_ref, x):
    high, low = split(x)
    width = x.shape[1]
    both = dot(high_ref[...], jnp.concatenate([high, low], axis=1))
    return both[:, :width] + (both[:, width:] + dot(low_ref[...], high))


def from_right(x, high_ref, low_ref):
    high, low = split(x)
    height = x.shape[0]
    both = dot(jnp.concatenate([high, low], axis=0), high_ref[...])
    return both[:height] + (both[height:] + dot(high, low_ref[...]))


def pairs(refs):
    return tuple(zip(refs[0::2], refs[1::2]))


def take(x, start, size, axis):
    return lax.slice_in_dim(x, start, start + size, axis=axis)


def front(zero, two, even, odd, axis):
    near = [take(x, 0, DENSE, axis) for x in (zero, two, even, odd)]
    far = [take(x, DENSE, DENSE, axis) for x in (zero, two, even, odd)]
    change, total = ROOT * (far[2] - far[3]), ROOT * (far[2] + far[3])
    join = partial(jnp.concatenate, axis=axis)
    return (
        near[0] + far[0],
        near[0] - far[0],
        join([near[1], -far[1]]),
        join([near[2] + change, -near[3] - total]),
        join([near[2] - change, near[3] - total]),
    )


def back(values, axis):
    first, second, turn, one, three = values
    real = [take(x, 0, DENSE, axis) for x in (turn, one, three)]
    imag = [take(x, DENSE, DENSE, axis) for x in (turn, one, three)]
    change, total = real[1] - real[2], -imag[1] - imag[2]
    halves = (
        (first + second, real[0], real[1] + real[2], imag[2] - imag[1]),
        (first - second, -imag[0], ROOT * (total + change), ROOT * (total - change)),
    )
    blocks = []
    for zero, two, even, odd in halves:
        plus, minus = zero + two, zero - two
        blocks.append((plus + even, minus + odd, plus - even, minus - odd))
    return [jnp.concatenate([near, far], axis=axis) for near, far in zip(*blocks)]


def angle(steps):
    wrapped = jnp.bitwise_and(steps, N - 1)
    wrapped = jnp.where(wrapped >= N // 2, wrapped - N, wrapped)
    return wrapped.astype(jnp.float32) * (2.0 * math.pi / N)


def iota(shape, dim):
    return lax.broadcasted_iota(jnp.int32, shape, dim)


def put(high_ref, low_ref, rows, cols, value):
    high, low = split(value)
    high_ref[rows, cols] = high
    low_ref[rows, cols] = low


def sample_form(refs, scratch):
    cos_ref, sin_ref = scratch
    for (start, _, blocks), (high_ref, low_ref) in zip(CLASSES, refs):
        width = LANES * blocks
        col = iota((HALF, width), 1)
        freq = start + 8 * (HALF * (col // LANES) + col % HALF)
        quarter = jnp.where(col % LANES >= HALF, 1, 0)
        if start == 0:
            freq = jnp.where(col == HALF, N // 2, freq)
            quarter = jnp.where(col == HALF, 0, quarter)
        fine = angle(freq * iota((HALF, width), 0))
        cos_ref[:, :width] = jnp.cos(fine)
        sin_ref[:, :width] = jnp.sin(fine)
        coarse = angle(freq[:8] * (HALF * iota((8, width), 0)) + INNER * quarter[:8])
        cos_high, sin_high = jnp.cos(coarse), jnp.sin(coarse)
        for part in range(DENSE // HALF):
            cos_part, sin_part = cos_high[part : part + 1], sin_high[part : part + 1]
            rows = pl.ds(HALF * part, HALF)
            cos_fine, sin_fine = cos_ref[:, :width], sin_ref[:, :width]
            put(high_ref, low_ref, rows, slice(None), cos_part * cos_fine - sin_part * sin_fine)
            if blocks == 4:
                rows = pl.ds(DENSE + HALF * part, HALF)
                value = sin_part * cos_fine + cos_part * sin_fine
                put(high_ref, low_ref, rows, slice(None), value)


def frequency_form(refs, scratch):
    cos_ref, sin_ref = scratch
    fine = angle(8 * iota((HALF, DENSE), 0) * iota((HALF, DENSE), 1))
    cos_ref[:, :DENSE] = jnp.cos(fine)
    sin_ref[:, :DENSE] = jnp.sin(fine)
    for (start, _, blocks), (high_ref, low_ref) in zip(CLASSES, refs):
        coarse = angle((start + 8 * HALF * iota((8, DENSE), 0)) * iota((8, DENSE), 1))
        cos_high, sin_high = jnp.cos(coarse), jnp.sin(coarse)
        for part in range(blocks):
            cos_part, sin_part = cos_high[part : part + 1], sin_high[part : part + 1]
            cos_fine, sin_fine = cos_ref[:, :DENSE], sin_ref[:, :DENSE]
            cosine = cos_part * cos_fine - sin_part * sin_fine
            sine = sin_part * cos_fine + cos_part * sin_fine
            turned = -sine
            if start == 0 and part == 0:
                flip = (1 - 2 * (iota((HALF, DENSE), 1) & 1)).astype(jnp.float32)
                turned = jnp.where(iota((HALF, DENSE), 0) == 0, flip, turned)
            upper, lower = pl.ds(LANES * part, HALF), pl.ds(LANES * part + HALF, HALF)
            put(high_ref, low_ref, upper, pl.ds(0, DENSE), cosine)
            put(high_ref, low_ref, lower, pl.ds(0, DENSE), turned)
            if blocks == 4:
                put(high_ref, low_ref, upper, pl.ds(DENSE, DENSE), sine)
                put(high_ref, low_ref, lower, pl.ds(DENSE, DENSE), cosine)


def signed(freq):
    return jnp.where(freq < N // 2, freq, freq - N)


def lane_frequency(device, shape):
    lane = iota(shape, 1)
    block = jnp.where(device < 4, device & 1, device & 3)
    start = jnp.where(device < 2, 0, jnp.where(device < 4, 4, 2))
    start = jnp.where(device < 8, start, jnp.where(device < 12, 1, 3))
    freq = signed(start + 8 * (HALF * block + lane % HALF))
    nyquist = (device == 0) & (lane == HALF)
    freq = jnp.where(nyquist, -(N // 2), freq)
    single = nyquist | ((device == 0) & (lane == 0))
    return freq.astype(jnp.float32), jnp.where(single, 1.0, 2.0)


def tables_kernel(smooth_ref, device_ref, *refs):
    device = device_ref[0]
    scratch = refs[-2:]
    w_refs, f_refs = pairs(refs[0:10]), pairs(refs[10:20])
    even_ref, odd_ref, last_ref = refs[20:23]
    sample_form(w_refs, scratch)
    frequency_form(f_refs, scratch)
    width = smooth_ref[0]
    decay = width * width * (-2.0 * math.pi**2 / (N * N))
    shape = (HALF, LANES)
    freq_y, weight = lane_frequency(device, shape)

    def factors(freq_x, weight):
        total = freq_x * freq_x + freq_y * freq_y
        scaled = jnp.exp(decay * total) * weight / jnp.maximum(total, 1.0)
        return (freq_x * freq_x - freq_y * freq_y) * scaled, 2.0 * freq_x * freq_y * scaled

    for start, first, blocks in CLASSES:
        for part in range(blocks):
            freq = signed(start + 8 * (HALF * part + iota(shape, 0)))
            row_weight = jnp.where(freq == 0, 1.0, 2.0) * (1.0 / (N * N))
            even, odd = factors(freq.astype(jnp.float32), weight * row_weight)
            rows = pl.ds(HALF * (first + part), HALF)
            even_ref[rows, :] = even
            odd_ref[rows, :] = odd
    even, odd = factors(jnp.full(shape, -N / 2, jnp.float32), weight * (1.0 / (N * N)))
    last_ref[0:8, :] = even[0:8]
    last_ref[8:16, :] = odd[0:8]


def tables(smoothing, device):
    low = jnp.bfloat16
    table = []
    for _, _, blocks in CLASSES:
        table += [jax.ShapeDtypeStruct((LANES * blocks, LANES * blocks), low)] * 2
    out = table + table + [
        jax.ShapeDtypeStruct((N // 2, LANES), jnp.float32),
        jax.ShapeDtypeStruct((N // 2, LANES), jnp.float32),
        jax.ShapeDtypeStruct((16, LANES), jnp.float32),
    ]
    scratch = [pltpu.VMEM((HALF, INNER), jnp.float32)] * 2
    smem = pl.BlockSpec(memory_space=pltpu.SMEM)
    result = call(tables_kernel, out, scratch, LIMIT[0], 10**9, [smem, smem])(smoothing, device)
    return result[0:10], result[10:20], result[20:23]


def quarters(blocks):
    first, second, third, fourth = blocks
    return (
        (first + third) + (second + fourth),
        (first + third) - (second + fourth),
        first - third,
        second - fourth,
    )


def pack_kernel(device_ref, x_ref, *outs):
    for index in range(8):
        start = pl.multiple_of(((device_ref[0] + index) & 3) * ROWS, ROWS)
        outs[index][...] = x_ref[index // 4, 0, pl.ds(start, ROWS), :]


def pack(device, shear):
    out = [jax.ShapeDtypeStruct((ROWS, INNER), jnp.float32)] * 8
    specs = [pl.BlockSpec(memory_space=pltpu.SMEM), pl.BlockSpec(memory_space=pltpu.VMEM)]
    return call(pack_kernel, out, (), LIMIT[1], 10**6, specs)(device, shear)


def columns_kernel(device_ref, *refs):
    blocks, table = refs[:4], pairs(refs[4:14])
    keep_ref, send_ref, all_ref = refs[14:]
    zero, two, even, odd = quarters([x[...] for x in blocks])
    device = device_ref[0]
    place = device & 3
    along = jnp.where(place == 0, 1.0, jnp.where(place == 2, -1.0, 0.0))
    across = jnp.where(place == 1, 1.0, jnp.where(place == 3, -1.0, 0.0))
    flip = jnp.where((place & 1) == 0, 1.0, -1.0)

    even, odd = along * even - across * odd, across * even + along * odd
    operands = front(zero, flip * two, even, odd, 1)
    for (_, first, count), operand, refs in zip(CLASSES, operands, table):
        value = from_right(operand, *refs)
        for part in range(count):
            all_ref[first + part] = value[:, LANES * part : LANES * (part + 1)]
    for index in range(8):
        there = other_chip(device, index)
        keep_ref[index] = all_ref[there]
        send_ref[index] = all_ref[there ^ 4]


def other_chip(device, index):
    return ((device & 12) ^ (2 * (index & 4))) + ((device + index) & 3)


def columns(device, blocks, table):
    out = [jax.ShapeDtypeStruct((8, ROWS, LANES), jnp.float32)] * 2
    specs = [pl.BlockSpec(memory_space=pltpu.SMEM)] + [pl.BlockSpec(memory_space=pltpu.VMEM)] * 14
    scratch = [pltpu.VMEM((DEV, ROWS, LANES), jnp.float32)]
    return call(columns_kernel, out, scratch, LIMIT[1], 2 * 10**9, specs)(device, *blocks, *table)


def merge_kernel(keep_ref, got_ref, *outs):
    for index in range(8):
        out_ref = outs[PLACES[index]]
        first = 2 if index == 2 else 0
        out_ref[first] = keep_ref[index]
        out_ref[first + 1] = got_ref[index]


def relay_kernel(x_ref, out_ref):
    out_ref[...] = x_ref[2:4]


def relay(x):
    out = jax.ShapeDtypeStruct((2,) + x.shape[1:], jnp.float32)
    return call(relay_kernel, out, (), 8, 10**6, [pl.BlockSpec(memory_space=pltpu.VMEM)])(x)


def merge(keep, got):
    counts = (2, 2, 4, 2, 2, 2, 2)
    out = [jax.ShapeDtypeStruct((n,) + keep.shape[1:], jnp.float32) for n in counts]
    specs = [pl.BlockSpec(memory_space=pltpu.VMEM)] * 2
    return call(merge_kernel, out, (), 8, 10**8, specs)(keep, got)


def to_frequency(device, g_refs, f_refs, part_ref, out_ref):
    flip_core = jnp.where((device & 4) == 0, 1.0, -1.0)
    flip_chip = jnp.where((device & 8) == 0, 1.0, -1.0)
    for step in range(4):
        near, far = g_refs[step], g_refs[4 + step]
        same, other = near[0] + far[0], near[1] + far[1]
        rows = pl.ds(pl.multiple_of(((device - step) & 3) * ROWS, ROWS), ROWS)
        part_ref[0, rows, :] = same + other
        part_ref[1, rows, :] = flip_core * (same - other)
        same, other = flip_chip * (near[0] - far[0]), flip_chip * (near[1] - far[1])
        part_ref[2, rows, :] = jnp.where(flip_core > 0, same, other)
        part_ref[3, rows, :] = jnp.where(flip_core > 0, other, same)
    operands = front(*[part_ref[i] for i in range(4)], 0)
    for (_, first, count), operand, refs in zip(CLASSES, operands, f_refs):
        out_ref[LANES * first : LANES * (first + count), :] = from_left(*refs, operand)


def first_kernel(device_ref, *refs):
    to_frequency(device_ref[0], refs[:8], pairs(refs[8:18]), refs[19], refs[18])


def first_pass(device, g, frequency):
    out = jax.ShapeDtypeStruct((N, LANES), jnp.float32)
    specs = [pl.BlockSpec(memory_space=pltpu.SMEM)] + [pl.BlockSpec(memory_space=pltpu.VMEM)] * 18
    scratch = [pltpu.VMEM((4, INNER, LANES), jnp.float32)]
    return call(first_kernel, out, scratch, LIMIT[2], 10**9, specs)(device, *g, *frequency)


def rows_kernel(device_ref, one_ref, *refs):
    g_refs, refs = refs[:8], refs[8:]
    table = pairs(refs[:10])
    even_ref, odd_ref, last_ref, keep_ref, send_ref, part_ref, two_ref, data_ref, out_ref = refs[20:]
    device = device_ref[0]
    to_frequency(device, g_refs, pairs(refs[10:20]), part_ref, two_ref)
    _, weight = lane_frequency(device, (8, LANES))
    total = jnp.zeros((HALF, LANES), jnp.float32)
    special = jnp.zeros((8, LANES), jnp.float32)
    row, lane = iota((HALF, LANES), 0), iota((HALF, LANES), 1)
    sign = jnp.where(lane < HALF, 1.0, -1.0)
    fix = (lane == HALF) & (device == 0)
    for part in range(DEV):
        upper, lower = pl.ds(LANES * part, HALF), pl.ds(LANES * part + HALF, HALF)
        x_one, x_two = one_ref[upper, :], two_ref[upper, :]
        y_one, y_two = one_ref[lower, :], two_ref[lower, :]
        x_two = jnp.where(fix, -x_one, sign * pltpu.roll(x_two, HALF, 1))
        y_two = jnp.where(fix, -y_one, sign * pltpu.roll(y_two, HALF, 1))
        rows = pl.ds(HALF * part, HALF)
        even, odd = even_ref[rows, :], odd_ref[rows, :]
        cosine = even * x_one - odd * y_two
        sine = even * y_one + odd * x_two
        if part == 0:
            edge, other = y_one[0:8], y_two[0:8]
            turned = sign[0:8] * pltpu.roll(edge, HALF, 1)
            turned = jnp.where(fix[0:8], pltpu.roll(other, HALF, 1), turned)
            edge = last_ref[0:8, :] * edge + last_ref[8:16, :] * turned
            edge = jnp.concatenate([edge] * 8, axis=0)
            cosine = jnp.where(row == 0, even * x_one, cosine)
            sine = jnp.where(row == 0, edge, sine)
            special = (cosine * cosine + sine * sine)[0:8]
        total = total + (cosine * cosine + sine * sine)
        data_ref[upper, :] = cosine
        data_ref[lower, :] = sine
    special = jnp.where(iota((8, LANES), 0) == 0, special, 0.0)
    energy = jnp.sum(total, axis=0, keepdims=True) + jnp.sum(special, axis=0, keepdims=True)
    energy = 0.5 * energy / weight[0:1]

    values = []
    for (_, first, count), refs in zip(CLASSES, table):
        values.append(from_left(*refs, data_ref[LANES * first : LANES * (first + count), :]))
    for r, value in enumerate(back(values, 0)):
        for part in range(4):
            out_ref[4 * r + part, 0:ROWS, :] = value[ROWS * part : ROWS * (part + 1)]
    for s in range(DEV):
        out_ref[s, ROWS : ROWS + 1, :] = out_ref[(s - 1) % DEV, ROWS - 1 : ROWS, :]
        out_ref[s, ROWS + 1 : ROWS + 2, :] = out_ref[(s + 1) % DEV, 0:1, :]
        out_ref[s, ROWS + 2 : ROWS + 3, :] = energy
        out_ref[s, ROWS + 3 : BLOCK, :] = jnp.zeros((BLOCK - ROWS - 3, LANES), jnp.float32)
    for index in range(8):
        there = other_chip(device, index)
        keep_ref[index] = out_ref[there]
        send_ref[index] = out_ref[there ^ 4]


def row_pass(device, one, g, sample, frequency, factors):
    out = [jax.ShapeDtypeStruct((8, BLOCK, LANES), jnp.float32)] * 2
    scratch = [
        pltpu.VMEM((4, INNER, LANES), jnp.float32),
        pltpu.VMEM((N, LANES), jnp.float32),
        pltpu.VMEM((N, LANES), jnp.float32),
        pltpu.VMEM((DEV, BLOCK, LANES), jnp.float32),
    ]
    specs = [pl.BlockSpec(memory_space=pltpu.SMEM)] + [pl.BlockSpec(memory_space=pltpu.VMEM)] * 32
    run = call(rows_kernel, out, scratch, LIMIT[3], 3 * 10**9, specs)
    return run(device, one, *g, *sample, *frequency, *factors)


def peaks_kernel(bins_ref, device_ref, *refs):
    got, table, offsets_ref, refs = refs[:8], pairs(refs[8:18]), refs[18], refs[19:]
    snr_ref, heights_ref, counts_ref, field_ref, wide_ref, side_ref, pick_ref, x_ref, own_ref, sem = refs
    for index in range(8):
        there = other_chip(device_ref[0], (index & 4) | (-index & 3))
        x_ref[there] = got[index][0]
        x_ref[there ^ 4] = got[index][1]

    def block(first, count):
        body = jnp.concatenate([x_ref[s] for s in range(first, first + count)], axis=1)
        pad = jnp.zeros((8, body.shape[1]), jnp.float32)
        return jnp.concatenate([body, pad], axis=0)

    values = []
    for (_, first, count), pair in zip(CLASSES, table):
        values.append(from_right(block(first, count), *pair))
    energy = x_ref[0, ROWS : BLOCK, :]
    for s in range(1, DEV):
        energy = energy + x_ref[s, ROWS : BLOCK, :]
    mean = jnp.sum(energy[2:3, :], axis=1, keepdims=True)
    inverse = 1.0 / jnp.sqrt(mean + 1e-06)
    for c, value in enumerate(back(values, 1)):
        cols = pl.ds(INNER * c, INNER)
        own_ref[:, cols] = value[0:ROWS] * inverse
        field_ref[8 : ROWS + 8, cols] = value[0:ROWS]
        field_ref[7:8, cols] = value[ROWS : ROWS + 1]
        field_ref[ROWS + 8 : ROWS + 9, cols] = value[ROWS + 1 : ROWS + 2]
    for start in (0,) + tuple(range(8, ROWS + 8, 16)) + (ROWS + 8,):
        size = 8 if start in (0, ROWS + 8) else 16
        value = field_ref[start : start + size, :]
        side = jnp.maximum(pltpu.roll(value, 1, 1), pltpu.roll(value, N - 1, 1))
        wide_ref[start : start + size, :] = jnp.maximum(side, value)
        side_ref[start : start + size, :] = side
    copies = []
    for part in range(8):
        rows = pl.ds(CELL * part, CELL)
        copies.append(pltpu.make_async_copy(own_ref.at[rows], snr_ref.at[rows], sem.at[part]))
        copies[-1].start()
    blocks = lax.shift_right_logical(iota((LANES, N), 1), 4) == iota((LANES, N), 0)
    blocks = jnp.where(blocks, 1.0, 0.0).astype(jnp.bfloat16)
    offsets = offsets_ref[...].astype(jnp.float32).astype(jnp.bfloat16)
    offsets = jnp.concatenate([offsets, offsets], axis=0)
    spread = jnp.dot(offsets, blocks, preferred_element_type=jnp.float32)
    code = (iota((CELL, N), 0) * CELL + (iota((CELL, N), 1) & (CELL - 1))).astype(jnp.float32)
    for p in range(ROWS // CELL):
        base = 8 + CELL * p
        value, side = field_ref[base : base + CELL, :], side_ref[base : base + CELL, :]
        above = wide_ref[base - 1 : base - 1 + CELL, :]
        below = wide_ref[base + 1 : base + 1 + CELL, :]
        nearest = jnp.maximum(side, jnp.maximum(above, below))
        chosen = spread[p : p + 1, :] == code
        height = jnp.where(chosen, value - nearest, 0.0)
        level = jnp.where(chosen, value, 0.0)
        pick_ref[8 * p : 8 * p + 8, :] = height[0:8] + height[8:16]
        pick_ref[HALF + 8 * p : HALF + 8 * p + 8, :] = level[0:8] + level[8:16]
    high, low = split(pick_ref[...])
    gather = partial(
        lax.dot_general,
        dimension_numbers=(((1,), (1,)), ((), ())),
        preferred_element_type=jnp.float32,
    )
    both = gather(jnp.concatenate([high, low], axis=0), blocks)
    both = both[0:LANES] + both[LANES : 2 * LANES]
    rows = [jnp.sum(both[8 * p : 8 * p + 8], axis=0, keepdims=True) for p in range(16)]
    picked = jnp.concatenate(rows, axis=0) * inverse
    heights, values = picked[0:8], picked[8:16]
    heights_ref[...] = heights
    weight = jax.nn.sigmoid(heights * 20.0)
    lane = iota((1, LANES), 1)
    counts = jnp.zeros((1, LANES), jnp.float32)
    for k in range(16):
        level = 0.25 * bins_ref[0, k].astype(jnp.float32)
        above = weight * jax.nn.sigmoid((values - level) * 10.0)
        summed = jnp.sum(jnp.sum(above, axis=0, keepdims=True), axis=1, keepdims=True)
        counts = counts + jnp.where(lane == k, summed, 0.0)
    for s in range(DEV):
        counts_ref[s] = jnp.broadcast_to(counts, (8, LANES))
    for copy in copies:
        copy.wait()


def peak_pass(thresholds, device, x, table, offsets):
    f32 = jnp.float32
    out = [
        jax.ShapeDtypeStruct((ROWS, N), f32),
        jax.ShapeDtypeStruct((8, LANES), f32),
        jax.ShapeDtypeStruct((DEV, 8, LANES), f32),
    ]
    scratch = [
        pltpu.VMEM((ROWS + 16, N), f32),
        pltpu.VMEM((ROWS + 16, N), f32),
        pltpu.VMEM((ROWS + 16, N), f32),
        pltpu.VMEM((LANES, N), f32),
        pltpu.VMEM((DEV, BLOCK, LANES), f32),
        pltpu.VMEM((ROWS, N), f32),
        pltpu.SemaphoreType.DMA((8,)),
    ]
    specs = [pl.BlockSpec(memory_space=pltpu.SMEM)] * 2 + [pl.BlockSpec(memory_space=pltpu.VMEM)] * 19
    places = [pl.BlockSpec(memory_space=pl.ANY)] + [pl.BlockSpec(memory_space=pltpu.VMEM)] * 2
    run = call(peaks_kernel, out, scratch, LIMIT[4], 2 * 10**9, specs, places)
    return run(thresholds, device, *x, *table, offsets)


def finish_kernel(counts_ref, heights_ref, total_ref, out_ref):
    total = counts_ref[0]
    for s in range(1, DEV):
        total = total + counts_ref[s]
    total_ref[...] = total[0:1, 0:16]
    out_ref[...] = heights_ref[...]


def finish(counts, heights):
    out = [
        jax.ShapeDtypeStruct((1, 16), jnp.float32),
        jax.ShapeDtypeStruct((8, LANES), jnp.float32),
    ]
    specs = [pl.BlockSpec(memory_space=pltpu.VMEM)] * 2
    return call(finish_kernel, out, (), 4, 10**6, specs)(counts, heights)


def chip_pairs(index):
    return [(d, (d & 12 ^ (2 * (index & 4))) + ((d + index) & 3)) for d in range(DEV)]


def body(shear, smoothing, offsets, thresholds):
    group = ("row", "col")
    device = lax.axis_index(group).astype(jnp.int32).reshape(1)

    def exchange(x):
        return lax.all_to_all(x, group, split_axis=0, concat_axis=0, tiled=True)

    def scatter(keep, send):
        got = lax.ppermute(send, group, [(d, d ^ 4) for d in range(DEV)])
        blocks = merge(keep, got)
        done = {0: blocks[0]}
        for index in ORDER:
            done[index] = lax.ppermute(blocks[PLACES[index]], group, chip_pairs(index))
        done[2] = lax.ppermute(relay(done[3]), group, chip_pairs(3))
        return [done[index] for index in range(8)]

    blocks = pack(device, shear)
    fields = []
    for field in range(2):
        got = [blocks[4 * field], None, None, None]
        for step in (2, 1, 3):
            pairs = [(c, (c + step) % 4) for c in range(4)]
            got[4 - step] = lax.ppermute(blocks[4 * field + step], "col", pairs)
        fields.append(got)
    sample, frequency, factors = tables(smoothing, device)
    g = columns(device, fields[0], sample)
    one = scatter(*g)
    g = columns(device, fields[1], sample)
    two = scatter(*g)
    one = first_pass(device, one, frequency)
    k = row_pass(device, one, two, sample, frequency, factors)
    out = peak_pass(thresholds, device, scatter(*k), frequency, offsets[0])
    snr, heights, counts = out
    counts, heights = finish(exchange(counts), heights)
    return snr[None], heights[None], counts


def solution(mesh):
    return jax.shard_map(
        body,
        mesh=mesh,
        in_specs=(
            P(None, "maps", "row", "col"),
            P("maps"),
            P("maps", ("row", "col"), None),
            P("maps", None),
        ),
        out_specs=(
            P("maps", ("row", "col"), None),
            P("maps", ("row", "col"), None),
            P("maps", None),
        ),
        check_vma=False,
    )
```
